32 devices in a mesh: pod: 4 (over y, z), mp: 8 (over x, core).
Axes of the slice: x: 4, y: 2, z: 2, core: 2. Of those that a mesh axis runs over, the one named last changes fastest.
The devices are a block of a 4x4x8 slice.
Arguments:
- d_pool: bfloat16 [65536, 26, 128], P(('pod', 'mp')), parts along dimension 0
- row_ids: int32 [128, 16384, 1], P(('pod', 'mp')), parts along dimension 0
- lengths: int32 [128, 16384], P(('pod', 'mp')), parts along dimension 0
- tables: bfloat16 [128, 16384, 128], P(('pod', 'mp')), parts along dimension 0
- row_accum: float32 [128, 16384], P(('pod', 'mp')), parts along dimension 0
- learn_rate: float32 [], replicated
Outputs:
- output 1: bfloat16 [128, 16384, 128], P(('pod', 'mp')), parts along dimension 0
- output 2: float32 [128, 16384], P(('pod', 'mp')), parts along dimension 0
There are 4 independent parts. The reference program is written for one: setup_inputs(seed, part) draws one part's arguments, and reference() takes and returns one part's arrays. A program takes and returns all parts, laid end to end along the dimension named above; an argument that names none is the same for every part.
All inputs are finite; a program needn't handle non-finite values.
Results may differ from the reference program's by a relative error of at most 0.001.
Values are sent between devices in bfloat16 or wider.
A program may use at most 768 MiB of HBM per device.

```python
import jax
import jax.numpy as jnp
from jax import lax

TABLES = 26
EMB_DIM = 128
TABLE_ROWS = 16384
MAX_HOT = 1
N_SLOTS = 32
BATCH_ALL = 16384
HOT_SET = 64
EPSILON = 1e-06
HOTNESS_LIST = (3, 2, 1, 2, 6, 1, 1, 1, 1, 7, 3, 8, 1, 6, 9, 5, 1, 1, 1, 12, 100, 27, 10, 3, 1, 1)


def slot_hotness():
    hot_list = [min(HOTNESS_LIST[table_idx], MAX_HOT) if table_idx < TABLES else 0 for table_idx in range(N_SLOTS)]
    return jnp.array(hot_list, dtype=jnp.int32)


def draw_routing(route_key):
    slot_hot = slot_hotness()[:, None]
    key_len, key_pick, key_hot, key_uni = jax.random.split(route_key, 4)
    id_shape = (N_SLOTS, BATCH_ALL, MAX_HOT)
    raw_len = jax.random.randint(key_len, (N_SLOTS, BATCH_ALL), 0, 1 << 20)
    lengths = jnp.where(slot_hot > 0, raw_len % (slot_hot + 1), 0)
    lengths = lengths.at[:, 0].set(slot_hot[:, 0])
    hot_pick = jax.random.randint(key_pick, id_shape, 0, 4)
    hot_ids = jax.random.randint(key_hot, id_shape, 0, HOT_SET) * (TABLE_ROWS // HOT_SET)
    uni_ids = jax.random.randint(key_uni, id_shape, 0, TABLE_ROWS)
    row_ids = jnp.where(hot_pick == 0, hot_ids, uni_ids)
    row_ids = row_ids.at[:, 0, 0].set(TABLE_ROWS - 1)
    row_ids = row_ids.at[:, 1, 0].set(0)
    return row_ids.astype(jnp.int32), lengths.astype(jnp.int32)


def setup_inputs(seed: int = 0, part: int = 0) -> dict:
    seed_key = jax.random.key(seed)
    part_key = jax.random.fold_in(seed_key, part)
    key_grad, key_tab, key_acc, key_route = jax.random.split(part_key, 4)
    d_pool = jax.random.normal(key_grad, (BATCH_ALL, TABLES, EMB_DIM), jnp.float32).astype(jnp.bfloat16)
    row_ids, lengths = draw_routing(key_route)
    tables = jax.random.normal(key_tab, (N_SLOTS, TABLE_ROWS, EMB_DIM), jnp.float32).astype(jnp.bfloat16)
    row_accum = jax.random.uniform(key_acc, (N_SLOTS, TABLE_ROWS), jnp.float32, 0.2, 1.0)
    learn_rate = jax.random.uniform(jax.random.key(seed + 1), (), jnp.float32, 0.5, 1.5)
    return {'d_pool': d_pool, 'row_ids': row_ids, 'lengths': lengths, 'tables': tables, 'row_accum': row_accum, 'learn_rate': learn_rate}


def reference(d_pool, row_ids, lengths, tables, row_accum, learn_rate):
    padded = jnp.pad(d_pool, ((0, 0), (0, N_SLOTS - TABLES), (0, 0)))
    by_slot = jnp.transpose(padded, (1, 0, 2))
    positions = jnp.arange(MAX_HOT)

    def one_slot(packed):
        slot_grad, slot_ids, slot_len, slot_table, slot_accum = packed
        grad_vals = slot_grad.astype(jnp.float32)

        def add_position(row_grad, pos_idx):
            keep_mask = (pos_idx < slot_len)[:, None]
            row_grad = row_grad.at[slot_ids[:, pos_idx]].add(jnp.where(keep_mask, grad_vals, 0.0))
            return row_grad, None

        row_grad, unused_out = lax.scan(add_position, jnp.zeros((TABLE_ROWS, EMB_DIM), jnp.float32), positions)
        new_accum = slot_accum + jnp.mean(row_grad * row_grad, axis=-1)
        row_scale = learn_rate / (jnp.sqrt(new_accum) + EPSILON)
        new_table = (slot_table.astype(jnp.float32) - row_grad * row_scale[:, None]).astype(jnp.bfloat16)
        return new_table, new_accum

    new_tables, new_accum = lax.map(one_slot, (by_slot, row_ids, lengths, tables, row_accum))
    return new_tables, new_accum
```

```python
import functools

import jax
import jax.numpy as jnp
from jax import lax
from jax.experimental import pallas as pl
from jax.experimental.pallas import tpu as pltpu
from jax.sharding import PartitionSpec as P


EPSILON = 1e-06
BANKS = 4
UNROLL = 8
BLOCK = 128


def update_kernel(slot, n_carried, ids_ref, lr_ref, grad_ref, tables_ref, accums_ref, *refs):
    out_tables_ref, out_accums_ref, *scratch = refs[n_carried:]
    table_ref, accum_ref = tables_ref.at[slot], accums_ref.at[slot]
    out_table_ref, out_accum_ref = out_tables_ref.at[slot], out_accums_ref.at[slot]
    banks = scratch[:BANKS]
    stage, table_v, accum_v, table_o, accum_o, grad_v, sem = scratch[BANKS:]
    segs, seg_rows, dim = grad_ref.shape
    n_rows = table_ref.shape[0]
    grad_copy = pltpu.make_async_copy(grad_ref, grad_v, sem.at[0])
    table_copy = pltpu.make_async_copy(table_ref, table_v, sem.at[1])
    accum_copy = pltpu.make_async_copy(accum_ref, accum_v, sem.at[2])
    grad_copy.start()
    table_copy.start()
    accum_copy.start()

    zero = jnp.zeros((BLOCK, dim), jnp.float32)

    def clear(i, carry):
        for bank in banks:
            bank[pl.ds(pl.multiple_of(i * BLOCK, BLOCK), BLOCK), :] = zero
        return carry

    lax.fori_loop(0, n_rows // BLOCK, clear, 0)
    for bank in banks:
        bank[pl.ds(n_rows, 8), :] = zero[:8]
    grad_copy.wait()
    per_bank = segs // BANKS
    for part in range(per_bank):
        def widen(i, carry):
            for j in range(BANKS):
                rows = pl.ds(pl.multiple_of(i * BLOCK, BLOCK), BLOCK)
                stage[j, rows, :] = grad_v[j * per_bank + part, rows, :].astype(jnp.float32)
            return carry

        lax.fori_loop(0, seg_rows // BLOCK, widen, 0)

        def add_rows(i, carry):
            base = i * UNROLL
            for u in range(UNROLL):
                for j in range(BANKS):
                    row = ids_ref[0, (j * per_bank + part) * seg_rows + base + u]
                    banks[j][pl.ds(row, 1), :] += stage[j, pl.ds(base + u, 1), :]
            return carry

        lax.fori_loop(0, seg_rows // UNROLL, add_rows, 0)

    table_copy.wait()
    accum_copy.wait()
    eye = lax.broadcasted_iota(jnp.int32, (BLOCK, dim), 0) == lax.broadcasted_iota(jnp.int32, (BLOCK, dim), 1)
    lr = lr_ref[0]

    def update(i, carry):
        rows = pl.ds(pl.multiple_of(i * BLOCK, BLOCK), BLOCK)
        grad = banks[0][rows, :]
        for bank in banks[1:]:
            grad = grad + bank[rows, :]
        old = jnp.where(eye, accum_v[pl.ds(i, 1), :], 0.0)
        new = jnp.sum(grad * grad * (1.0 / dim) + old, axis=1, keepdims=True)
        scale = lr / (jnp.sqrt(new) + EPSILON)
        table_o[rows, :] = (table_v[rows, :].astype(jnp.float32) - grad * scale).astype(jnp.bfloat16)
        accum_o[pl.ds(i, 1), :] = jnp.sum(jnp.where(eye, new, 0.0), axis=0, keepdims=True)
        return carry

    lax.fori_loop(0, n_rows // BLOCK, update, 0)
    out_copy = pltpu.make_async_copy(table_o, out_table_ref, sem.at[0])
    out_acc = pltpu.make_async_copy(accum_o, out_accum_ref, sem.at[1])
    out_copy.start()
    out_acc.start()
    out_copy.wait()
    out_acc.wait()


def update_slot(slot, ids, lr, grad, tables, accums, carried):
    _, n_rows, dim = tables.shape
    segs, seg_rows, _ = grad.shape
    return pl.pallas_call(
        functools.partial(update_kernel, slot, len(carried)),
        out_shape=tuple(jax.ShapeDtypeStruct(x.shape, x.dtype) for x in (tables, accums)),
        in_specs=[pl.BlockSpec(memory_space=pltpu.SMEM)] * 2 + [pl.BlockSpec(memory_space=pl.ANY)] * (3 + len(carried)),
        out_specs=(pl.BlockSpec(memory_space=pl.ANY),) * 2,
        input_output_aliases={5 + i: i for i in range(len(carried))},
        scratch_shapes=[pltpu.VMEM((n_rows + 8, dim), jnp.float32)] * BANKS + [
            pltpu.VMEM((BANKS, seg_rows, dim), jnp.float32),
            pltpu.VMEM((n_rows, dim), jnp.bfloat16),
            pltpu.VMEM((n_rows // BLOCK, BLOCK), jnp.float32),
            pltpu.VMEM((n_rows, dim), jnp.bfloat16),
            pltpu.VMEM((n_rows // BLOCK, BLOCK), jnp.float32),
            pltpu.VMEM((segs, seg_rows, dim), jnp.bfloat16),
            pltpu.SemaphoreType.DMA((3,)),
        ],
        compiler_params=pltpu.CompilerParams(vmem_limit_bytes=66000000),
        cost_estimate=pl.CostEstimate(flops=n_rows * dim * 400, bytes_accessed=4 * n_rows * dim * 2, transcendentals=0),
    )(ids, lr, grad, tables, accums, *carried)


def solution(mesh):
    n_group = mesh.shape['mp']
    slot_spec = P(('pod', 'mp'))

    def local_step(d_pool, row_ids, lengths, tables, row_accum, learn_rate):
        slots_dev, n_rows, _ = tables.shape
        by_table = jnp.transpose(d_pool, (1, 0, 2))
        n_tab = by_table.shape[0]
        padded = jnp.pad(by_table, ((0, slots_dev * n_group - n_tab), (0, 0), (0, 0)))
        ids = jnp.where(lengths > 0, row_ids[:, :, 0], n_rows)
        lr = learn_rate.reshape(1)
        accums = row_accum.reshape(slots_dev, -1, BLOCK)
        got = []
        for k in range(slots_dev):
            got.append(lax.all_to_all(padded[k::slots_dev], 'mp', 0, 0, tiled=True))
        carried = ()
        for k in range(slots_dev):
            carried = update_slot(k, ids[k:k + 1], lr, got[k], tables, accums, carried)
        return carried[0], carried[1].reshape(row_accum.shape)

    return jax.shard_map(local_step, mesh=mesh, in_specs=(slot_spec, slot_spec, slot_spec, slot_spec, slot_spec, P()), out_specs=(slot_spec, slot_spec), check_vma=False)
```

```python
import functools

import jax
import jax.numpy as jnp
from jax import lax
from jax.experimental import pallas as pl
from jax.experimental.pallas import tpu as pltpu
from jax.sharding import PartitionSpec as P


EPSILON = 1e-06
BANKS = 4
UNROLL = 8
BLOCK = 128
CHUNK = 1024
MAX_LANE = 64
VMEM_LIMIT = 66000000


def plan_kernel(n_dev, n_rows, ids_ref, lengths_ref, plan_ref, *refs):
    *packed_refs, ids_v, len_v = refs
    n_slots, batch = ids_ref.shape
    part = batch // n_dev
    for d in range(n_dev):
        ids_v[d * n_slots:(d + 1) * n_slots, :] = ids_ref[:, d * part:(d + 1) * part]
        len_v[d * n_slots:(d + 1) * n_slots, :] = lengths_ref[:, d * part:(d + 1) * part]
    rows = n_dev * n_slots
    below = lax.broadcasted_iota(jnp.int32, (BLOCK, BLOCK), 0) < lax.broadcasted_iota(jnp.int32, (BLOCK, BLOCK), 1)
    prefix = jnp.where(below, 1.0, 0.0).astype(jnp.bfloat16)
    lane = lax.broadcasted_iota(jnp.int32, (rows, BLOCK), 1)
    count = jnp.zeros((rows, 1), jnp.int32)
    starts = jnp.zeros((rows, BLOCK), jnp.int32)
    moves = []
    for b in range(part // BLOCK):
        cols = slice(b * BLOCK, (b + 1) * BLOCK)
        valid = len_v[:, cols] > 0
        ones = jnp.where(valid, 1.0, 0.0)
        local = jnp.dot(ones.astype(jnp.bfloat16), prefix, preferred_element_type=jnp.float32).astype(jnp.int32)
        place = jnp.where(valid, local, -1)
        for d in range(n_dev):
            plan_ref[d, :, cols] = place[d * n_slots:(d + 1) * n_slots, :]
        starts = jnp.where(lane == b, count, starts)
        shift = (b * BLOCK + lane) - (count + local)
        moves.append(jnp.where(valid, (shift << 16) | ids_v[:, cols], n_rows))
        count = count + jnp.sum(ones, axis=1, keepdims=True).astype(jnp.int32)
    most = jnp.max(count, axis=0, keepdims=True)
    starts = jnp.where(lane == MAX_LANE, most, starts)
    for d in range(n_dev):
        plan_ref[d, :, part:] = starts[d * n_slots:(d + 1) * n_slots, :]
    move = jnp.concatenate(moves, axis=1)
    step = 1
    while step < part:
        come = pltpu.roll(move, part - step, 1)
        bit = step << 16
        stay = jnp.where((move & bit) != 0, n_rows, move)
        move = jnp.where((come & bit) != 0, come, stay)
        step *= 2
    spot = lax.broadcasted_iota(jnp.int32, (rows, part), 1)
    packed = jnp.where(spot < count, move & 0xFFFF, n_rows)
    for s in range(n_slots):
        for d in range(n_dev):
            packed_refs[s][d:d + 1, :] = packed[d * n_slots + s:d * n_slots + s + 1, :]


def make_plan(ids, lengths, n_dev, n_rows):
    n_slots, batch = ids.shape
    part = batch // n_dev
    return pl.pallas_call(
        functools.partial(plan_kernel, n_dev, n_rows),
        out_shape=(jax.ShapeDtypeStruct((n_dev, n_slots, part + BLOCK), jnp.int32),)
        + (jax.ShapeDtypeStruct((n_dev, part), jnp.int32),) * n_slots,
        in_specs=[pl.BlockSpec(memory_space=pltpu.VMEM)] * 2,
        out_specs=(pl.BlockSpec(memory_space=pltpu.VMEM),) * (1 + n_slots),
        scratch_shapes=[pltpu.VMEM((n_dev * n_slots, part), jnp.int32)] * 2,
        compiler_params=pltpu.CompilerParams(vmem_limit_bytes=32000000),
        cost_estimate=pl.CostEstimate(flops=20000000, bytes_accessed=2000000, transcendentals=0),
    )(ids, lengths)


def pack_kernel(slot, n_used, starts_ref, plan_ref, tables_ref, out_ref, grad_v, stage, pack_v, in_sem, out_sem):
    _, cap, _ = out_ref.shape
    n_slots = plan_ref.shape[1]
    part = tables_ref.shape[1]
    slot_row = lax.broadcasted_iota(jnp.int32, (BLOCK, BLOCK), 0)

    def fetch(d, buf):
        return pltpu.make_async_copy(tables_ref.at[d * n_slots + slot], grad_v.at[buf], in_sem.at[buf])

    def emit(d, buf):
        return pltpu.make_async_copy(pack_v.at[buf], out_ref.at[d], out_sem.at[buf])

    fetch(0, 0).start()

    def table(d, carry):
        buf = d % 2

        @pl.when(d + 1 < n_used)
        def _():
            fetch(d + 1, 1 - buf).start()

        fetch(d, buf).wait()

        @pl.when(d >= 2)
        def _():
            emit(d - 2, buf).wait()

        for b in range(part // BLOCK):
            place = plan_ref[d, slot:slot + 1, b * BLOCK:(b + 1) * BLOCK]
            pick = jnp.where(slot_row == place, 1.0, 0.0).astype(jnp.bfloat16)
            rows = jnp.dot(pick, grad_v[buf, b * BLOCK:(b + 1) * BLOCK, :], preferred_element_type=jnp.float32)
            stage[pl.ds(starts_ref[d, slot, b], BLOCK), :] = rows
        pack_v[buf] = stage[:cap, :].astype(jnp.bfloat16)
        emit(d, buf).start()
        return carry

    lax.fori_loop(0, n_used, table, 0)
    for d in range(max(n_used - 2, 0), n_used):
        emit(d, d % 2).wait()


def pack_slot(slot, cap, starts, plan, by_table):
    n_dev, n_slots, _ = plan.shape
    n_tab, part, dim = by_table.shape
    n_used = len(range(slot, n_tab, n_slots))
    return pl.pallas_call(
        functools.partial(pack_kernel, slot, n_used),
        out_shape=jax.ShapeDtypeStruct((n_dev, cap, dim), by_table.dtype),
        in_specs=[pl.BlockSpec(memory_space=pltpu.SMEM), pl.BlockSpec(memory_space=pltpu.VMEM), pl.BlockSpec(memory_space=pl.ANY)],
        out_specs=pl.BlockSpec(memory_space=pl.ANY),
        scratch_shapes=[
            pltpu.VMEM((2, part, dim), by_table.dtype),
            pltpu.VMEM((cap + BLOCK, dim), jnp.float32),
            pltpu.VMEM((2, cap, dim), by_table.dtype),
            pltpu.SemaphoreType.DMA((2,)),
            pltpu.SemaphoreType.DMA((2,)),
        ],
        compiler_params=pltpu.CompilerParams(vmem_limit_bytes=VMEM_LIMIT),
        cost_estimate=pl.CostEstimate(flops=n_used * part * dim * 20, bytes_accessed=n_used * part * dim * 3, transcendentals=0),
    )(starts, plan, by_table)


def apply_kernel(slot, n_carried, ids_ref, lr_ref, grad_ref, tables_ref, accums_ref, *refs):
    out_tables_ref, out_accums_ref, *scratch = refs[n_carried:]
    out_table_ref, out_accum_ref = out_tables_ref.at[slot], out_accums_ref.at[slot]
    banks = scratch[:BANKS]
    stage, table_v, accum_v, grad_v, sem = scratch[BANKS:]
    segs, seg_rows, dim = grad_ref.shape
    n_rows = tables_ref.shape[1]
    grad_copy = pltpu.make_async_copy(grad_ref, grad_v, sem.at[0])
    table_copy = pltpu.make_async_copy(tables_ref.at[slot], table_v, sem.at[1])
    accum_copy = pltpu.make_async_copy(accums_ref.at[slot], accum_v, sem.at[2])
    grad_copy.start()
    table_copy.start()
    accum_copy.start()

    zero = jnp.zeros((BLOCK, dim), jnp.float32)

    def clear(i, carry):
        for bank in banks:
            bank[pl.ds(pl.multiple_of(i * BLOCK, BLOCK), BLOCK), :] = zero
        return carry

    lax.fori_loop(0, n_rows // BLOCK, clear, 0)
    for bank in banks:
        bank[pl.ds(n_rows, 8), :] = zero[:8]
    grad_copy.wait()
    per_bank = segs // BANKS
    for part in range(per_bank):
        def widen(i, carry):
            for j in range(BANKS):
                rows = pl.ds(pl.multiple_of(i * 64, 64), 64)
                stage[j, rows, :] = grad_v[j * per_bank + part, rows, :].astype(jnp.float32)
            return carry

        lax.fori_loop(0, seg_rows // 64, widen, 0)

        def add_rows(i, carry):
            base = i * UNROLL
            for u in range(UNROLL):
                for j in range(BANKS):
                    row = ids_ref[j * per_bank + part, base + u]
                    banks[j][pl.ds(row, 1), :] += stage[j, pl.ds(base + u, 1), :]
            return carry

        lax.fori_loop(0, seg_rows // UNROLL, add_rows, 0)

    table_copy.wait()
    accum_copy.wait()
    eye = lax.broadcasted_iota(jnp.int32, (BLOCK, dim), 0) == lax.broadcasted_iota(jnp.int32, (BLOCK, dim), 1)
    lr = lr_ref[0]

    def update(c, carry):
        for s in range(CHUNK // BLOCK):
            i = c * (CHUNK // BLOCK) + s
            rows = pl.ds(pl.multiple_of(i * BLOCK, BLOCK), BLOCK)
            grad = banks[0][rows, :]
            for bank in banks[1:]:
                grad = grad + bank[rows, :]
            old = jnp.where(eye, accum_v[pl.ds(i, 1), :], 0.0)
            new = jnp.sum(grad * grad * (1.0 / dim) + old, axis=1, keepdims=True)
            scale = lr / (jnp.sqrt(new) + EPSILON)
            table_v[rows, :] = (table_v[rows, :].astype(jnp.float32) - grad * scale).astype(jnp.bfloat16)
            accum_v[pl.ds(i, 1), :] = jnp.sum(jnp.where(eye, new, 0.0), axis=0, keepdims=True)
        done = pl.ds(pl.multiple_of(c * CHUNK, CHUNK), CHUNK)
        pltpu.make_async_copy(table_v.at[done], out_table_ref.at[done], sem.at[0]).start()
        return carry

    lax.fori_loop(0, n_rows // CHUNK, update, 0)
    out_acc = pltpu.make_async_copy(accum_v, out_accum_ref, sem.at[1])
    out_acc.start()
    pltpu.make_async_copy(table_v, out_table_ref, sem.at[0]).wait()
    out_acc.wait()


def apply_slot(slot, ids, lr, grad, tables, accums, carried):
    _, n_rows, dim = tables.shape
    segs, seg_rows, _ = grad.shape
    return pl.pallas_call(
        functools.partial(apply_kernel, slot, len(carried)),
        out_shape=tuple(jax.ShapeDtypeStruct(x.shape, x.dtype) for x in (tables, accums)),
        in_specs=[pl.BlockSpec(memory_space=pltpu.SMEM)] * 2 + [pl.BlockSpec(memory_space=pl.ANY)] * (3 + len(carried)),
        out_specs=(pl.BlockSpec(memory_space=pl.ANY),) * 2,
        input_output_aliases={5 + i: i for i in range(len(carried))},
        scratch_shapes=[pltpu.VMEM((n_rows + 8, dim), jnp.float32)] * BANKS + [
            pltpu.VMEM((BANKS, seg_rows, dim), jnp.float32),
            pltpu.VMEM((n_rows, dim), tables.dtype),
            pltpu.VMEM((n_rows // BLOCK, BLOCK), jnp.float32),
            pltpu.VMEM((segs, seg_rows, dim), grad.dtype),
            pltpu.SemaphoreType.DMA((3,)),
        ],
        compiler_params=pltpu.CompilerParams(vmem_limit_bytes=VMEM_LIMIT),
        cost_estimate=pl.CostEstimate(flops=n_rows * dim * 400, bytes_accessed=4 * n_rows * dim * 2, transcendentals=0),
    )(ids, lr, grad, tables, accums, *carried)


def solution(mesh):
    n_group = mesh.shape['mp']
    slot_spec = P(('pod', 'mp'))

    def local_step(d_pool, row_ids, lengths, tables, row_accum, learn_rate):
        n_slots, n_rows, _ = tables.shape
        by_table = jnp.transpose(d_pool, (1, 0, 2))
        part = by_table.shape[1]
        plan_out, *ids = make_plan(row_ids[:, :, 0], lengths, n_group, n_rows)
        plan = lax.all_to_all(plan_out, 'mp', 0, 0, tiled=True)
        starts = plan[:, :, part:]
        most = jnp.max(starts[:, :, MAX_LANE])
        lr = learn_rate.reshape(1)
        accums = row_accum.reshape(n_slots, -1, BLOCK)
        caps = tuple(c for c in CAPS(part))

        def exchange(level):
            def run(operands):
                by_table, plan, starts, ids, lr, tables, accums = operands
                got = []
                for k in range(n_slots):
                    pack = pack_slot(k, caps[level], starts, plan, by_table)
                    got.append(lax.all_to_all(pack, 'mp', 0, 0, tiled=True))
                carried = ()
                for k in range(n_slots):
                    carried = apply_slot(k, ids[k], lr, got[k], tables, accums, carried)
                return carried

            return run

        level = sum((most > cap).astype(jnp.int32) for cap in caps[:-1])
        operands = (by_table, plan, starts, tuple(ids), lr, tables, accums)
        new_tables, new_accums = lax.switch(level, [exchange(i) for i in range(len(caps))], operands)
        return new_tables, new_accums.reshape(row_accum.shape)

    return jax.shard_map(local_step, mesh=mesh, in_specs=(slot_spec, slot_spec, slot_spec, slot_spec, slot_spec, P()), out_specs=(slot_spec, slot_spec), check_vma=False)


def CAPS(part):
    return (part * 9 // 16, part)
```

```python
import functools

import jax
import jax.numpy as jnp
from jax import lax
from jax.experimental import pallas as pl
from jax.experimental.pallas import tpu as pltpu
from jax.sharding import PartitionSpec as P


EPSILON = 1e-06
TINY = 1e-36
BANKS = 4
UNROLL = 8
BLOCK = 128
CHUNK = 1024
MAX_LANE = 64
VMEM_LIMIT = 66000000


def plan_kernel(n_dev, n_rows, ids_ref, lengths_ref, plan_ref, *refs):
    *packed_refs, ids_v, len_v = refs
    n_slots, batch = ids_ref.shape
    part = batch // n_dev
    for d in range(n_dev):
        ids_v[d * n_slots:(d + 1) * n_slots, :] = ids_ref[:, d * part:(d + 1) * part]
        len_v[d * n_slots:(d + 1) * n_slots, :] = lengths_ref[:, d * part:(d + 1) * part]
    rows = n_dev * n_slots
    below = lax.broadcasted_iota(jnp.int32, (BLOCK, BLOCK), 0) < lax.broadcasted_iota(jnp.int32, (BLOCK, BLOCK), 1)
    prefix = jnp.where(below, 1.0, 0.0).astype(jnp.bfloat16)
    lane = lax.broadcasted_iota(jnp.int32, (rows, BLOCK), 1)
    count = jnp.zeros((rows, 1), jnp.int32)
    starts = jnp.zeros((rows, BLOCK), jnp.int32)
    moves = []
    for b in range(part // BLOCK):
        cols = slice(b * BLOCK, (b + 1) * BLOCK)
        valid = len_v[:, cols] > 0
        ones = jnp.where(valid, 1.0, 0.0)
        local = jnp.dot(ones.astype(jnp.bfloat16), prefix, preferred_element_type=jnp.float32).astype(jnp.int32)
        place = jnp.where(valid, local, -1)
        for d in range(n_dev):
            plan_ref[d, :, cols] = place[d * n_slots:(d + 1) * n_slots, :]
        starts = jnp.where(lane == b, count, starts)
        shift = (b * BLOCK + lane) - (count + local)
        moves.append(jnp.where(valid, (shift << 16) | ids_v[:, cols], n_rows))
        count = count + jnp.sum(ones, axis=1, keepdims=True).astype(jnp.int32)
    most = jnp.max(count, axis=0, keepdims=True)
    starts = jnp.where(lane == MAX_LANE, most, starts)
    for d in range(n_dev):
        plan_ref[d, :, part:] = starts[d * n_slots:(d + 1) * n_slots, :]
    move = jnp.concatenate(moves, axis=1)
    step = 1
    while step < part:
        come = pltpu.roll(move, part - step, 1)
        bit = step << 16
        stay = jnp.where((move & bit) != 0, n_rows, move)
        move = jnp.where((come & bit) != 0, come, stay)
        step *= 2
    spot = lax.broadcasted_iota(jnp.int32, (rows, part), 1)
    packed = jnp.where(spot < count, move & 0xFFFF, n_rows)
    for s in range(n_slots):
        for j in range(n_dev // 2):
            low, high = ((2 * j + h) * n_slots + s for h in range(2))
            packed_refs[s][:, j * part:(j + 1) * part] = packed[low:low + 1, :] | (packed[high:high + 1, :] << 16)
        packed_refs[s][:, n_dev // 2 * part:] = jnp.broadcast_to(most, (1, BLOCK))


def make_plan(ids, lengths, n_dev, n_rows):
    n_slots, batch = ids.shape
    part = batch // n_dev
    return pl.pallas_call(
        functools.partial(plan_kernel, n_dev, n_rows),
        out_shape=(jax.ShapeDtypeStruct((n_dev, n_slots, part + BLOCK), jnp.int32),)
        + (jax.ShapeDtypeStruct((1, batch // 2 + BLOCK), jnp.int32),) * n_slots,
        in_specs=[pl.BlockSpec(memory_space=pltpu.VMEM)] * 2,
        out_specs=(pl.BlockSpec(memory_space=pltpu.VMEM),) * (1 + n_slots),
        scratch_shapes=[pltpu.VMEM((n_dev * n_slots, part), jnp.int32)] * 2,
        compiler_params=pltpu.CompilerParams(vmem_limit_bytes=32000000),
        cost_estimate=pl.CostEstimate(flops=20000000, bytes_accessed=2000000, transcendentals=0),
    )(ids, lengths)


def pack_kernel(slot, n_used, starts_ref, plan_ref, tables_ref, out_ref, grad_v, stage, pack_v, in_sem, out_sem):
    _, cap, _ = out_ref.shape
    n_slots = plan_ref.shape[1]
    part = tables_ref.shape[1]
    slot_row = lax.broadcasted_iota(jnp.int32, (BLOCK, BLOCK), 0)

    def fetch(d, buf):
        return pltpu.make_async_copy(tables_ref.at[d * n_slots + slot], grad_v.at[buf], in_sem.at[buf])

    def emit(d, buf):
        return pltpu.make_async_copy(pack_v.at[buf], out_ref.at[d], out_sem.at[buf])

    for d in range(n_used):
        fetch(d, d).start()

    def table(d, carry):
        buf = d % 2
        fetch(d, d).wait()

        @pl.when(d >= 2)
        def _():
            emit(d - 2, buf).wait()

        for b in range(part // BLOCK):
            place = plan_ref[d, slot:slot + 1, b * BLOCK:(b + 1) * BLOCK]
            pick = jnp.where(slot_row == place, 1.0, 0.0).astype(jnp.bfloat16)
            rows = jnp.dot(pick, grad_v[d, b * BLOCK:(b + 1) * BLOCK, :], preferred_element_type=jnp.float32)
            stage[pl.ds(starts_ref[d, slot, b], BLOCK), :] = rows
        pack_v[buf] = stage[:cap, :].astype(jnp.bfloat16)
        emit(d, buf).start()
        return carry

    lax.fori_loop(0, n_used, table, 0)
    for d in range(max(n_used - 2, 0), n_used):
        emit(d, d % 2).wait()


def pack_slot(slot, cap, starts, plan, by_table):
    n_dev, n_slots, _ = plan.shape
    n_tab, part, dim = by_table.shape
    n_used = len(range(slot, n_tab, n_slots))
    return pl.pallas_call(
        functools.partial(pack_kernel, slot, n_used),
        out_shape=jax.ShapeDtypeStruct((n_dev, cap, dim), by_table.dtype),
        in_specs=[pl.BlockSpec(memory_space=pltpu.SMEM), pl.BlockSpec(memory_space=pltpu.VMEM), pl.BlockSpec(memory_space=pl.ANY)],
        out_specs=pl.BlockSpec(memory_space=pl.ANY),
        scratch_shapes=[
            pltpu.VMEM((n_used, part, dim), by_table.dtype),
            pltpu.VMEM((cap + BLOCK, dim), jnp.float32),
            pltpu.VMEM((2, cap, dim), by_table.dtype),
            pltpu.SemaphoreType.DMA((n_used,)),
            pltpu.SemaphoreType.DMA((2,)),
        ],
        compiler_params=pltpu.CompilerParams(vmem_limit_bytes=VMEM_LIMIT),
        cost_estimate=pl.CostEstimate(flops=n_used * part * dim * 20, bytes_accessed=n_used * part * dim * 3, transcendentals=0),
    )(starts, plan, by_table)


def apply_kernel(slot, n_carried, ids_ref, lr_ref, grad_ref, tables_ref, accums_ref, *refs):
    carried_refs, (out_tables_ref, out_accums_ref, *scratch) = refs[:n_carried], refs[n_carried:]
    banks = scratch[:BANKS]
    stage, table_v, grad_v, sem = scratch[BANKS:]
    segs, seg_rows, dim = grad_ref.shape
    n_rows = tables_ref.shape[1]
    id_stride = (ids_ref.shape[1] - BLOCK) // BANKS
    grad_copy = pltpu.make_async_copy(grad_ref, grad_v, sem.at[0])
    table_copy = pltpu.make_async_copy(tables_ref.at[slot], table_v, sem.at[1])
    grad_copy.start()
    table_copy.start()

    zero = jnp.zeros((BLOCK, dim), jnp.float32)

    def clear(i, carry):
        for bank in banks:
            bank[pl.ds(pl.multiple_of(i * BLOCK, BLOCK), BLOCK), :] = zero
        return carry

    lax.fori_loop(0, n_rows // BLOCK, clear, 0)
    for bank in banks:
        bank[pl.ds(n_rows, 8), :] = zero[:8]
    grad_copy.wait()

    def widen(i, carry):
        for j in range(segs):
            rows = pl.ds(pl.multiple_of(i * 32, 32), 32)
            stage[j, rows, :] = grad_v[j, rows, :].astype(jnp.float32)
        return carry

    lax.fori_loop(0, seg_rows // 32, widen, 0)

    def add_rows(i, carry):
        base = i * UNROLL
        for u in range(UNROLL):
            for j, bank in enumerate(banks):
                pair = ids_ref[0, j * id_stride + u + base]
                first, second = pair & 0xFFFF, pair >> 16
                same = jnp.full((1, dim), first) == jnp.full((1, dim), second)
                add_first = stage[2 * j, pl.ds(base + u, 1), :]
                add_second = stage[2 * j + 1, pl.ds(base + u, 1), :]
                add_second = jnp.where(same, add_first + add_second, add_second)
                old_first = bank[pl.ds(first, 1), :]
                old_second = bank[pl.ds(second, 1), :]
                bank[pl.ds(first, 1), :] = old_first + add_first
                bank[pl.ds(second, 1), :] = old_second + add_second
        return carry

    lax.fori_loop(0, (ids_ref[0, BANKS * id_stride] + UNROLL - 1) // UNROLL, add_rows, 0)

    table_copy.wait()
    out_accums_ref[...] = (carried_refs[1] if n_carried else accums_ref)[...]
    eye = lax.broadcasted_iota(jnp.int32, (BLOCK, dim), 0) == lax.broadcasted_iota(jnp.int32, (BLOCK, dim), 1)
    lr = lr_ref[0]

    def update(c, carry):
        for s in range(CHUNK // BLOCK):
            i = c * (CHUNK // BLOCK) + s
            rows = pl.ds(pl.multiple_of(i * BLOCK, BLOCK), BLOCK)
            cols = pl.ds(pl.multiple_of(i * BLOCK, BLOCK), BLOCK)
            grad = banks[0][rows, :]
            for bank in banks[1:]:
                grad = grad + bank[rows, :]
            old = jnp.where(eye, accums_ref[slot:slot + 1, cols], 0.0)
            new = jnp.sum(grad * grad * (1.0 / dim) + old, axis=1, keepdims=True)
            out_accums_ref[slot:slot + 1, cols] = jnp.sum(jnp.where(eye, new, 0.0), axis=0, keepdims=True)
            root = lax.rsqrt(jnp.maximum(new, TINY))
            scale = lr * root / (1.0 + EPSILON * root)
            table_v[rows, :] = (table_v[rows, :].astype(jnp.float32) - grad * scale).astype(jnp.bfloat16)
        done = pl.ds(pl.multiple_of(c * CHUNK, CHUNK), CHUNK)
        pltpu.make_async_copy(table_v.at[done], out_tables_ref.at[slot, done], sem.at[0]).start()
        return carry

    lax.fori_loop(0, n_rows // CHUNK, update, 0)
    pltpu.make_async_copy(table_v, out_tables_ref.at[slot], sem.at[0]).wait()


def apply_slot(slot, ids, lr, grad, tables, accums, carried):
    _, n_rows, dim = tables.shape
    segs, seg_rows, _ = grad.shape
    return pl.pallas_call(
        functools.partial(apply_kernel, slot, len(carried)),
        out_shape=tuple(jax.ShapeDtypeStruct(x.shape, x.dtype) for x in (tables, accums)),
        in_specs=[pl.BlockSpec(memory_space=pltpu.SMEM)] * 2
        + [pl.BlockSpec(memory_space=pl.ANY)] * 2
        + [pl.BlockSpec(memory_space=pltpu.VMEM)]
        + [pl.BlockSpec(memory_space=pl.ANY), pl.BlockSpec(memory_space=pltpu.VMEM)][:len(carried)],
        out_specs=(pl.BlockSpec(memory_space=pl.ANY), pl.BlockSpec(memory_space=pltpu.VMEM)),
        input_output_aliases={5: 0} if carried else {},
        scratch_shapes=[pltpu.VMEM((n_rows + 8, dim), jnp.float32)] * BANKS + [
            pltpu.VMEM((segs, seg_rows, dim), jnp.float32),
            pltpu.VMEM((n_rows, dim), tables.dtype),
            pltpu.VMEM((segs, seg_rows, dim), grad.dtype),
            pltpu.SemaphoreType.DMA((2,)),
        ],
        compiler_params=pltpu.CompilerParams(vmem_limit_bytes=VMEM_LIMIT),
        cost_estimate=pl.CostEstimate(flops=n_rows * dim * 400, bytes_accessed=4 * n_rows * dim * 2, transcendentals=0),
    )(ids, lr, grad, tables, accums, *carried)


def solution(mesh):
    n_group = mesh.shape['mp']
    slot_spec = P(('pod', 'mp'))

    def local_step(d_pool, row_ids, lengths, tables, row_accum, learn_rate):
        n_slots, n_rows, _ = tables.shape
        by_table = jnp.transpose(d_pool, (1, 0, 2))
        part = by_table.shape[1]
        plan_out, *ids = make_plan(row_ids[:, :, 0], lengths, n_group, n_rows)
        plan = lax.all_to_all(plan_out, 'mp', 0, 0, tiled=True)
        starts = plan[:, :, part:]
        most = jnp.max(starts[:, :, MAX_LANE])
        lr = learn_rate.reshape(1)
        caps = tuple(c for c in CAPS(part))

        def exchange(level):
            def run(operands):
                by_table, plan, starts, ids, lr, tables, accums = operands
                got = []
                for k in range(n_slots):
                    pack = pack_slot(k, caps[level], starts, plan, by_table)
                    got.append(lax.all_to_all(pack, 'mp', 0, 0, tiled=True))
                carried = ()
                for k in range(n_slots):
                    carried = apply_slot(k, ids[k], lr, got[k], tables, accums, carried)
                return tuple(carried)

            return run

        level = sum((most > cap).astype(jnp.int32) for cap in caps[:-1])
        operands = (by_table, plan, starts, tuple(ids), lr, tables, row_accum)
        return lax.switch(level, [exchange(i) for i in range(len(caps))], operands)

    return jax.shard_map(local_step, mesh=mesh, in_specs=(slot_spec, slot_spec, slot_spec, slot_spec, slot_spec, P()), out_specs=(slot_spec, slot_spec), check_vma=False)


def CAPS(part):
    return (part * 9 // 16, part)
```

```python
import functools

import jax
import jax.numpy as jnp
from jax import lax
from jax.experimental import pallas as pl
from jax.experimental.pallas import tpu as pltpu
from jax.sharding import PartitionSpec as P


EPSILON = 1e-06
TINY = 1e-36
BANKS = 4
UNROLL = 8
BLOCK = 128
CHUNK = 1024
MAX_LANE = 64
VMEM_LIMIT = 66000000


def plan_kernel(n_dev, n_rows, me_ref, ids_ref, lengths_ref, plan_ref, *refs):
    *packed_refs, ids_v, len_v = refs
    me = me_ref[0]
    n_slots, batch = ids_ref.shape
    part = batch // n_dev
    for d in range(n_dev):
        ids_v[d * n_slots:(d + 1) * n_slots, :] = ids_ref[:, d * part:(d + 1) * part]
        len_v[d * n_slots:(d + 1) * n_slots, :] = lengths_ref[:, d * part:(d + 1) * part]
    rows = n_dev * n_slots
    below = lax.broadcasted_iota(jnp.int32, (BLOCK, BLOCK), 0) < lax.broadcasted_iota(jnp.int32, (BLOCK, BLOCK), 1)
    prefix = jnp.where(below, 1.0, 0.0).astype(jnp.bfloat16)
    lane = lax.broadcasted_iota(jnp.int32, (rows, BLOCK), 1)
    count = jnp.zeros((rows, 1), jnp.int32)
    starts = jnp.zeros((rows, BLOCK), jnp.int32)
    moves = []
    for b in range(part // BLOCK):
        cols = slice(b * BLOCK, (b + 1) * BLOCK)
        valid = len_v[:, cols] > 0
        ones = jnp.where(valid, 1.0, 0.0)
        local = jnp.dot(ones.astype(jnp.bfloat16), prefix, preferred_element_type=jnp.float32).astype(jnp.int32)
        place = jnp.where(valid, local, -1)
        for d in range(n_dev):
            plan_ref[d, :, cols] = place[d * n_slots:(d + 1) * n_slots, :]
        starts = jnp.where(lane == b, count, starts)
        shift = (b * BLOCK + lane) - (count + local)
        moves.append(jnp.where(valid, (shift << 16) | ids_v[:, cols], n_rows))
        count = count + jnp.sum(ones, axis=1, keepdims=True).astype(jnp.int32)
    most = jnp.max(count, axis=0, keepdims=True)
    starts = jnp.where(lane == MAX_LANE, most, starts)
    for d in range(n_dev):
        plan_ref[d, :, part:] = starts[d * n_slots:(d + 1) * n_slots, :]
    move = jnp.concatenate(moves, axis=1)
    step = 1
    while step < part:
        come = pltpu.roll(move, part - step, 1)
        bit = step << 16
        stay = jnp.where((move & bit) != 0, n_rows, move)
        move = jnp.where((come & bit) != 0, come, stay)
        step *= 2
    spot = lax.broadcasted_iota(jnp.int32, (rows, part), 1)
    ids_v[...] = jnp.where(spot < count, move & 0xFFFF, n_rows)
    for s in range(n_slots):
        for j in range(n_dev // 2):
            low, high = (ids_v[pl.ds((me + (n_dev - 2 * j - h)) % n_dev * n_slots + s, 1), :] for h in range(2))
            packed_refs[s][:, j * part:(j + 1) * part] = low | (high << 16)
        packed_refs[s][:, n_dev // 2 * part:] = jnp.broadcast_to(most, (1, BLOCK))


def make_plan(me, ids, lengths, n_dev, n_rows):
    n_slots, batch = ids.shape
    part = batch // n_dev
    return pl.pallas_call(
        functools.partial(plan_kernel, n_dev, n_rows),
        out_shape=(jax.ShapeDtypeStruct((n_dev, n_slots, part + BLOCK), jnp.int32),)
        + (jax.ShapeDtypeStruct((1, batch // 2 + BLOCK), jnp.int32),) * n_slots,
        in_specs=[pl.BlockSpec(memory_space=pltpu.SMEM)] + [pl.BlockSpec(memory_space=pltpu.VMEM)] * 2,
        out_specs=(pl.BlockSpec(memory_space=pltpu.VMEM),) * (1 + n_slots),
        scratch_shapes=[pltpu.VMEM((n_dev * n_slots, part), jnp.int32)] * 2,
        compiler_params=pltpu.CompilerParams(vmem_limit_bytes=32000000),
        cost_estimate=pl.CostEstimate(flops=20000000, bytes_accessed=2000000, transcendentals=0),
    )(me, ids, lengths)


def pack_kernel(slot, me_ref, starts_ref, plan_ref, tables_ref, *refs):
    n_dev, n_slots, _ = plan_ref.shape
    n_tab, part, _ = tables_ref.shape
    out_refs, (grad_v, stage, pack_v, in_sem, out_sem) = refs[:n_dev], refs[n_dev:]
    cap = pack_v.shape[1]
    slot_row = lax.broadcasted_iota(jnp.int32, (BLOCK, BLOCK), 0)
    me = me_ref[0]

    def fetch(o):
        table = jnp.minimum((me + o) % n_dev * n_slots + slot, n_tab - 1)
        return pltpu.make_async_copy(tables_ref.at[table], grad_v.at[o], in_sem.at[o])

    for o in range(n_dev):
        fetch(o).start()

    def one(o, carry):
        d = (me + o) % n_dev
        fetch(o).wait()

        @pl.when(d * n_slots + slot < n_tab)
        def _():
            for b in range(part // BLOCK):
                place = plan_ref[d, slot:slot + 1, b * BLOCK:(b + 1) * BLOCK]
                pick = jnp.where(slot_row == place, 1.0, 0.0).astype(jnp.bfloat16)
                rows = jnp.dot(pick, grad_v[o, b * BLOCK:(b + 1) * BLOCK, :], preferred_element_type=jnp.float32)
                stage[pl.ds(starts_ref[d, slot, b], BLOCK), :] = rows
            pack_v[o] = stage[:cap, :].astype(jnp.bfloat16)

        return carry

    lax.fori_loop(0, n_dev, one, 0)
    copies = [pltpu.make_async_copy(pack_v.at[o], out_refs[o], out_sem.at[o]) for o in range(n_dev)]
    for copy in copies:
        copy.start()
    for copy in copies:
        copy.wait()


def pack_slot(slot, cap, me, starts, plan, by_table):
    n_dev, _, _ = plan.shape
    _, part, dim = by_table.shape
    return pl.pallas_call(
        functools.partial(pack_kernel, slot),
        out_shape=(jax.ShapeDtypeStruct((cap, dim), by_table.dtype),) * n_dev,
        in_specs=[pl.BlockSpec(memory_space=pltpu.SMEM)] * 2 + [pl.BlockSpec(memory_space=pltpu.VMEM), pl.BlockSpec(memory_space=pl.ANY)],
        out_specs=(pl.BlockSpec(memory_space=pl.ANY),) * n_dev,
        scratch_shapes=[
            pltpu.VMEM((n_dev, part, dim), by_table.dtype),
            pltpu.VMEM((cap + BLOCK, dim), jnp.float32),
            pltpu.VMEM((n_dev, cap, dim), by_table.dtype),
            pltpu.SemaphoreType.DMA((n_dev,)),
            pltpu.SemaphoreType.DMA((n_dev,)),
        ],
        compiler_params=pltpu.CompilerParams(vmem_limit_bytes=VMEM_LIMIT),
        cost_estimate=pl.CostEstimate(flops=n_dev * part * dim * 20, bytes_accessed=n_dev * part * dim * 3, transcendentals=0),
    )(me, starts, plan, by_table)


def apply_kernel(slot, n_carried, n_dev, ids_ref, lr_ref, tables_ref, accums_ref, *refs):
    grad_refs, carried_refs = refs[:n_dev], refs[n_dev:n_dev + n_carried]
    out_tables_ref, out_accums_ref, *scratch = refs[n_dev + n_carried:]
    banks = scratch[:BANKS]
    stage, table_v, grad_v, sem = scratch[BANKS:]
    segs, seg_rows, dim = grad_v.shape
    n_rows = tables_ref.shape[1]
    id_stride = (ids_ref.shape[1] - BLOCK) // BANKS
    grad_copies = [pltpu.make_async_copy(ref, grad_v.at[o], sem.at[2 + o]) for o, ref in enumerate(grad_refs)]
    table_copy = pltpu.make_async_copy(tables_ref.at[slot], table_v, sem.at[1])
    for copy in grad_copies:
        copy.start()
    table_copy.start()

    zero = jnp.zeros((BLOCK, dim), jnp.float32)

    def clear(i, carry):
        for bank in banks:
            bank[pl.ds(pl.multiple_of(i * BLOCK, BLOCK), BLOCK), :] = zero
        return carry

    lax.fori_loop(0, n_rows // BLOCK, clear, 0)
    for bank in banks:
        bank[pl.ds(n_rows, 8), :] = zero[:8]
    for copy in grad_copies:
        copy.wait()

    def widen(i, carry):
        for j in range(segs):
            rows = pl.ds(pl.multiple_of(i * 32, 32), 32)
            stage[j, rows, :] = grad_v[j, rows, :].astype(jnp.float32)
        return carry

    lax.fori_loop(0, seg_rows // 32, widen, 0)

    def add_rows(i, carry):
        base = i * UNROLL
        for u in range(UNROLL):
            for j, bank in enumerate(banks):
                pair = ids_ref[0, j * id_stride + u + base]
                first, second = pair & 0xFFFF, pair >> 16
                same = jnp.full((1, dim), first) == jnp.full((1, dim), second)
                add_first = stage[2 * j, pl.ds(base + u, 1), :]
                add_second = stage[2 * j + 1, pl.ds(base + u, 1), :]
                add_second = jnp.where(same, add_first + add_second, add_second)
                old_first = bank[pl.ds(first, 1), :]
                old_second = bank[pl.ds(second, 1), :]
                bank[pl.ds(first, 1), :] = old_first + add_first
                bank[pl.ds(second, 1), :] = old_second + add_second
        return carry

    lax.fori_loop(0, (ids_ref[0, BANKS * id_stride] + UNROLL - 1) // UNROLL, add_rows, 0)

    table_copy.wait()
    out_accums_ref[...] = (carried_refs[1] if n_carried else accums_ref)[...]
    eye = lax.broadcasted_iota(jnp.int32, (BLOCK, dim), 0) == lax.broadcasted_iota(jnp.int32, (BLOCK, dim), 1)
    lr = lr_ref[0]

    def update(c, carry):
        for s in range(CHUNK // BLOCK):
            i = c * (CHUNK // BLOCK) + s
            rows = pl.ds(pl.multiple_of(i * BLOCK, BLOCK), BLOCK)
            cols = pl.ds(pl.multiple_of(i * BLOCK, BLOCK), BLOCK)
            grad = banks[0][rows, :]
            for bank in banks[1:]:
                grad = grad + bank[rows, :]
            old = jnp.where(eye, accums_ref[slot:slot + 1, cols], 0.0)
            new = jnp.sum(grad * grad * (1.0 / dim) + old, axis=1, keepdims=True)
            out_accums_ref[slot:slot + 1, cols] = jnp.sum(jnp.where(eye, new, 0.0), axis=0, keepdims=True)
            root = lax.rsqrt(jnp.maximum(new, TINY))
            scale = lr * root / (1.0 + EPSILON * root)
            table_v[rows, :] = (table_v[rows, :].astype(jnp.float32) - grad * scale).astype(jnp.bfloat16)
        done = pl.ds(pl.multiple_of(c * CHUNK, CHUNK), CHUNK)
        pltpu.make_async_copy(table_v.at[done], out_tables_ref.at[slot, done], sem.at[0]).start()
        return carry

    lax.fori_loop(0, n_rows // CHUNK, update, 0)
    pltpu.make_async_copy(table_v, out_tables_ref.at[slot], sem.at[0]).wait()


def apply_slot(slot, ids, lr, grads, tables, accums, carried):
    _, n_rows, dim = tables.shape
    segs, (seg_rows, _) = len(grads), grads[0].shape
    return pl.pallas_call(
        functools.partial(apply_kernel, slot, len(carried), segs),
        out_shape=tuple(jax.ShapeDtypeStruct(x.shape, x.dtype) for x in (tables, accums)),
        in_specs=[pl.BlockSpec(memory_space=pltpu.SMEM)] * 2
        + [pl.BlockSpec(memory_space=pl.ANY), pl.BlockSpec(memory_space=pltpu.VMEM)]
        + [pl.BlockSpec(memory_space=pl.ANY)] * segs
        + [pl.BlockSpec(memory_space=pl.ANY), pl.BlockSpec(memory_space=pltpu.VMEM)][:len(carried)],
        out_specs=(pl.BlockSpec(memory_space=pl.ANY), pl.BlockSpec(memory_space=pltpu.VMEM)),
        input_output_aliases={4 + segs: 0} if carried else {},
        scratch_shapes=[pltpu.VMEM((n_rows + 8, dim), jnp.float32)] * BANKS + [
            pltpu.VMEM((segs, seg_rows, dim), jnp.float32),
            pltpu.VMEM((n_rows, dim), tables.dtype),
            pltpu.VMEM((segs, seg_rows, dim), grads[0].dtype),
            pltpu.SemaphoreType.DMA((2 + segs,)),
        ],
        compiler_params=pltpu.CompilerParams(vmem_limit_bytes=VMEM_LIMIT),
        cost_estimate=pl.CostEstimate(flops=n_rows * dim * 400, bytes_accessed=4 * n_rows * dim * 2, transcendentals=0),
    )(ids, lr, tables, accums, *grads, *carried)


def routes(n_dev, n_slots, n_tab, slot, offset):
    pairs = [(d, (d + offset) % n_dev) for d in range(n_dev)]
    return [(src, dst) for src, dst in pairs if dst * n_slots + slot < n_tab]


def solution(mesh):
    n_group = mesh.shape['mp']
    slot_spec = P(('pod', 'mp'))

    def local_step(d_pool, row_ids, lengths, tables, row_accum, learn_rate):
        n_slots, n_rows, _ = tables.shape
        by_table = jnp.transpose(d_pool, (1, 0, 2))
        part = by_table.shape[1]
        me = lax.axis_index('mp').reshape(1)
        n_tab = by_table.shape[0]
        plan_out, *ids = make_plan(me, row_ids[:, :, 0], lengths, n_group, n_rows)
        plan = lax.all_to_all(plan_out, 'mp', 0, 0, tiled=True)
        starts = plan[:, :, part:]
        most = jnp.max(starts[:, :, MAX_LANE])
        lr = learn_rate.reshape(1)
        caps = tuple(c for c in CAPS(part))

        def exchange(level):
            def run(operands):
                me, by_table, plan, starts, ids, lr, tables, accums = operands
                got = []
                for k in range(n_slots):
                    pack = pack_slot(k, caps[level], me, starts, plan, by_table)
                    got.append([pack[0]] + [lax.ppermute(pack[o], 'mp', routes(n_group, n_slots, n_tab, k, o)) for o in range(1, n_group)])
                carried = ()
                for k in range(n_slots):
                    carried = apply_slot(k, ids[k], lr, got[k], tables, accums, carried)
                return tuple(carried)

            return run

        level = sum((most > cap).astype(jnp.int32) for cap in caps[:-1])
        operands = (me, by_table, plan, starts, tuple(ids), lr, tables, row_accum)
        return lax.switch(level, [exchange(i) for i in range(len(caps))], operands)

    return jax.shard_map(local_step, mesh=mesh, in_specs=(slot_spec, slot_spec, slot_spec, slot_spec, slot_spec, P()), out_specs=(slot_spec, slot_spec), check_vma=False)


def CAPS(part):
    return (part * 9 // 16, part)
```

```python
import functools

import jax
import jax.numpy as jnp
from jax import lax
from jax.experimental import pallas as pl
from jax.experimental.pallas import tpu as pltpu
from jax.sharding import PartitionSpec as P


EPSILON = 1e-06
TINY = 1e-36
BANKS = 4
UNROLL = 8
BLOCK = 128
CHUNK = 1024
MAX_LANE = 64
VMEM_LIMIT = 66000000


def plan_kernel(n_dev, n_rows, ids_ref, lengths_ref, plan_ref, *refs):
    *packed_refs, ids_v, len_v = refs
    n_slots, batch = ids_ref.shape
    part = batch // n_dev
    for d in range(n_dev):
        ids_v[d * n_slots:(d + 1) * n_slots, :] = ids_ref[:, d * part:(d + 1) * part]
        len_v[d * n_slots:(d + 1) * n_slots, :] = lengths_ref[:, d * part:(d + 1) * part]
    rows = n_dev * n_slots
    below = lax.broadcasted_iota(jnp.int32, (BLOCK, BLOCK), 0) < lax.broadcasted_iota(jnp.int32, (BLOCK, BLOCK), 1)
    prefix = jnp.where(below, 1.0, 0.0).astype(jnp.bfloat16)
    lane = lax.broadcasted_iota(jnp.int32, (rows, BLOCK), 1)
    count = jnp.zeros((rows, 1), jnp.int32)
    starts = jnp.zeros((rows, BLOCK), jnp.int32)
    moves = []
    for b in range(part // BLOCK):
        cols = slice(b * BLOCK, (b + 1) * BLOCK)
        valid = len_v[:, cols] > 0
        ones = jnp.where(valid, 1.0, 0.0)
        local = jnp.dot(ones.astype(jnp.bfloat16), prefix, preferred_element_type=jnp.float32).astype(jnp.int32)
        place = jnp.where(valid, local, -1)
        for d in range(n_dev):
            plan_ref[d, :, cols] = place[d * n_slots:(d + 1) * n_slots, :]
        starts = jnp.where(lane == b, count, starts)
        shift = (b * BLOCK + lane) - (count + local)
        moves.append(jnp.where(valid, (shift << 16) | ids_v[:, cols], n_rows))
        count = count + jnp.sum(ones, axis=1, keepdims=True).astype(jnp.int32)
    most = jnp.max(count, axis=0, keepdims=True)
    starts = jnp.where(lane == MAX_LANE, most, starts)
    for d in range(n_dev):
        plan_ref[d, :, part:] = starts[d * n_slots:(d + 1) * n_slots, :]
    move = jnp.concatenate(moves, axis=1)
    step = 1
    while step < part:
        come = pltpu.roll(move, part - step, 1)
        bit = step << 16
        stay = jnp.where((move & bit) != 0, n_rows, move)
        move = jnp.where((come & bit) != 0, come, stay)
        step *= 2
    spot = lax.broadcasted_iota(jnp.int32, (rows, part), 1)
    packed = jnp.where(spot < count, move & 0xFFFF, n_rows)
    for s in range(n_slots):
        for j in range(n_dev // 2):
            low, high = ((2 * j + h) * n_slots + s for h in range(2))
            packed_refs[s][:, j * part:(j + 1) * part] = packed[low:low + 1, :] | (packed[high:high + 1, :] << 16)
        packed_refs[s][:, n_dev // 2 * part:] = jnp.broadcast_to(most, (1, BLOCK))


def make_plan(ids, lengths, n_dev, n_rows):
    n_slots, batch = ids.shape
    part = batch // n_dev
    return pl.pallas_call(
        functools.partial(plan_kernel, n_dev, n_rows),
        out_shape=(jax.ShapeDtypeStruct((n_dev, n_slots, part + BLOCK), jnp.int32),)
        + (jax.ShapeDtypeStruct((1, batch // 2 + BLOCK), jnp.int32),) * n_slots,
        in_specs=[pl.BlockSpec(memory_space=pltpu.VMEM)] * 2,
        out_specs=(pl.BlockSpec(memory_space=pltpu.VMEM),) * (1 + n_slots),
        scratch_shapes=[pltpu.VMEM((n_dev * n_slots, part), jnp.int32)] * 2,
        compiler_params=pltpu.CompilerParams(vmem_limit_bytes=32000000),
        cost_estimate=pl.CostEstimate(flops=20000000, bytes_accessed=2000000, transcendentals=0),
    )(ids, lengths)


def share_kernel(n_dev, plan_ref, plans_ref, starts_ref, most_ref, send_sem, recv_sem, own_sem):
    pod, me = lax.axis_index('pod'), lax.axis_index('mp')
    barrier = pltpu.get_barrier_semaphore()
    for o in range(1, n_dev):
        pl.semaphore_signal(barrier, inc=1, device_id=(pod, (me + o) % n_dev), device_id_type=pl.DeviceIdType.MESH)
    pl.semaphore_wait(barrier, n_dev - 1)
    copies = [
        pltpu.make_async_remote_copy(
            src_ref=plan_ref.at[(me + o) % n_dev],
            dst_ref=plans_ref.at[me],
            send_sem=send_sem.at[o],
            recv_sem=recv_sem.at[o],
            device_id=(pod, (me + o) % n_dev),
            device_id_type=pl.DeviceIdType.MESH,
        )
        for o in range(1, n_dev)
    ]
    for copy in copies:
        copy.start()
    own = pltpu.make_async_copy(plan_ref.at[me], plans_ref.at[me], own_sem)
    own.start()
    own.wait()
    for copy in copies:
        copy.wait()
    part = plans_ref.shape[2] - BLOCK
    starts = plans_ref[:, :, part:]
    starts_ref[...] = starts
    most_ref[0] = jnp.max(starts[:, :, MAX_LANE:MAX_LANE + 1])


def share_plan(plan):
    n_dev, n_slots, _ = plan.shape
    return pl.pallas_call(
        functools.partial(share_kernel, n_dev),
        out_shape=(
            jax.ShapeDtypeStruct(plan.shape, plan.dtype),
            jax.ShapeDtypeStruct((n_dev, n_slots, BLOCK), plan.dtype),
            jax.ShapeDtypeStruct((1,), plan.dtype),
        ),
        in_specs=[pl.BlockSpec(memory_space=pltpu.VMEM)],
        out_specs=(pl.BlockSpec(memory_space=pltpu.VMEM), pl.BlockSpec(memory_space=pltpu.VMEM), pl.BlockSpec(memory_space=pltpu.SMEM)),
        scratch_shapes=[pltpu.SemaphoreType.DMA((n_dev,)), pltpu.SemaphoreType.DMA((n_dev,)), pltpu.SemaphoreType.DMA],
        compiler_params=pltpu.CompilerParams(collective_id=0, has_side_effects=True, vmem_limit_bytes=16000000),
        cost_estimate=pl.CostEstimate(flops=20000000, bytes_accessed=2000000, transcendentals=0),
    )(plan)


def pack_kernel(slots, starts_ref, plan_ref, tables_ref, out_ref, grad_v, stage, pack_v, in_sem, out_sem):
    n_slots = plan_ref.shape[1]
    cap = out_ref.shape[2]
    n_tab, part, _ = tables_ref.shape
    slot_row = lax.broadcasted_iota(jnp.int32, (BLOCK, BLOCK), 0)
    used = [[d for d in range(out_ref.shape[0]) if d * n_slots + slot < n_tab] for slot in slots]

    def fetch(i, d):
        return pltpu.make_async_copy(tables_ref.at[d * n_slots + slots[i]], grad_v.at[i, d], in_sem.at[i, d])

    def emit(i, d):
        return pltpu.make_async_copy(pack_v.at[i, d], out_ref.at[d, i], out_sem.at[i, d])

    for i, dests in enumerate(used):
        for d in dests:
            fetch(i, d).start()
    for i, dests in enumerate(used):
        def table(d, carry):
            fetch(i, d).wait()
            for b in range(part // BLOCK):
                place = plan_ref[d, slots[i]:slots[i] + 1, b * BLOCK:(b + 1) * BLOCK]
                pick = jnp.where(slot_row == place, 1.0, 0.0).astype(jnp.bfloat16)
                rows = jnp.dot(pick, grad_v[i, d, b * BLOCK:(b + 1) * BLOCK, :], preferred_element_type=jnp.float32)
                stage[pl.ds(starts_ref[d, slots[i], b], BLOCK), :] = rows
            pack_v[i, d] = stage[:cap, :].astype(jnp.bfloat16)
            emit(i, d).start()
            return carry

        lax.fori_loop(0, len(dests), table, 0)
    for i, dests in enumerate(used):
        for d in dests:
            emit(i, d).wait()


def pack_slots(slots, cap, starts, plan, by_table):
    n_dev = plan.shape[0]
    _, part, dim = by_table.shape
    n = len(slots)
    return pl.pallas_call(
        functools.partial(pack_kernel, slots),
        out_shape=jax.ShapeDtypeStruct((n_dev, n, cap, dim), by_table.dtype),
        in_specs=[pl.BlockSpec(memory_space=pltpu.SMEM), pl.BlockSpec(memory_space=pltpu.VMEM), pl.BlockSpec(memory_space=pl.ANY)],
        out_specs=pl.BlockSpec(memory_space=pl.ANY),
        scratch_shapes=[
            pltpu.VMEM((n, n_dev, part, dim), by_table.dtype),
            pltpu.VMEM((cap + BLOCK, dim), jnp.float32),
            pltpu.VMEM((n, n_dev, cap, dim), by_table.dtype),
            pltpu.SemaphoreType.DMA((n, n_dev)),
            pltpu.SemaphoreType.DMA((n, n_dev)),
        ],
        compiler_params=pltpu.CompilerParams(vmem_limit_bytes=VMEM_LIMIT),
        cost_estimate=pl.CostEstimate(flops=n * n_dev * part * dim * 20, bytes_accessed=n * n_dev * part * dim * 3, transcendentals=0),
    )(starts, plan, by_table)


def apply_kernel(slot, place, n_carried, ids_ref, lr_ref, grad_ref, tables_ref, accums_ref, *refs):
    carried_refs, (out_tables_ref, out_accums_ref, *scratch) = refs[:n_carried], refs[n_carried:]
    banks = scratch[:BANKS]
    stage, table_v, grad_v, sem = scratch[BANKS:]
    segs, seg_rows, dim = grad_v.shape
    n_rows = tables_ref.shape[1]
    id_stride = (ids_ref.shape[1] - BLOCK) // BANKS
    grad_copy = pltpu.make_async_copy(grad_ref.at[:, place], grad_v, sem.at[0])
    table_copy = pltpu.make_async_copy(tables_ref.at[slot], table_v, sem.at[1])
    grad_copy.start()
    table_copy.start()

    zero = jnp.zeros((BLOCK, dim), jnp.float32)

    def clear(i, carry):
        for bank in banks:
            bank[pl.ds(pl.multiple_of(i * BLOCK, BLOCK), BLOCK), :] = zero
        return carry

    lax.fori_loop(0, n_rows // BLOCK, clear, 0)
    for bank in banks:
        bank[pl.ds(n_rows, 8), :] = zero[:8]
    grad_copy.wait()

    def widen(i, carry):
        for j in range(segs):
            rows = pl.ds(pl.multiple_of(i * 32, 32), 32)
            stage[j, rows, :] = grad_v[j, rows, :].astype(jnp.float32)
        return carry

    lax.fori_loop(0, seg_rows // 32, widen, 0)

    def add_rows(i, carry):
        base = i * UNROLL
        for u in range(UNROLL):
            for j, bank in enumerate(banks):
                pair = ids_ref[0, j * id_stride + u + base]
                first, second = pair & 0xFFFF, pair >> 16
                same = jnp.full((1, dim), first) == jnp.full((1, dim), second)
                add_first = stage[2 * j, pl.ds(base + u, 1), :]
                add_second = stage[2 * j + 1, pl.ds(base + u, 1), :]
                add_second = jnp.where(same, add_first + add_second, add_second)
                old_first = bank[pl.ds(first, 1), :]
                old_second = bank[pl.ds(second, 1), :]
                bank[pl.ds(first, 1), :] = old_first + add_first
                bank[pl.ds(second, 1), :] = old_second + add_second
        return carry

    lax.fori_loop(0, (ids_ref[0, BANKS * id_stride] + UNROLL - 1) // UNROLL, add_rows, 0)

    table_copy.wait()
    out_accums_ref[...] = (carried_refs[1] if n_carried else accums_ref)[...]
    eye = lax.broadcasted_iota(jnp.int32, (BLOCK, dim), 0) == lax.broadcasted_iota(jnp.int32, (BLOCK, dim), 1)
    lr = lr_ref[0]

    def update(c, carry):
        for s in range(CHUNK // BLOCK):
            i = c * (CHUNK // BLOCK) + s
            rows = pl.ds(pl.multiple_of(i * BLOCK, BLOCK), BLOCK)
            cols = pl.ds(pl.multiple_of(i * BLOCK, BLOCK), BLOCK)
            grad = banks[0][rows, :]
            for bank in banks[1:]:
                grad = grad + bank[rows, :]
            old = jnp.where(eye, accums_ref[slot:slot + 1, cols], 0.0)
            new = jnp.sum(grad * grad * (1.0 / dim) + old, axis=1, keepdims=True)
            out_accums_ref[slot:slot + 1, cols] = jnp.sum(jnp.where(eye, new, 0.0), axis=0, keepdims=True)
            root = lax.rsqrt(jnp.maximum(new, TINY))
            scale = lr * root / (1.0 + EPSILON * root)
            table_v[rows, :] = (table_v[rows, :].astype(jnp.float32) - grad * scale).astype(jnp.bfloat16)
        done = pl.ds(pl.multiple_of(c * CHUNK, CHUNK), CHUNK)
        pltpu.make_async_copy(table_v.at[done], out_tables_ref.at[slot, done], sem.at[0]).start()
        return carry

    lax.fori_loop(0, n_rows // CHUNK, update, 0)
    pltpu.make_async_copy(table_v, out_tables_ref.at[slot], sem.at[0]).wait()


def apply_slot(slot, place, ids, lr, grad, tables, accums, carried):
    _, n_rows, dim = tables.shape
    segs, _, seg_rows, _ = grad.shape
    return pl.pallas_call(
        functools.partial(apply_kernel, slot, place, len(carried)),
        out_shape=tuple(jax.ShapeDtypeStruct(x.shape, x.dtype) for x in (tables, accums)),
        in_specs=[pl.BlockSpec(memory_space=pltpu.SMEM)] * 2
        + [pl.BlockSpec(memory_space=pl.ANY)] * 2
        + [pl.BlockSpec(memory_space=pltpu.VMEM)]
        + [pl.BlockSpec(memory_space=pl.ANY), pl.BlockSpec(memory_space=pltpu.VMEM)][:len(carried)],
        out_specs=(pl.BlockSpec(memory_space=pl.ANY), pl.BlockSpec(memory_space=pltpu.VMEM)),
        input_output_aliases={5: 0} if carried else {},
        scratch_shapes=[pltpu.VMEM((n_rows + 8, dim), jnp.float32)] * BANKS + [
            pltpu.VMEM((segs, seg_rows, dim), jnp.float32),
            pltpu.VMEM((n_rows, dim), tables.dtype),
            pltpu.VMEM((segs, seg_rows, dim), grad.dtype),
            pltpu.SemaphoreType.DMA((2,)),
        ],
        compiler_params=pltpu.CompilerParams(vmem_limit_bytes=VMEM_LIMIT),
        cost_estimate=pl.CostEstimate(flops=n_rows * dim * 400, bytes_accessed=4 * n_rows * dim * 2, transcendentals=0),
    )(ids, lr, grad, tables, accums, *carried)


def solution(mesh):
    n_group = mesh.shape['mp']
    slot_spec = P(('pod', 'mp'))

    def local_step(d_pool, row_ids, lengths, tables, row_accum, learn_rate):
        n_slots, n_rows, _ = tables.shape
        by_table = jnp.transpose(d_pool, (1, 0, 2))
        part = by_table.shape[1]
        plan_out, *ids = make_plan(row_ids[:, :, 0], lengths, n_group, n_rows)
        plan, starts, most = share_plan(plan_out)
        most = most[0]
        lr = learn_rate.reshape(1)
        caps = tuple(c for c in CAPS(part))

        def exchange(level):
            def run(operands):
                by_table, plan, starts, ids, lr, tables, accums = operands
                got = []
                for c, slots in enumerate(CHUNKS(n_slots)):
                    pack = pack_slots(slots, caps[level], starts, plan, by_table)
                    swapped = lax.all_to_all(pack, 'mp', 0, 0, tiled=True)
                    got += [(k, i, c, swapped) for i, k in enumerate(slots)]
                carried = ()
                for k, i, c, swapped in got:
                    carried = apply_slot(k, i, ids[k], lr, swapped, tables, accums, carried)
                return tuple(carried)

            return run

        level = sum((most > cap).astype(jnp.int32) for cap in caps[:-1])
        operands = (by_table, plan, starts, tuple(ids), lr, tables, row_accum)
        return lax.switch(level, [exchange(i) for i in range(len(caps))], operands)

    return jax.shard_map(local_step, mesh=mesh, in_specs=(slot_spec, slot_spec, slot_spec, slot_spec, slot_spec, P()), out_specs=(slot_spec, slot_spec), check_vma=False)


def CAPS(part):
    return (part * 9 // 16, part)


def CHUNKS(n_slots):
    return (0,), tuple(range(1, n_slots - 1)), (n_slots - 1,)
```

```python
import functools

import jax
import jax.numpy as jnp
from jax import lax
from jax.experimental import pallas as pl
from jax.experimental.pallas import tpu as pltpu
from jax.sharding import PartitionSpec as P


EPSILON = 1e-06
TINY = 1e-36
BANKS = 4
UNROLL = 8
BLOCK = 128
CHUNK = 1024
MAX_LANE = 64
VMEM_LIMIT = 66000000


def gather_parts(src_ref, dst, n_dev):
    n_slots, batch = src_ref.shape
    part = batch // n_dev
    for d in range(n_dev):
        dst[d * n_slots:(d + 1) * n_slots, :] = src_ref[:, d * part:(d + 1) * part]


def block_prefix(len_v, b, prefix):
    valid = len_v[:, b * BLOCK:(b + 1) * BLOCK] > 0
    ones = jnp.where(valid, 1.0, 0.0)
    local = jnp.dot(ones.astype(jnp.bfloat16), prefix, preferred_element_type=jnp.float32).astype(jnp.int32)
    return valid, local, jnp.sum(ones, axis=1, keepdims=True).astype(jnp.int32)


def prefix_matrix():
    below = lax.broadcasted_iota(jnp.int32, (BLOCK, BLOCK), 0) < lax.broadcasted_iota(jnp.int32, (BLOCK, BLOCK), 1)
    return jnp.where(below, 1.0, 0.0).astype(jnp.bfloat16)


def plan_kernel(lengths_ref, plan_ref, len_v):
    n_dev, n_slots, width = plan_ref.shape
    part, rows = width - BLOCK, n_dev * n_slots
    gather_parts(lengths_ref, len_v, n_dev)
    prefix = prefix_matrix()
    lane = lax.broadcasted_iota(jnp.int32, (rows, BLOCK), 1)
    count = jnp.zeros((rows, 1), jnp.int32)
    starts = jnp.zeros((rows, BLOCK), jnp.int32)
    for b in range(part // BLOCK):
        valid, local, more = block_prefix(len_v, b, prefix)
        place = jnp.where(valid, local, -1)
        for d in range(n_dev):
            plan_ref[d, :, b * BLOCK:(b + 1) * BLOCK] = place[d * n_slots:(d + 1) * n_slots, :]
        starts = jnp.where(lane == b, count, starts)
        count = count + more
    starts = jnp.where(lane == MAX_LANE, jnp.max(count, axis=0, keepdims=True), starts)
    for d in range(n_dev):
        plan_ref[d, :, part:] = starts[d * n_slots:(d + 1) * n_slots, :]


def make_plan(lengths, n_dev):
    n_slots, batch = lengths.shape
    part = batch // n_dev
    return pl.pallas_call(
        plan_kernel,
        out_shape=jax.ShapeDtypeStruct((n_dev, n_slots, part + BLOCK), jnp.int32),
        in_specs=[pl.BlockSpec(memory_space=pltpu.VMEM)],
        out_specs=pl.BlockSpec(memory_space=pltpu.VMEM),
        scratch_shapes=[pltpu.VMEM((n_dev * n_slots, part), jnp.int32)],
        compiler_params=pltpu.CompilerParams(vmem_limit_bytes=16000000),
        cost_estimate=pl.CostEstimate(flops=10000000, bytes_accessed=1000000, transcendentals=0),
    )(lengths)


def ids_kernel(n_dev, n_rows, ids_ref, lengths_ref, *refs):
    *packed_refs, ids_v, len_v = refs
    n_slots, batch = ids_ref.shape
    part, rows = batch // n_dev, n_dev * n_slots
    gather_parts(ids_ref, ids_v, n_dev)
    gather_parts(lengths_ref, len_v, n_dev)
    prefix = prefix_matrix()
    lane = lax.broadcasted_iota(jnp.int32, (rows, BLOCK), 1)
    count = jnp.zeros((rows, 1), jnp.int32)
    moves = []
    for b in range(part // BLOCK):
        valid, local, more = block_prefix(len_v, b, prefix)
        shift = (b * BLOCK + lane) - (count + local)
        moves.append(jnp.where(valid, (shift << 16) | ids_v[:, b * BLOCK:(b + 1) * BLOCK], n_rows))
        count = count + more
    move = jnp.concatenate(moves, axis=1)
    step = 1
    while step < part:
        come = pltpu.roll(move, part - step, 1)
        bit = step << 16
        stay = jnp.where((move & bit) != 0, n_rows, move)
        move = jnp.where((come & bit) != 0, come, stay)
        step *= 2
    spot = lax.broadcasted_iota(jnp.int32, (rows, part), 1)
    packed = jnp.where(spot < count, move & 0xFFFF, n_rows)
    most = jnp.max(count, axis=0, keepdims=True)
    for s in range(n_slots):
        for j in range(n_dev // 2):
            low, high = ((2 * j + h) * n_slots + s for h in range(2))
            packed_refs[s][:, j * part:(j + 1) * part] = packed[low:low + 1, :] | (packed[high:high + 1, :] << 16)
        packed_refs[s][:, n_dev // 2 * part:] = jnp.broadcast_to(most, (1, BLOCK))


def pack_ids(ids, lengths, n_dev, n_rows):
    n_slots, batch = ids.shape
    part = batch // n_dev
    assert n_rows < 1 << 15 and part <= 1 << 15
    return pl.pallas_call(
        functools.partial(ids_kernel, n_dev, n_rows),
        out_shape=(jax.ShapeDtypeStruct((1, batch // 2 + BLOCK), jnp.int32),) * n_slots,
        in_specs=[pl.BlockSpec(memory_space=pltpu.VMEM)] * 2,
        out_specs=(pl.BlockSpec(memory_space=pltpu.VMEM),) * n_slots,
        scratch_shapes=[pltpu.VMEM((n_dev * n_slots, part), jnp.int32)] * 2,
        compiler_params=pltpu.CompilerParams(vmem_limit_bytes=32000000),
        cost_estimate=pl.CostEstimate(flops=20000000, bytes_accessed=2000000, transcendentals=0),
    )(ids, lengths)


def share_kernel(n_dev, plan_ref, plans_ref, starts_ref, most_ref, send_sem, recv_sem, own_sem):
    pod, me = lax.axis_index('pod'), lax.axis_index('mp')
    barrier = pltpu.get_barrier_semaphore()
    for o in range(1, n_dev):
        pl.semaphore_signal(barrier, inc=1, device_id=(pod, (me + o) % n_dev), device_id_type=pl.DeviceIdType.MESH)
    pl.semaphore_wait(barrier, n_dev - 1)
    copies = [
        pltpu.make_async_remote_copy(
            src_ref=plan_ref.at[(me + o) % n_dev],
            dst_ref=plans_ref.at[me],
            send_sem=send_sem.at[o],
            recv_sem=recv_sem.at[o],
            device_id=(pod, (me + o) % n_dev),
            device_id_type=pl.DeviceIdType.MESH,
        )
        for o in range(1, n_dev)
    ]
    for copy in copies:
        copy.start()
    own = pltpu.make_async_copy(plan_ref.at[me], plans_ref.at[me], own_sem)
    own.start()
    own.wait()
    for copy in copies:
        copy.wait()
    part = plans_ref.shape[2] - BLOCK
    starts = plans_ref[:, :, part:]
    starts_ref[...] = starts
    most_ref[0] = jnp.max(starts[:, :, MAX_LANE:MAX_LANE + 1])


def share_plan(plan):
    n_dev, n_slots, _ = plan.shape
    return pl.pallas_call(
        functools.partial(share_kernel, n_dev),
        out_shape=(
            jax.ShapeDtypeStruct(plan.shape, plan.dtype),
            jax.ShapeDtypeStruct((n_dev, n_slots, BLOCK), plan.dtype),
            jax.ShapeDtypeStruct((1,), plan.dtype),
        ),
        in_specs=[pl.BlockSpec(memory_space=pltpu.VMEM)],
        out_specs=(pl.BlockSpec(memory_space=pltpu.VMEM), pl.BlockSpec(memory_space=pltpu.VMEM), pl.BlockSpec(memory_space=pltpu.SMEM)),
        scratch_shapes=[pltpu.SemaphoreType.DMA((n_dev,)), pltpu.SemaphoreType.DMA((n_dev,)), pltpu.SemaphoreType.DMA],
        compiler_params=pltpu.CompilerParams(collective_id=0, has_side_effects=True, vmem_limit_bytes=16000000),
        cost_estimate=pl.CostEstimate(flops=20000000, bytes_accessed=2000000, transcendentals=0),
    )(plan)


def pack_kernel(slots, starts_ref, plan_ref, tables_ref, out_ref, grad_v, stage, pack_v, in_sem, out_sem):
    n_slots = plan_ref.shape[1]
    cap = out_ref.shape[2]
    n_tab, part, _ = tables_ref.shape
    slot_row = lax.broadcasted_iota(jnp.int32, (BLOCK, BLOCK), 0)
    used = [[d for d in range(out_ref.shape[0]) if d * n_slots + slot < n_tab] for slot in slots]

    def fetch(i, d):
        return pltpu.make_async_copy(tables_ref.at[d * n_slots + slots[i]], grad_v.at[i, d], in_sem.at[i, d])

    def emit(i, d):
        return pltpu.make_async_copy(pack_v.at[i, d], out_ref.at[d, i], out_sem.at[i, d])

    for i, dests in enumerate(used):
        for d in dests:
            fetch(i, d).start()
    for i, dests in enumerate(used):
        def table(d, carry):
            fetch(i, d).wait()
            for b in range(part // BLOCK):
                place = plan_ref[d, slots[i]:slots[i] + 1, b * BLOCK:(b + 1) * BLOCK]
                pick = jnp.where(slot_row == place, 1.0, 0.0).astype(jnp.bfloat16)
                rows = jnp.dot(pick, grad_v[i, d, b * BLOCK:(b + 1) * BLOCK, :], preferred_element_type=jnp.float32)
                stage[pl.ds(starts_ref[d, slots[i], b], BLOCK), :] = rows
            pack_v[i, d] = stage[:cap, :].astype(jnp.bfloat16)
            emit(i, d).start()
            return carry

        lax.fori_loop(0, len(dests), table, 0)
    for i, dests in enumerate(used):
        for d in dests:
            emit(i, d).wait()


def pack_slots(slots, cap, starts, plan, by_table):
    n_dev = plan.shape[0]
    _, part, dim = by_table.shape
    n = len(slots)
    return pl.pallas_call(
        functools.partial(pack_kernel, slots),
        out_shape=jax.ShapeDtypeStruct((n_dev, n, cap, dim), by_table.dtype),
        in_specs=[pl.BlockSpec(memory_space=pltpu.SMEM), pl.BlockSpec(memory_space=pltpu.VMEM), pl.BlockSpec(memory_space=pl.ANY)],
        out_specs=pl.BlockSpec(memory_space=pl.ANY),
        scratch_shapes=[
            pltpu.VMEM((n, n_dev, part, dim), by_table.dtype),
            pltpu.VMEM((cap + BLOCK, dim), jnp.float32),
            pltpu.VMEM((n, n_dev, cap, dim), by_table.dtype),
            pltpu.SemaphoreType.DMA((n, n_dev)),
            pltpu.SemaphoreType.DMA((n, n_dev)),
        ],
        compiler_params=pltpu.CompilerParams(vmem_limit_bytes=VMEM_LIMIT),
        cost_estimate=pl.CostEstimate(flops=n * n_dev * part * dim * 20, bytes_accessed=n * n_dev * part * dim * 3, transcendentals=0),
    )(starts, plan, by_table)


def apply_kernel(slots, n_carried, lr_ref, grad_ref, tables_ref, accums_ref, *refs):
    n = len(slots)
    ids_refs, carried_refs = refs[:n], refs[n:n + n_carried]
    out_tables_ref, out_accums_ref, *scratch = refs[n + n_carried:]
    ids_s, banks, (stage, table_v, grad_v, sem, out_sem) = scratch[:n], scratch[n:n + BANKS], scratch[n + BANKS:]
    _, segs, seg_rows, dim = grad_v.shape
    n_rows = tables_ref.shape[1]
    id_stride = (ids_refs[0].shape[1] - BLOCK) // BANKS
    copies = [
        (
            pltpu.make_async_copy(grad_ref.at[:, i], grad_v.at[i], sem.at[i, 0]),
            pltpu.make_async_copy(ids_refs[i], ids_s[i], sem.at[i, 1]),
            pltpu.make_async_copy(tables_ref.at[slot], table_v.at[i], sem.at[i, 2]),
        )
        for i, slot in enumerate(slots)
    ]
    for grad_copy, ids_copy, table_copy in copies:
        ids_copy.start()
        grad_copy.start()
        table_copy.start()

    zero = jnp.zeros((BLOCK, dim), jnp.float32)

    def clear(i, carry):
        for bank in banks:
            bank[pl.ds(pl.multiple_of(i * BLOCK, BLOCK), BLOCK), :] = zero
        return carry

    lax.fori_loop(0, n_rows // BLOCK, clear, 0)
    for bank in banks:
        bank[pl.ds(n_rows, 8), :] = zero[:8]
    out_accums_ref[...] = (carried_refs[1] if n_carried else accums_ref)[...]
    eye = lax.broadcasted_iota(jnp.int32, (BLOCK, dim), 0) == lax.broadcasted_iota(jnp.int32, (BLOCK, dim), 1)
    lr = lr_ref[0]

    for i, slot in enumerate(slots):
        grad_copy, ids_copy, table_copy = copies[i]
        ids_copy.wait()
        grad_copy.wait()

        def widen(t, carry):
            for j in range(segs):
                rows = pl.ds(pl.multiple_of(t * 32, 32), 32)
                stage[j, rows, :] = grad_v[i, j, rows, :].astype(jnp.float32)
            return carry

        lax.fori_loop(0, seg_rows // 32, widen, 0)

        def add_rows(t, carry):
            base = t * UNROLL
            for u in range(UNROLL):
                for j, bank in enumerate(banks):
                    pair = ids_s[i][0, j * id_stride + u + base]
                    first, second = pair & 0xFFFF, pair >> 16
                    same = jnp.full((1, dim), first) == jnp.full((1, dim), second)
                    add_first = stage[2 * j, pl.ds(base + u, 1), :]
                    add_second = stage[2 * j + 1, pl.ds(base + u, 1), :]
                    add_second = jnp.where(same, add_first + add_second, add_second)
                    old_first = bank[pl.ds(first, 1), :]
                    old_second = bank[pl.ds(second, 1), :]
                    bank[pl.ds(first, 1), :] = old_first + add_first
                    bank[pl.ds(second, 1), :] = old_second + add_second
            return carry

        lax.fori_loop(0, (ids_s[i][0, BANKS * id_stride] + UNROLL - 1) // UNROLL, add_rows, 0)
        table_copy.wait()

        def update(c, carry):
            for s in range(CHUNK // BLOCK):
                first_row = pl.multiple_of((c * (CHUNK // BLOCK) + s) * BLOCK, BLOCK)
                rows = pl.ds(first_row, BLOCK)
                grad = banks[0][rows, :]
                for bank in banks[1:]:
                    grad = grad + bank[rows, :]
                if i + 1 < n:
                    for bank in banks:
                        bank[rows, :] = zero
                old = jnp.where(eye, accums_ref[slot:slot + 1, rows], 0.0)
                new = jnp.sum(grad * grad * (1.0 / dim) + old, axis=1, keepdims=True)
                out_accums_ref[slot:slot + 1, rows] = jnp.sum(jnp.where(eye, new, 0.0), axis=0, keepdims=True)
                root = lax.rsqrt(jnp.maximum(new, TINY))
                scale = lr * root / (1.0 + EPSILON * root)
                table_v[i, rows, :] = (table_v[i, rows, :].astype(jnp.float32) - grad * scale).astype(jnp.bfloat16)
            done = pl.ds(pl.multiple_of(c * CHUNK, CHUNK), CHUNK)
            pltpu.make_async_copy(table_v.at[i, done], out_tables_ref.at[slot, done], out_sem.at[i]).start()
            return carry

        lax.fori_loop(0, n_rows // CHUNK, update, 0)
    for i, slot in enumerate(slots):
        pltpu.make_async_copy(table_v.at[i], out_tables_ref.at[slot], out_sem.at[i]).wait()


def apply_slots(slots, ids, lr, grad, tables, accums, carried):
    _, n_rows, dim = tables.shape
    segs, n, seg_rows, _ = grad.shape
    assert segs == 2 * BANKS
    return pl.pallas_call(
        functools.partial(apply_kernel, slots, len(carried)),
        out_shape=tuple(jax.ShapeDtypeStruct(x.shape, x.dtype) for x in (tables, accums)),
        in_specs=[pl.BlockSpec(memory_space=pltpu.SMEM)]
        + [pl.BlockSpec(memory_space=pl.ANY)] * 2
        + [pl.BlockSpec(memory_space=pltpu.VMEM)]
        + [pl.BlockSpec(memory_space=pl.ANY)] * n
        + [pl.BlockSpec(memory_space=pl.ANY), pl.BlockSpec(memory_space=pltpu.VMEM)][:len(carried)],
        out_specs=(pl.BlockSpec(memory_space=pl.ANY), pl.BlockSpec(memory_space=pltpu.VMEM)),
        input_output_aliases={4 + n: 0} if carried else {},
        scratch_shapes=[pltpu.SMEM(ids[0].shape, jnp.int32)] * n
        + [pltpu.VMEM((n_rows + 8, dim), jnp.float32)] * BANKS
        + [
            pltpu.VMEM((segs, seg_rows, dim), jnp.float32),
            pltpu.VMEM((n, n_rows, dim), tables.dtype),
            pltpu.VMEM((n, segs, seg_rows, dim), grad.dtype),
            pltpu.SemaphoreType.DMA((n, 3)),
            pltpu.SemaphoreType.DMA((n,)),
        ],
        compiler_params=pltpu.CompilerParams(vmem_limit_bytes=VMEM_LIMIT),
        cost_estimate=pl.CostEstimate(flops=n * n_rows * dim * 400, bytes_accessed=4 * n * n_rows * dim * 2, transcendentals=0),
    )(lr, grad, tables, accums, *(ids[k] for k in slots), *carried)


def solution(mesh):
    n_group = mesh.shape['mp']
    slot_spec = P(('pod', 'mp'))

    def local_step(d_pool, row_ids, lengths, tables, row_accum, learn_rate):
        n_slots, n_rows, _ = tables.shape
        by_table = jnp.transpose(d_pool, (1, 0, 2))
        part = by_table.shape[1]
        plan_out = make_plan(lengths, n_group)
        plan, starts, most = share_plan(plan_out)
        most = most[0]
        lr = learn_rate.reshape(1)
        caps = CAPS(part)

        def exchange(level):
            def run(operands):
                by_table, plan, starts, row_ids, lengths, lr, tables, accums = operands
                got = []
                for slots in CHUNKS(n_slots):
                    pack = pack_slots(slots, caps[level], starts, plan, by_table)
                    got.append(lax.all_to_all(pack, 'mp', 0, 0, tiled=True))
                ids = pack_ids(row_ids[:, :, 0], lengths, n_group, n_rows)
                carried = ()
                for c, slots in enumerate(CHUNKS(n_slots)):
                    carried = apply_slots(slots, ids, lr, got[c], tables, accums, carried)
                return tuple(carried)

            return run

        level = sum((most > cap).astype(jnp.int32) for cap in caps[:-1])
        operands = (by_table, plan, starts, row_ids, lengths, lr, tables, row_accum)
        return lax.switch(level, [exchange(i) for i in range(len(caps))], operands)

    return jax.shard_map(local_step, mesh=mesh, in_specs=(slot_spec, slot_spec, slot_spec, slot_spec, slot_spec, P()), out_specs=(slot_spec, slot_spec), check_vma=False)


def CAPS(part):
    return part * 35 // 64, part * 39 // 64, part


def CHUNKS(n_slots):
    return (0,), tuple(range(1, n_slots - 1)), (n_slots - 1,)
```

```python
import functools

import jax
import jax.numpy as jnp
from jax import lax
from jax.experimental import pallas as pl
from jax.experimental.pallas import tpu as pltpu
from jax.sharding import PartitionSpec as P


EPSILON = 1e-06
TINY = 1e-36
BANKS = 4
UNROLL = 16
BLOCK = 128
CHUNK = 1024
MAX_LANE = 64
VMEM_LIMIT = 66000000


def gather_parts(src_ref, dst, n_dev):
    n_slots, batch = src_ref.shape
    part = batch // n_dev
    for d in range(n_dev):
        dst[d * n_slots:(d + 1) * n_slots, :] = src_ref[:, d * part:(d + 1) * part]


def block_prefix(len_v, b, prefix):
    valid = len_v[:, b * BLOCK:(b + 1) * BLOCK] > 0
    ones = jnp.where(valid, 1.0, 0.0)
    local = jnp.dot(ones.astype(jnp.bfloat16), prefix, preferred_element_type=jnp.float32).astype(jnp.int32)
    return valid, local, jnp.sum(ones, axis=1, keepdims=True).astype(jnp.int32)


def prefix_matrix():
    below = lax.broadcasted_iota(jnp.int32, (BLOCK, BLOCK), 0) < lax.broadcasted_iota(jnp.int32, (BLOCK, BLOCK), 1)
    return jnp.where(below, 1.0, 0.0).astype(jnp.bfloat16)


def plan_kernel(lengths_ref, plan_ref, len_v):
    n_dev, n_slots, width = plan_ref.shape
    part, rows = width - BLOCK, n_dev * n_slots
    gather_parts(lengths_ref, len_v, n_dev)
    prefix = prefix_matrix()
    lane = lax.broadcasted_iota(jnp.int32, (rows, BLOCK), 1)
    count = jnp.zeros((rows, 1), jnp.int32)
    starts = jnp.zeros((rows, BLOCK), jnp.int32)
    for b in range(part // BLOCK):
        valid, local, more = block_prefix(len_v, b, prefix)
        place = jnp.where(valid, local, -1)
        for d in range(n_dev):
            plan_ref[d, :, b * BLOCK:(b + 1) * BLOCK] = place[d * n_slots:(d + 1) * n_slots, :]
        starts = jnp.where(lane == b, count, starts)
        count = count + more
    starts = jnp.where(lane == MAX_LANE, jnp.max(count, axis=0, keepdims=True), starts)
    for d in range(n_dev):
        plan_ref[d, :, part:] = starts[d * n_slots:(d + 1) * n_slots, :]


def make_plan(lengths, n_dev):
    n_slots, batch = lengths.shape
    part = batch // n_dev
    return pl.pallas_call(
        plan_kernel,
        out_shape=jax.ShapeDtypeStruct((n_dev, n_slots, part + BLOCK), jnp.int32),
        in_specs=[pl.BlockSpec(memory_space=pltpu.VMEM)],
        out_specs=pl.BlockSpec(memory_space=pltpu.VMEM),
        scratch_shapes=[pltpu.VMEM((n_dev * n_slots, part), jnp.int32)],
        compiler_params=pltpu.CompilerParams(vmem_limit_bytes=16000000),
        cost_estimate=pl.CostEstimate(flops=10000000, bytes_accessed=1000000, transcendentals=0),
    )(lengths)


def ids_kernel(n_dev, n_rows, ids_ref, lengths_ref, *refs):
    *packed_refs, ids_v, len_v = refs
    n_slots, batch = ids_ref.shape
    part, rows = batch // n_dev, n_dev * n_slots
    gather_parts(ids_ref, ids_v, n_dev)
    gather_parts(lengths_ref, len_v, n_dev)
    prefix = prefix_matrix()
    lane = lax.broadcasted_iota(jnp.int32, (rows, BLOCK), 1)
    count = jnp.zeros((rows, 1), jnp.int32)
    moves = []
    for b in range(part // BLOCK):
        valid, local, more = block_prefix(len_v, b, prefix)
        shift = (b * BLOCK + lane) - (count + local)
        moves.append(jnp.where(valid, (shift << 16) | ids_v[:, b * BLOCK:(b + 1) * BLOCK], n_rows))
        count = count + more
    move = jnp.concatenate(moves, axis=1)
    step = 1
    while step < part:
        come = pltpu.roll(move, part - step, 1)
        bit = step << 16
        stay = jnp.where((move & bit) != 0, n_rows, move)
        move = jnp.where((come & bit) != 0, come, stay)
        step *= 2
    spot = lax.broadcasted_iota(jnp.int32, (rows, part), 1)
    packed = jnp.where(spot < count, move & 0xFFFF, n_rows)
    most = jnp.max(count, axis=0, keepdims=True)
    for s in range(n_slots):
        for d in range(n_dev):
            packed_refs[s][:, d * part:(d + 1) * part] = packed[d * n_slots + s:d * n_slots + s + 1, :]
        packed_refs[s][:, n_dev * part:] = jnp.broadcast_to(most, (1, BLOCK))


def pack_ids(ids, lengths, n_dev, n_rows):
    n_slots, batch = ids.shape
    part = batch // n_dev
    assert n_rows < 1 << 15 and part <= 1 << 15
    return pl.pallas_call(
        functools.partial(ids_kernel, n_dev, n_rows),
        out_shape=(jax.ShapeDtypeStruct((1, batch + BLOCK), jnp.int32),) * n_slots,
        in_specs=[pl.BlockSpec(memory_space=pltpu.VMEM)] * 2,
        out_specs=(pl.BlockSpec(memory_space=pltpu.VMEM),) * n_slots,
        scratch_shapes=[pltpu.VMEM((n_dev * n_slots, part), jnp.int32)] * 2,
        compiler_params=pltpu.CompilerParams(vmem_limit_bytes=32000000),
        cost_estimate=pl.CostEstimate(flops=20000000, bytes_accessed=2000000, transcendentals=0),
    )(ids, lengths)


def share_kernel(n_dev, plan_ref, plans_ref, starts_ref, most_ref, send_sem, recv_sem, own_sem):
    pod, me = lax.axis_index('pod'), lax.axis_index('mp')
    barrier = pltpu.get_barrier_semaphore()
    for o in range(1, n_dev):
        pl.semaphore_signal(barrier, inc=1, device_id=(pod, (me + o) % n_dev), device_id_type=pl.DeviceIdType.MESH)
    pl.semaphore_wait(barrier, n_dev - 1)
    copies = [
        pltpu.make_async_remote_copy(
            src_ref=plan_ref.at[(me + o) % n_dev],
            dst_ref=plans_ref.at[me],
            send_sem=send_sem.at[o],
            recv_sem=recv_sem.at[o],
            device_id=(pod, (me + o) % n_dev),
            device_id_type=pl.DeviceIdType.MESH,
        )
        for o in range(1, n_dev)
    ]
    for copy in copies:
        copy.start()
    own = pltpu.make_async_copy(plan_ref.at[me], plans_ref.at[me], own_sem)
    own.start()
    own.wait()
    for copy in copies:
        copy.wait()
    part = plans_ref.shape[2] - BLOCK
    starts = plans_ref[:, :, part:]
    starts_ref[...] = starts
    most_ref[0] = jnp.max(starts[:, :, MAX_LANE:MAX_LANE + 1])


def share_plan(plan):
    n_dev, n_slots, _ = plan.shape
    return pl.pallas_call(
        functools.partial(share_kernel, n_dev),
        out_shape=(
            jax.ShapeDtypeStruct(plan.shape, plan.dtype),
            jax.ShapeDtypeStruct((n_dev, n_slots, BLOCK), plan.dtype),
            jax.ShapeDtypeStruct((1,), plan.dtype),
        ),
        in_specs=[pl.BlockSpec(memory_space=pltpu.VMEM)],
        out_specs=(pl.BlockSpec(memory_space=pltpu.VMEM), pl.BlockSpec(memory_space=pltpu.VMEM), pl.BlockSpec(memory_space=pltpu.SMEM)),
        scratch_shapes=[pltpu.SemaphoreType.DMA((n_dev,)), pltpu.SemaphoreType.DMA((n_dev,)), pltpu.SemaphoreType.DMA],
        compiler_params=pltpu.CompilerParams(collective_id=0, has_side_effects=True, vmem_limit_bytes=16000000),
        cost_estimate=pl.CostEstimate(flops=20000000, bytes_accessed=2000000, transcendentals=0),
    )(plan)


def pack_kernel(slots, starts_ref, plan_ref, tables_ref, out_ref, grad_v, stage, pack_v, in_sem, out_sem):
    n_slots = plan_ref.shape[1]
    cap = out_ref.shape[2]
    n_tab, part, _ = tables_ref.shape
    slot_row = lax.broadcasted_iota(jnp.int32, (BLOCK, BLOCK), 0)
    used = [[d for d in range(out_ref.shape[0]) if d * n_slots + slot < n_tab] for slot in slots]

    def fetch(i, d):
        return pltpu.make_async_copy(tables_ref.at[d * n_slots + slots[i]], grad_v.at[i, d], in_sem.at[i, d])

    def emit(i, d):
        return pltpu.make_async_copy(pack_v.at[i, d], out_ref.at[d, i], out_sem.at[i, d])

    for i, dests in enumerate(used):
        for d in dests:
            fetch(i, d).start()
    for i, dests in enumerate(used):
        def table(d, carry):
            fetch(i, d).wait()
            for b in range(part // BLOCK):
                place = plan_ref[d, slots[i]:slots[i] + 1, b * BLOCK:(b + 1) * BLOCK]
                pick = jnp.where(slot_row == place, 1.0, 0.0).astype(jnp.bfloat16)
                rows = jnp.dot(pick, grad_v[i, d, b * BLOCK:(b + 1) * BLOCK, :], preferred_element_type=jnp.float32)
                stage[pl.ds(starts_ref[d, slots[i], b], BLOCK), :] = rows
            pack_v[i, d] = stage[:cap, :].astype(jnp.bfloat16)
            emit(i, d).start()
            return carry

        lax.fori_loop(0, len(dests), table, 0)
    for i, dests in enumerate(used):
        for d in dests:
            emit(i, d).wait()


def pack_slots(slots, cap, starts, plan, by_table):
    n_dev = plan.shape[0]
    _, part, dim = by_table.shape
    n = len(slots)
    return pl.pallas_call(
        functools.partial(pack_kernel, slots),
        out_shape=jax.ShapeDtypeStruct((n_dev, n, cap, dim), by_table.dtype),
        in_specs=[pl.BlockSpec(memory_space=pltpu.SMEM), pl.BlockSpec(memory_space=pltpu.VMEM), pl.BlockSpec(memory_space=pl.ANY)],
        out_specs=pl.BlockSpec(memory_space=pl.ANY),
        scratch_shapes=[
            pltpu.VMEM((n, n_dev, part, dim), by_table.dtype),
            pltpu.VMEM((cap + BLOCK, dim), jnp.float32),
            pltpu.VMEM((n, n_dev, cap, dim), by_table.dtype),
            pltpu.SemaphoreType.DMA((n, n_dev)),
            pltpu.SemaphoreType.DMA((n, n_dev)),
        ],
        compiler_params=pltpu.CompilerParams(vmem_limit_bytes=VMEM_LIMIT),
        cost_estimate=pl.CostEstimate(flops=n * n_dev * part * dim * 20, bytes_accessed=n * n_dev * part * dim * 3, transcendentals=0),
    )(starts, plan, by_table)


def apply_kernel(slots, n_carried, lr_ref, grad_ref, tables_ref, accums_ref, *refs):
    n = len(slots)
    ids_refs, carried_refs = refs[:n], refs[n:n + n_carried]
    out_tables_ref, out_accums_ref, *scratch = refs[n + n_carried:]
    banks, (stage, table_v, grad_v, done_v, sem, out_sem, ids_sem), scalars = scratch[:BANKS], scratch[BANKS:BANKS + 7], scratch[BANKS + 7:]
    _, segs, seg_rows, dim = grad_v.shape
    part = (ids_refs[0].shape[1] - BLOCK) // segs
    ids_s = [scalars[i * (segs + 1):(i + 1) * (segs + 1)] for i in range(n)]
    n_rows = tables_ref.shape[1]
    copies = [
        (
            pltpu.make_async_copy(grad_ref.at[:, i], grad_v.at[i], sem.at[i, 0]),
            [pltpu.make_async_copy(ids_refs[i].at[:, j * part:(j + 1) * part], ids_s[i][j], ids_sem.at[i, j]) for j in range(segs)]
            + [pltpu.make_async_copy(ids_refs[i].at[:, segs * part:], ids_s[i][segs], ids_sem.at[i, segs])],
            pltpu.make_async_copy(tables_ref.at[slot], table_v.at[i], sem.at[i, 2]),
        )
        for i, slot in enumerate(slots)
    ]
    for grad_copy, ids_copies, table_copy in copies:
        for copy in ids_copies:
            copy.start()
        grad_copy.start()
        table_copy.start()

    if n_carried:
        done_copy = pltpu.make_async_copy(carried_refs[1], done_v, out_sem.at[n])
        done_copy.start()
    zero = jnp.zeros((BLOCK, dim), jnp.float32)

    def clear(i, carry):
        for bank in banks:
            bank[pl.ds(pl.multiple_of(i * BLOCK, BLOCK), BLOCK), :] = zero
        return carry

    lax.fori_loop(0, n_rows // BLOCK, clear, 0)
    for bank in banks:
        bank[pl.ds(n_rows, 8), :] = zero[:8]
    eye = lax.broadcasted_iota(jnp.int32, (BLOCK, dim), 0) == lax.broadcasted_iota(jnp.int32, (BLOCK, dim), 1)
    lr = lr_ref[0]

    for i, slot in enumerate(slots):
        grad_copy, ids_copies, table_copy = copies[i]
        for copy in ids_copies:
            copy.wait()
        grad_copy.wait()

        def widen(t, carry):
            for j in range(segs):
                rows = pl.ds(pl.multiple_of(t * 32, 32), 32)
                stage[j, rows, :] = grad_v[i, j, rows, :].astype(jnp.float32)
            return carry

        lax.fori_loop(0, seg_rows // 32, widen, 0)

        def add_rows(t, carry):
            base = t * UNROLL
            for u in range(UNROLL):
                for j, bank in enumerate(banks):
                    first, second = ids_s[i][2 * j][0, base + u], ids_s[i][2 * j + 1][0, base + u]
                    same = jnp.full((1, dim), first) == jnp.full((1, dim), second)
                    add_first = stage[2 * j, pl.ds(base + u, 1), :]
                    add_second = stage[2 * j + 1, pl.ds(base + u, 1), :]
                    add_second = jnp.where(same, add_first + add_second, add_second)
                    old_first = bank[pl.ds(first, 1), :]
                    old_second = bank[pl.ds(second, 1), :]
                    bank[pl.ds(first, 1), :] = old_first + add_first
                    bank[pl.ds(second, 1), :] = old_second + add_second
            return carry

        lax.fori_loop(0, (ids_s[i][segs][0, 0] + UNROLL - 1) // UNROLL, add_rows, 0)
        table_copy.wait()
        if n_carried and i == 0:
            done_copy.wait()

        def update(c, carry):
            for s in range(CHUNK // BLOCK):
                first_row = pl.multiple_of((c * (CHUNK // BLOCK) + s) * BLOCK, BLOCK)
                rows = pl.ds(first_row, BLOCK)
                grad = banks[0][rows, :]
                for bank in banks[1:]:
                    grad = grad + bank[rows, :]
                if i + 1 < n:
                    for bank in banks:
                        bank[rows, :] = zero
                old = jnp.where(eye, accums_ref[slot:slot + 1, rows], 0.0)
                new = jnp.sum(grad * grad * (1.0 / dim) + old, axis=1, keepdims=True)
                done_v[slot:slot + 1, rows] = jnp.sum(jnp.where(eye, new, 0.0), axis=0, keepdims=True)
                root = lax.rsqrt(jnp.maximum(new, TINY))
                scale = lr * root / (1.0 + EPSILON * root)
                table_v[i, rows, :] = (table_v[i, rows, :].astype(jnp.float32) - grad * scale).astype(jnp.bfloat16)
            done = pl.ds(pl.multiple_of(c * CHUNK, CHUNK), CHUNK)
            pltpu.make_async_copy(table_v.at[i, done], out_tables_ref.at[slot, done], out_sem.at[i]).start()
            if i == n - 1:
                pltpu.make_async_copy(done_v.at[:, done], out_accums_ref.at[:, done], out_sem.at[n]).start()
            return carry

        lax.fori_loop(0, n_rows // CHUNK, update, 0)
    for i, slot in enumerate(slots):
        pltpu.make_async_copy(table_v.at[i], out_tables_ref.at[slot], out_sem.at[i]).wait()
    pltpu.make_async_copy(done_v, out_accums_ref, out_sem.at[n]).wait()


def apply_slots(slots, ids, lr, grad, tables, accums, carried):
    _, n_rows, dim = tables.shape
    segs, n, seg_rows, _ = grad.shape
    part = (ids[0].shape[1] - BLOCK) // segs
    assert segs == 2 * BANKS
    return pl.pallas_call(
        functools.partial(apply_kernel, slots, len(carried)),
        out_shape=tuple(jax.ShapeDtypeStruct(x.shape, x.dtype) for x in (tables, accums)),
        in_specs=[pl.BlockSpec(memory_space=pltpu.SMEM)]
        + [pl.BlockSpec(memory_space=pl.ANY)] * 2
        + [pl.BlockSpec(memory_space=pltpu.VMEM)]
        + [pl.BlockSpec(memory_space=pl.ANY)] * n
        + [pl.BlockSpec(memory_space=pl.ANY)] * len(carried),
        out_specs=(pl.BlockSpec(memory_space=pl.ANY),) * 2,
        input_output_aliases={4 + n: 0, 5 + n: 1} if carried else {},
        scratch_shapes=[pltpu.VMEM((n_rows + 8, dim), jnp.float32)] * BANKS
        + [
            pltpu.VMEM((segs, seg_rows, dim), jnp.float32),
            pltpu.VMEM((n, n_rows, dim), tables.dtype),
            pltpu.VMEM((n, segs, seg_rows, dim), grad.dtype),
            pltpu.VMEM(accums.shape, accums.dtype),
            pltpu.SemaphoreType.DMA((n, 3)),
            pltpu.SemaphoreType.DMA((n + 1,)),
            pltpu.SemaphoreType.DMA((n, segs + 1)),
        ]
        + ([pltpu.SMEM((1, part), jnp.int32)] * segs + [pltpu.SMEM((1, BLOCK), jnp.int32)]) * n,
        compiler_params=pltpu.CompilerParams(vmem_limit_bytes=VMEM_LIMIT),
        cost_estimate=pl.CostEstimate(flops=n * n_rows * dim * 400, bytes_accessed=4 * n * n_rows * dim * 2, transcendentals=0),
    )(lr, grad, tables, accums, *(ids[k] for k in slots), *carried)


def solution(mesh):
    n_group = mesh.shape['mp']
    slot_spec = P(('pod', 'mp'))

    def local_step(d_pool, row_ids, lengths, tables, row_accum, learn_rate):
        n_slots, n_rows, _ = tables.shape
        by_table = jnp.transpose(d_pool, (1, 0, 2))
        part = by_table.shape[1]
        plan_out = make_plan(lengths, n_group)
        plan, starts, most = share_plan(plan_out)
        most = most[0]
        lr = learn_rate.reshape(1)
        caps = CAPS(part)

        def exchange(level):
            def run(operands):
                by_table, plan, starts, row_ids, lengths, lr, tables, accums = operands
                got = []
                for slots in CHUNKS(n_slots):
                    pack = pack_slots(slots, caps[level], starts, plan, by_table)
                    got.append(lax.all_to_all(pack, 'mp', 0, 0, tiled=True))
                ids = pack_ids(row_ids[:, :, 0], lengths, n_group, n_rows)
                carried = ()
                for c, slots in enumerate(CHUNKS(n_slots)):
                    carried = apply_slots(slots, ids, lr, got[c], tables, accums, carried)
                return tuple(carried)

            return run

        level = sum((most > cap).astype(jnp.int32) for cap in caps[:-1])
        operands = (by_table, plan, starts, row_ids, lengths, lr, tables, row_accum)
        return lax.switch(level, [exchange(i) for i in range(len(caps))], operands)

    return jax.shard_map(local_step, mesh=mesh, in_specs=(slot_spec, slot_spec, slot_spec, slot_spec, slot_spec, P()), out_specs=(slot_spec, slot_spec), check_vma=False)


def CAPS(part):
    return part * 35 // 64, part * 39 // 64, part


def CHUNKS(n_slots):
    return (0,), tuple(range(1, n_slots - 1)), (n_slots - 1,)
```

```python
import functools

import jax
import jax.numpy as jnp
from jax import lax
from jax.experimental import pallas as pl
from jax.experimental.pallas import tpu as pltpu
from jax.sharding import PartitionSpec as P


EPSILON = 1e-06
TINY = 1e-36
BANKS = 4
UNROLL = 16
BLOCK = 128
CHUNK = 1024
MAX_LANE = 64
VMEM_LIMIT = 66000000


def gather_parts(src_ref, dst, n_dev):
    n_slots, batch = src_ref.shape
    part = batch // n_dev
    for d in range(n_dev):
        dst[d * n_slots:(d + 1) * n_slots, :] = src_ref[:, d * part:(d + 1) * part]


def block_prefix(len_v, b, prefix):
    valid = len_v[:, b * BLOCK:(b + 1) * BLOCK] > 0
    ones = jnp.where(valid, 1.0, 0.0)
    local = jnp.dot(ones.astype(jnp.bfloat16), prefix, preferred_element_type=jnp.float32).astype(jnp.int32)
    return valid, local, jnp.sum(ones, axis=1, keepdims=True).astype(jnp.int32)


def prefix_matrix():
    below = lax.broadcasted_iota(jnp.int32, (BLOCK, BLOCK), 0) < lax.broadcasted_iota(jnp.int32, (BLOCK, BLOCK), 1)
    return jnp.where(below, 1.0, 0.0).astype(jnp.bfloat16)


def plan_kernel(lengths_ref, plan_ref, len_v):
    n_dev, n_slots, width = plan_ref.shape
    part, rows = width - BLOCK, n_dev * n_slots
    gather_parts(lengths_ref, len_v, n_dev)
    prefix = prefix_matrix()
    lane = lax.broadcasted_iota(jnp.int32, (rows, BLOCK), 1)
    count = jnp.zeros((rows, 1), jnp.int32)
    starts = jnp.zeros((rows, BLOCK), jnp.int32)
    for b in range(part // BLOCK):
        valid, local, more = block_prefix(len_v, b, prefix)
        place = jnp.where(valid, local, -1)
        for d in range(n_dev):
            plan_ref[d, :, b * BLOCK:(b + 1) * BLOCK] = place[d * n_slots:(d + 1) * n_slots, :]
        starts = jnp.where(lane == b, count, starts)
        count = count + more
    starts = jnp.where(lane == MAX_LANE, jnp.max(count, axis=0, keepdims=True), starts)
    for d in range(n_dev):
        plan_ref[d, :, part:] = starts[d * n_slots:(d + 1) * n_slots, :]


def make_plan(lengths, n_dev):
    n_slots, batch = lengths.shape
    part = batch // n_dev
    return pl.pallas_call(
        plan_kernel,
        out_shape=jax.ShapeDtypeStruct((n_dev, n_slots, part + BLOCK), jnp.int32),
        in_specs=[pl.BlockSpec(memory_space=pltpu.VMEM)],
        out_specs=pl.BlockSpec(memory_space=pltpu.VMEM),
        scratch_shapes=[pltpu.VMEM((n_dev * n_slots, part), jnp.int32)],
        compiler_params=pltpu.CompilerParams(vmem_limit_bytes=16000000),
        cost_estimate=pl.CostEstimate(flops=10000000, bytes_accessed=1000000, transcendentals=0),
    )(lengths)


def ids_kernel(n_dev, n_rows, hop_slots, me_ref, ids_ref, lengths_ref, *refs):
    *packed_refs, ids_v, len_v = refs
    n_slots, batch = ids_ref.shape
    part, rows = batch // n_dev, n_dev * n_slots
    gather_parts(ids_ref, ids_v, n_dev)
    gather_parts(lengths_ref, len_v, n_dev)
    prefix = prefix_matrix()
    lane = lax.broadcasted_iota(jnp.int32, (rows, BLOCK), 1)
    count = jnp.zeros((rows, 1), jnp.int32)
    moves = []
    for b in range(part // BLOCK):
        valid, local, more = block_prefix(len_v, b, prefix)
        shift = (b * BLOCK + lane) - (count + local)
        moves.append(jnp.where(valid, (shift << 16) | ids_v[:, b * BLOCK:(b + 1) * BLOCK], n_rows))
        count = count + more
    move = jnp.concatenate(moves, axis=1)
    step = 1
    while step < part:
        come = pltpu.roll(move, part - step, 1)
        bit = step << 16
        stay = jnp.where((move & bit) != 0, n_rows, move)
        move = jnp.where((come & bit) != 0, come, stay)
        step *= 2
    spot = lax.broadcasted_iota(jnp.int32, (rows, part), 1)
    ids_v[...] = jnp.where(spot < count, move & 0xFFFF, n_rows)
    most = jnp.max(count, axis=0, keepdims=True)
    for s in range(n_slots):
        for d in range(n_dev):
            sender = (me_ref[0] + (n_dev - d)) % n_dev if s in hop_slots else d
            packed_refs[s][:, d * part:(d + 1) * part] = ids_v[pl.ds(sender * n_slots + s, 1), :]
        packed_refs[s][:, n_dev * part:] = jnp.broadcast_to(most, (1, BLOCK))


def pack_ids(me, ids, lengths, n_dev, n_rows, hop_slots):
    n_slots, batch = ids.shape
    part = batch // n_dev
    assert n_rows < 1 << 15 and part <= 1 << 15
    return pl.pallas_call(
        functools.partial(ids_kernel, n_dev, n_rows, hop_slots),
        out_shape=(jax.ShapeDtypeStruct((1, batch + BLOCK), jnp.int32),) * n_slots,
        in_specs=[pl.BlockSpec(memory_space=pltpu.SMEM)] + [pl.BlockSpec(memory_space=pltpu.VMEM)] * 2,
        out_specs=(pl.BlockSpec(memory_space=pltpu.VMEM),) * n_slots,
        scratch_shapes=[pltpu.VMEM((n_dev * n_slots, part), jnp.int32)] * 2,
        compiler_params=pltpu.CompilerParams(vmem_limit_bytes=32000000),
        cost_estimate=pl.CostEstimate(flops=20000000, bytes_accessed=2000000, transcendentals=0),
    )(me, ids, lengths)


def share_kernel(n_dev, plan_ref, plans_ref, starts_ref, most_ref, send_sem, recv_sem, own_sem):
    pod, me = lax.axis_index('pod'), lax.axis_index('mp')
    barrier = pltpu.get_barrier_semaphore()
    for o in range(1, n_dev):
        pl.semaphore_signal(barrier, inc=1, device_id=(pod, (me + o) % n_dev), device_id_type=pl.DeviceIdType.MESH)
    pl.semaphore_wait(barrier, n_dev - 1)
    copies = [
        pltpu.make_async_remote_copy(
            src_ref=plan_ref.at[(me + o) % n_dev],
            dst_ref=plans_ref.at[me],
            send_sem=send_sem.at[o],
            recv_sem=recv_sem.at[o],
            device_id=(pod, (me + o) % n_dev),
            device_id_type=pl.DeviceIdType.MESH,
        )
        for o in range(1, n_dev)
    ]
    for copy in copies:
        copy.start()
    own = pltpu.make_async_copy(plan_ref.at[me], plans_ref.at[me], own_sem)
    own.start()
    own.wait()
    for copy in copies:
        copy.wait()
    part = plans_ref.shape[2] - BLOCK
    starts = plans_ref[:, :, part:]
    starts_ref[...] = starts
    most_ref[0] = jnp.max(starts[:, :, MAX_LANE:MAX_LANE + 1])


def share_plan(plan):
    n_dev, n_slots, _ = plan.shape
    return pl.pallas_call(
        functools.partial(share_kernel, n_dev),
        out_shape=(
            jax.ShapeDtypeStruct(plan.shape, plan.dtype),
            jax.ShapeDtypeStruct((n_dev, n_slots, BLOCK), plan.dtype),
            jax.ShapeDtypeStruct((1,), plan.dtype),
        ),
        in_specs=[pl.BlockSpec(memory_space=pltpu.VMEM)],
        out_specs=(pl.BlockSpec(memory_space=pltpu.VMEM), pl.BlockSpec(memory_space=pltpu.VMEM), pl.BlockSpec(memory_space=pltpu.SMEM)),
        scratch_shapes=[pltpu.SemaphoreType.DMA((n_dev,)), pltpu.SemaphoreType.DMA((n_dev,)), pltpu.SemaphoreType.DMA],
        compiler_params=pltpu.CompilerParams(collective_id=0, has_side_effects=True, vmem_limit_bytes=16000000),
        cost_estimate=pl.CostEstimate(flops=20000000, bytes_accessed=2000000, transcendentals=0),
    )(plan)


def pack_kernel(slots, starts_ref, plan_ref, tables_ref, out_ref, grad_v, stage, pack_v, in_sem, out_sem):
    n_slots = plan_ref.shape[1]
    cap = out_ref.shape[2]
    n_tab, part, _ = tables_ref.shape
    slot_row = lax.broadcasted_iota(jnp.int32, (BLOCK, BLOCK), 0)
    used = [[d for d in range(out_ref.shape[0]) if d * n_slots + slot < n_tab] for slot in slots]

    def fetch(i, d):
        return pltpu.make_async_copy(tables_ref.at[d * n_slots + slots[i]], grad_v.at[i, d], in_sem.at[i, d])

    def emit(i, d):
        return pltpu.make_async_copy(pack_v.at[i, d], out_ref.at[d, i], out_sem.at[i, d])

    for i, dests in enumerate(used):
        for d in dests:
            fetch(i, d).start()
    for i, dests in enumerate(used):
        def table(d, carry):
            fetch(i, d).wait()
            for b in range(part // BLOCK):
                place = plan_ref[d, slots[i]:slots[i] + 1, b * BLOCK:(b + 1) * BLOCK]
                pick = jnp.where(slot_row == place, 1.0, 0.0).astype(jnp.bfloat16)
                rows = jnp.dot(pick, grad_v[i, d, b * BLOCK:(b + 1) * BLOCK, :], preferred_element_type=jnp.float32)
                stage[pl.ds(starts_ref[d, slots[i], b], BLOCK), :] = rows
            pack_v[i, d] = stage[:cap, :].astype(jnp.bfloat16)
            emit(i, d).start()
            return carry

        lax.fori_loop(0, len(dests), table, 0)
    for i, dests in enumerate(used):
        for d in dests:
            emit(i, d).wait()


def pack_slots(slots, cap, starts, plan, by_table):
    n_dev = plan.shape[0]
    _, part, dim = by_table.shape
    n = len(slots)
    return pl.pallas_call(
        functools.partial(pack_kernel, slots),
        out_shape=jax.ShapeDtypeStruct((n_dev, n, cap, dim), by_table.dtype),
        in_specs=[pl.BlockSpec(memory_space=pltpu.SMEM), pl.BlockSpec(memory_space=pltpu.VMEM), pl.BlockSpec(memory_space=pl.ANY)],
        out_specs=pl.BlockSpec(memory_space=pl.ANY),
        scratch_shapes=[
            pltpu.VMEM((n, n_dev, part, dim), by_table.dtype),
            pltpu.VMEM((cap + BLOCK, dim), jnp.float32),
            pltpu.VMEM((n, n_dev, cap, dim), by_table.dtype),
            pltpu.SemaphoreType.DMA((n, n_dev)),
            pltpu.SemaphoreType.DMA((n, n_dev)),
        ],
        compiler_params=pltpu.CompilerParams(vmem_limit_bytes=VMEM_LIMIT),
        cost_estimate=pl.CostEstimate(flops=n * n_dev * part * dim * 20, bytes_accessed=n * n_dev * part * dim * 3, transcendentals=0),
    )(starts, plan, by_table)


def pack_hops_kernel(slot, me_ref, starts_ref, plan_ref, tables_ref, *refs):
    n_dev, n_slots, _ = plan_ref.shape
    n_tab, part, _ = tables_ref.shape
    out_refs, (grad_v, stage, pack_v, in_sem, out_sem) = refs[:n_dev], refs[n_dev:]
    cap = pack_v.shape[1]
    slot_row = lax.broadcasted_iota(jnp.int32, (BLOCK, BLOCK), 0)
    me = me_ref[0]

    def fetch(o):
        table = jnp.minimum((me + o) % n_dev * n_slots + slot, n_tab - 1)
        return pltpu.make_async_copy(tables_ref.at[table], grad_v.at[o], in_sem.at[o])

    for o in range(n_dev):
        fetch(o).start()

    def one(o, carry):
        d = (me + o) % n_dev
        fetch(o).wait()

        @pl.when(d * n_slots + slot < n_tab)
        def _():
            for b in range(part // BLOCK):
                place = plan_ref[d, slot:slot + 1, b * BLOCK:(b + 1) * BLOCK]
                pick = jnp.where(slot_row == place, 1.0, 0.0).astype(jnp.bfloat16)
                rows = jnp.dot(pick, grad_v[o, b * BLOCK:(b + 1) * BLOCK, :], preferred_element_type=jnp.float32)
                stage[pl.ds(starts_ref[d, slot, b], BLOCK), :] = rows
            pack_v[o] = stage[:cap, :].astype(jnp.bfloat16)

        return carry

    lax.fori_loop(0, n_dev, one, 0)
    copies = [pltpu.make_async_copy(pack_v.at[o], out_refs[o], out_sem.at[o]) for o in range(n_dev)]
    for copy in copies:
        copy.start()
    for copy in copies:
        copy.wait()


def pack_hops(slot, cap, me, starts, plan, by_table):
    n_dev, _, _ = plan.shape
    _, part, dim = by_table.shape
    return pl.pallas_call(
        functools.partial(pack_hops_kernel, slot),
        out_shape=(jax.ShapeDtypeStruct((cap, dim), by_table.dtype),) * n_dev,
        in_specs=[pl.BlockSpec(memory_space=pltpu.SMEM)] * 2 + [pl.BlockSpec(memory_space=pltpu.VMEM), pl.BlockSpec(memory_space=pl.ANY)],
        out_specs=(pl.BlockSpec(memory_space=pl.ANY),) * n_dev,
        scratch_shapes=[
            pltpu.VMEM((n_dev, part, dim), by_table.dtype),
            pltpu.VMEM((cap + BLOCK, dim), jnp.float32),
            pltpu.VMEM((n_dev, cap, dim), by_table.dtype),
            pltpu.SemaphoreType.DMA((n_dev,)),
            pltpu.SemaphoreType.DMA((n_dev,)),
        ],
        compiler_params=pltpu.CompilerParams(vmem_limit_bytes=VMEM_LIMIT),
        cost_estimate=pl.CostEstimate(flops=n_dev * part * dim * 20, bytes_accessed=n_dev * part * dim * 3, transcendentals=0),
    )(me, starts, plan, by_table)


def apply_kernel(slots, n_carried, n_grads, lr_ref, tables_ref, accums_ref, *refs):
    n = len(slots)
    grad_refs, refs = refs[:n_grads], refs[n_grads:]
    ids_refs, carried_refs = refs[:n], refs[n:n + n_carried]
    out_tables_ref, out_accums_ref, *scratch = refs[n + n_carried:]
    banks, (stage, table_v, grad_v, done_v, sem, out_sem, ids_sem, grad_sem), scalars = scratch[:BANKS], scratch[BANKS:BANKS + 8], scratch[BANKS + 8:]
    _, segs, seg_rows, dim = grad_v.shape
    part = (ids_refs[0].shape[1] - BLOCK) // segs
    ids_s = [scalars[i * (segs + 1):(i + 1) * (segs + 1)] for i in range(n)]
    n_rows = tables_ref.shape[1]
    copies = [
        (
            [pltpu.make_async_copy(ref, grad_v.at[i, o], grad_sem.at[i, o]) for o, ref in enumerate(grad_refs)]
            if n_grads > 1
            else [pltpu.make_async_copy(grad_refs[0].at[:, i], grad_v.at[i], grad_sem.at[i, 0])],
            [pltpu.make_async_copy(ids_refs[i].at[:, j * part:(j + 1) * part], ids_s[i][j], ids_sem.at[i, j]) for j in range(segs)]
            + [pltpu.make_async_copy(ids_refs[i].at[:, segs * part:], ids_s[i][segs], ids_sem.at[i, segs])],
            pltpu.make_async_copy(tables_ref.at[slot], table_v.at[i], sem.at[i]),
        )
        for i, slot in enumerate(slots)
    ]
    for grad_copies, ids_copies, table_copy in copies:
        for copy in ids_copies + grad_copies:
            copy.start()
        table_copy.start()

    if n_carried:
        done_copy = pltpu.make_async_copy(carried_refs[1], done_v, out_sem.at[n])
        done_copy.start()
    zero = jnp.zeros((BLOCK, dim), jnp.float32)

    def clear(i, carry):
        for bank in banks:
            bank[pl.ds(pl.multiple_of(i * BLOCK, BLOCK), BLOCK), :] = zero
        return carry

    lax.fori_loop(0, n_rows // BLOCK, clear, 0)
    for bank in banks:
        bank[pl.ds(n_rows, 8), :] = zero[:8]
    eye = lax.broadcasted_iota(jnp.int32, (BLOCK, dim), 0) == lax.broadcasted_iota(jnp.int32, (BLOCK, dim), 1)
    lr = lr_ref[0]

    for i, slot in enumerate(slots):
        grad_copies, ids_copies, table_copy = copies[i]
        for copy in ids_copies + grad_copies:
            copy.wait()

        def widen(t, carry):
            for j in range(segs):
                rows = pl.ds(pl.multiple_of(t * 32, 32), 32)
                stage[j, rows, :] = grad_v[i, j, rows, :].astype(jnp.float32)
            return carry

        lax.fori_loop(0, seg_rows // 32, widen, 0)

        def add_rows(t, carry):
            base = t * UNROLL
            for u in range(UNROLL):
                for j, bank in enumerate(banks):
                    first, second = ids_s[i][2 * j][0, base + u], ids_s[i][2 * j + 1][0, base + u]
                    same = jnp.full((1, dim), first) == jnp.full((1, dim), second)
                    add_first = stage[2 * j, pl.ds(base + u, 1), :]
                    add_second = stage[2 * j + 1, pl.ds(base + u, 1), :]
                    add_second = jnp.where(same, add_first + add_second, add_second)
                    old_first = bank[pl.ds(first, 1), :]
                    old_second = bank[pl.ds(second, 1), :]
                    bank[pl.ds(first, 1), :] = old_first + add_first
                    bank[pl.ds(second, 1), :] = old_second + add_second
            return carry

        lax.fori_loop(0, (ids_s[i][segs][0, 0] + UNROLL - 1) // UNROLL, add_rows, 0)
        table_copy.wait()
        if n_carried and i == 0:
            done_copy.wait()

        def update(c, carry):
            for s in range(CHUNK // BLOCK):
                first_row = pl.multiple_of((c * (CHUNK // BLOCK) + s) * BLOCK, BLOCK)
                rows = pl.ds(first_row, BLOCK)
                grad = banks[0][rows, :]
                for bank in banks[1:]:
                    grad = grad + bank[rows, :]
                if i + 1 < n:
                    for bank in banks:
                        bank[rows, :] = zero
                old = jnp.where(eye, accums_ref[slot:slot + 1, rows], 0.0)
                new = jnp.sum(grad * grad * (1.0 / dim) + old, axis=1, keepdims=True)
                done_v[slot:slot + 1, rows] = jnp.sum(jnp.where(eye, new, 0.0), axis=0, keepdims=True)
                root = lax.rsqrt(jnp.maximum(new, TINY))
                scale = lr * root / (1.0 + EPSILON * root)
                table_v[i, rows, :] = (table_v[i, rows, :].astype(jnp.float32) - grad * scale).astype(jnp.bfloat16)
            done = pl.ds(pl.multiple_of(c * CHUNK, CHUNK), CHUNK)
            pltpu.make_async_copy(table_v.at[i, done], out_tables_ref.at[slot, done], out_sem.at[i]).start()
            if i == n - 1:
                pltpu.make_async_copy(done_v.at[:, done], out_accums_ref.at[:, done], out_sem.at[n]).start()
            return carry

        lax.fori_loop(0, n_rows // CHUNK, update, 0)
    for i, slot in enumerate(slots):
        pltpu.make_async_copy(table_v.at[i], out_tables_ref.at[slot], out_sem.at[i]).wait()
    pltpu.make_async_copy(done_v, out_accums_ref, out_sem.at[n]).wait()


def apply_slots(slots, ids, lr, grads, tables, accums, carried):
    _, n_rows, dim = tables.shape
    n, segs = len(slots), (len(grads) if len(grads) > 1 else grads[0].shape[0])
    seg_rows = grads[0].shape[-2]
    part = (ids[0].shape[1] - BLOCK) // segs
    assert segs == 2 * BANKS
    return pl.pallas_call(
        functools.partial(apply_kernel, slots, len(carried), len(grads)),
        out_shape=tuple(jax.ShapeDtypeStruct(x.shape, x.dtype) for x in (tables, accums)),
        in_specs=[pl.BlockSpec(memory_space=pltpu.SMEM)]
        + [pl.BlockSpec(memory_space=pl.ANY), pl.BlockSpec(memory_space=pltpu.VMEM)]
        + [pl.BlockSpec(memory_space=pl.ANY)] * (len(grads) + n)
        + [pl.BlockSpec(memory_space=pl.ANY)] * len(carried),
        out_specs=(pl.BlockSpec(memory_space=pl.ANY),) * 2,
        input_output_aliases={3 + len(grads) + n + i: i for i in range(len(carried))},
        scratch_shapes=[pltpu.VMEM((n_rows + 8, dim), jnp.float32)] * BANKS
        + [
            pltpu.VMEM((segs, seg_rows, dim), jnp.float32),
            pltpu.VMEM((n, n_rows, dim), tables.dtype),
            pltpu.VMEM((n, segs, seg_rows, dim), grads[0].dtype),
            pltpu.VMEM(accums.shape, accums.dtype),
            pltpu.SemaphoreType.DMA((n,)),
            pltpu.SemaphoreType.DMA((n + 1,)),
            pltpu.SemaphoreType.DMA((n, segs + 1)),
            pltpu.SemaphoreType.DMA((n, segs)),
        ]
        + ([pltpu.SMEM((1, part), jnp.int32)] * segs + [pltpu.SMEM((1, BLOCK), jnp.int32)]) * n,
        compiler_params=pltpu.CompilerParams(vmem_limit_bytes=VMEM_LIMIT),
        cost_estimate=pl.CostEstimate(flops=n * n_rows * dim * 400, bytes_accessed=4 * n * n_rows * dim * 2, transcendentals=0),
    )(lr, tables, accums, *grads, *(ids[k] for k in slots), *carried)


def routes(n_dev, n_slots, n_tab, slot, offset):
    pairs = [(d, (d + offset) % n_dev) for d in range(n_dev)]
    return [(src, dst) for src, dst in pairs if dst * n_slots + slot < n_tab]


def solution(mesh):
    n_group = mesh.shape['mp']
    slot_spec = P(('pod', 'mp'))

    def local_step(d_pool, row_ids, lengths, tables, row_accum, learn_rate):
        n_slots, n_rows, _ = tables.shape
        by_table = jnp.transpose(d_pool, (1, 0, 2))
        part = by_table.shape[1]
        me = lax.axis_index('mp').reshape(1)
        n_tab = by_table.shape[0]
        plan_out = make_plan(lengths, n_group)
        plan, starts, most = share_plan(plan_out)
        most = most[0]
        lr = learn_rate.reshape(1)
        caps = CAPS(part)

        def exchange(level):
            def run(operands):
                me, by_table, plan, starts, row_ids, lengths, lr, tables, accums = operands
                got = {}
                chunks, hop_slots = CHUNKS(n_slots)
                for c, slots in enumerate(chunks):
                    if slots == hop_slots:
                        pack = pack_hops(slots[0], caps[level], me, starts, plan, by_table)
                    else:
                        pack = pack_slots(slots, caps[level], starts, plan, by_table)
                    if slots == hop_slots:
                        hops = [lax.ppermute(pack[o], 'mp', routes(n_group, n_slots, n_tab, slots[0], o)) for o in range(1, n_group)]
                        got[c] = [pack[0]] + hops
                    else:
                        got[c] = [lax.all_to_all(pack, 'mp', 0, 0, tiled=True)]
                ids = pack_ids(me, row_ids[:, :, 0], lengths, n_group, n_rows, hop_slots)
                carried = ()
                for c, slots in enumerate(chunks):
                    carried = apply_slots(slots, ids, lr, got[c], tables, accums, carried)
                return tuple(carried)

            return run

        level = sum((most > cap).astype(jnp.int32) for cap in caps[:-1])
        operands = (me, by_table, plan, starts, row_ids, lengths, lr, tables, row_accum)
        return lax.switch(level, [exchange(i) for i in range(len(caps))], operands)

    return jax.shard_map(local_step, mesh=mesh, in_specs=(slot_spec, slot_spec, slot_spec, slot_spec, slot_spec, P()), out_specs=(slot_spec, slot_spec), check_vma=False)


def CAPS(part):
    return part * 35 // 64, part * 39 // 64, part


def CHUNKS(n_slots):
    return tuple((k,) for k in range(n_slots)), (n_slots - 2,)
```

```python
import functools

import jax
import jax.numpy as jnp
from jax import lax
from jax.experimental import pallas as pl
from jax.experimental.pallas import tpu as pltpu
from jax.sharding import PartitionSpec as P


EPSILON = 1e-06
TINY = 1e-36
BANKS = 4
UNROLL = 16
BLOCK = 128
CHUNK = 1024
MAX_LANE = 64
VMEM_LIMIT = 66000000


def gather_parts(src_ref, dst, n_dev):
    n_slots, batch = src_ref.shape
    part = batch // n_dev
    for d in range(n_dev):
        dst[d * n_slots:(d + 1) * n_slots, :] = src_ref[:, d * part:(d + 1) * part]


def block_prefix(len_v, b, prefix):
    valid = len_v[:, b * BLOCK:(b + 1) * BLOCK] > 0
    ones = jnp.where(valid, 1.0, 0.0)
    local = jnp.dot(ones.astype(jnp.bfloat16), prefix, preferred_element_type=jnp.float32).astype(jnp.int32)
    return valid, local, jnp.sum(ones, axis=1, keepdims=True).astype(jnp.int32)


def prefix_matrix():
    below = lax.broadcasted_iota(jnp.int32, (BLOCK, BLOCK), 0) < lax.broadcasted_iota(jnp.int32, (BLOCK, BLOCK), 1)
    return jnp.where(below, 1.0, 0.0).astype(jnp.bfloat16)


def plan_kernel(lengths_ref, plan_ref, len_v):
    n_dev, n_slots, width = plan_ref.shape
    part, rows = width - BLOCK, n_dev * n_slots
    gather_parts(lengths_ref, len_v, n_dev)
    prefix = prefix_matrix()
    lane = lax.broadcasted_iota(jnp.int32, (rows, BLOCK), 1)
    count = jnp.zeros((rows, 1), jnp.int32)
    starts = jnp.zeros((rows, BLOCK), jnp.int32)
    for b in range(part // BLOCK):
        valid, local, more = block_prefix(len_v, b, prefix)
        place = jnp.where(valid, local, -1)
        for d in range(n_dev):
            plan_ref[d, :, b * BLOCK:(b + 1) * BLOCK] = place[d * n_slots:(d + 1) * n_slots, :]
        starts = jnp.where(lane == b, count, starts)
        count = count + more
    starts = jnp.where(lane == MAX_LANE, jnp.max(count, axis=0, keepdims=True), starts)
    for d in range(n_dev):
        plan_ref[d, :, part:] = starts[d * n_slots:(d + 1) * n_slots, :]


def make_plan(lengths, n_dev):
    n_slots, batch = lengths.shape
    part = batch // n_dev
    return pl.pallas_call(
        plan_kernel,
        out_shape=jax.ShapeDtypeStruct((n_dev, n_slots, part + BLOCK), jnp.int32),
        in_specs=[pl.BlockSpec(memory_space=pltpu.VMEM)],
        out_specs=pl.BlockSpec(memory_space=pltpu.VMEM),
        scratch_shapes=[pltpu.VMEM((n_dev * n_slots, part), jnp.int32)],
        compiler_params=pltpu.CompilerParams(vmem_limit_bytes=16000000),
        cost_estimate=pl.CostEstimate(flops=10000000, bytes_accessed=1000000, transcendentals=0),
    )(lengths)


def ids_kernel(n_dev, n_rows, hop_slots, me_ref, ids_ref, lengths_ref, *refs):
    *packed_refs, ids_v, len_v = refs
    n_slots, batch = ids_ref.shape
    part, rows = batch // n_dev, n_dev * n_slots
    gather_parts(ids_ref, ids_v, n_dev)
    gather_parts(lengths_ref, len_v, n_dev)
    prefix = prefix_matrix()
    lane = lax.broadcasted_iota(jnp.int32, (rows, BLOCK), 1)
    count = jnp.zeros((rows, 1), jnp.int32)
    moves = []
    for b in range(part // BLOCK):
        valid, local, more = block_prefix(len_v, b, prefix)
        shift = (b * BLOCK + lane) - (count + local)
        moves.append(jnp.where(valid, (shift << 16) | ids_v[:, b * BLOCK:(b + 1) * BLOCK], n_rows))
        count = count + more
    move = jnp.concatenate(moves, axis=1)
    step = 1
    while step < part:
        come = pltpu.roll(move, part - step, 1)
        bit = step << 16
        stay = jnp.where((move & bit) != 0, n_rows, move)
        move = jnp.where((come & bit) != 0, come, stay)
        step *= 2
    spot = lax.broadcasted_iota(jnp.int32, (rows, part), 1)
    ids_v[...] = jnp.where(spot < count, move & 0xFFFF, n_rows)
    most = jnp.max(count, axis=0, keepdims=True)
    for s in range(n_slots):
        for d in range(n_dev):
            sender = (me_ref[0] + (n_dev - d)) % n_dev if s in hop_slots else d
            packed_refs[s][:, d * part:(d + 1) * part] = ids_v[pl.ds(sender * n_slots + s, 1), :]
        packed_refs[s][:, n_dev * part:] = jnp.broadcast_to(most, (1, BLOCK))


def pack_ids(me, ids, lengths, n_dev, n_rows, hop_slots):
    n_slots, batch = ids.shape
    part = batch // n_dev
    assert n_rows < 1 << 15 and part <= 1 << 15
    return pl.pallas_call(
        functools.partial(ids_kernel, n_dev, n_rows, hop_slots),
        out_shape=(jax.ShapeDtypeStruct((1, batch + BLOCK), jnp.int32),) * n_slots,
        in_specs=[pl.BlockSpec(memory_space=pltpu.SMEM)] + [pl.BlockSpec(memory_space=pltpu.VMEM)] * 2,
        out_specs=(pl.BlockSpec(memory_space=pltpu.VMEM),) * n_slots,
        scratch_shapes=[pltpu.VMEM((n_dev * n_slots, part), jnp.int32)] * 2,
        compiler_params=pltpu.CompilerParams(vmem_limit_bytes=32000000),
        cost_estimate=pl.CostEstimate(flops=20000000, bytes_accessed=2000000, transcendentals=0),
    )(me, ids, lengths)


def share_kernel(n_dev, caps, plan_ref, plans_ref, starts_ref, level_ref, send_sem, recv_sem, own_sem):
    pod, me = lax.axis_index('pod'), lax.axis_index('mp')
    barrier = pltpu.get_barrier_semaphore()
    for o in range(1, n_dev):
        pl.semaphore_signal(barrier, inc=1, device_id=(pod, (me + o) % n_dev), device_id_type=pl.DeviceIdType.MESH)
    pl.semaphore_wait(barrier, n_dev - 1)
    copies = [
        pltpu.make_async_remote_copy(
            src_ref=plan_ref.at[(me + o) % n_dev],
            dst_ref=plans_ref.at[me],
            send_sem=send_sem.at[o],
            recv_sem=recv_sem.at[o],
            device_id=(pod, (me + o) % n_dev),
            device_id_type=pl.DeviceIdType.MESH,
        )
        for o in range(1, n_dev)
    ]
    for copy in copies:
        copy.start()
    own = pltpu.make_async_copy(plan_ref.at[me], plans_ref.at[me], own_sem)
    own.start()
    own.wait()
    for copy in copies:
        copy.wait()
    part = plans_ref.shape[2] - BLOCK
    starts = plans_ref[:, :, part:]
    starts_ref[...] = starts
    most = jnp.max(starts[:, :, MAX_LANE:MAX_LANE + 1])
    level_ref[0] = sum((most > cap).astype(jnp.int32) for cap in caps[:-1])


def share_plan(plan, caps):
    n_dev, n_slots, _ = plan.shape
    return pl.pallas_call(
        functools.partial(share_kernel, n_dev, caps),
        out_shape=(
            jax.ShapeDtypeStruct(plan.shape, plan.dtype),
            jax.ShapeDtypeStruct((n_dev, n_slots, BLOCK), plan.dtype),
            jax.ShapeDtypeStruct((1,), plan.dtype),
        ),
        in_specs=[pl.BlockSpec(memory_space=pltpu.VMEM)],
        out_specs=(pl.BlockSpec(memory_space=pltpu.VMEM), pl.BlockSpec(memory_space=pltpu.VMEM), pl.BlockSpec(memory_space=pltpu.SMEM)),
        scratch_shapes=[pltpu.SemaphoreType.DMA((n_dev,)), pltpu.SemaphoreType.DMA((n_dev,)), pltpu.SemaphoreType.DMA],
        compiler_params=pltpu.CompilerParams(collective_id=0, has_side_effects=True, vmem_limit_bytes=16000000),
        cost_estimate=pl.CostEstimate(flops=20000000, bytes_accessed=2000000, transcendentals=0),
    )(plan)


def pack_kernel(slots, starts_ref, plan_ref, tables_ref, out_ref, grad_v, stage, pack_v, in_sem, out_sem):
    n_slots = plan_ref.shape[1]
    cap = out_ref.shape[2]
    n_tab, part, _ = tables_ref.shape
    slot_row = lax.broadcasted_iota(jnp.int32, (BLOCK, BLOCK), 0)
    used = [[d for d in range(out_ref.shape[0]) if d * n_slots + slot < n_tab] for slot in slots]

    def fetch(i, d):
        return pltpu.make_async_copy(tables_ref.at[d * n_slots + slots[i]], grad_v.at[i, d], in_sem.at[i, d])

    def emit(i, d):
        return pltpu.make_async_copy(pack_v.at[i, d], out_ref.at[d, i], out_sem.at[i, d])

    for i, dests in enumerate(used):
        for d in dests:
            fetch(i, d).start()
    for i, dests in enumerate(used):
        def table(d, carry):
            fetch(i, d).wait()
            for b in range(part // BLOCK):
                place = plan_ref[d, slots[i]:slots[i] + 1, b * BLOCK:(b + 1) * BLOCK]
                pick = jnp.where(slot_row == place, 1.0, 0.0).astype(jnp.bfloat16)
                rows = jnp.dot(pick, grad_v[i, d, b * BLOCK:(b + 1) * BLOCK, :], preferred_element_type=jnp.float32)
                stage[pl.ds(starts_ref[d, slots[i], b], BLOCK), :] = rows
            pack_v[i, d] = stage[:cap, :].astype(jnp.bfloat16)
            emit(i, d).start()
            return carry

        lax.fori_loop(0, len(dests), table, 0)
    for i, dests in enumerate(used):
        for d in dests:
            emit(i, d).wait()


def pack_slots(slots, cap, starts, plan, by_table):
    n_dev = plan.shape[0]
    _, part, dim = by_table.shape
    n = len(slots)
    return pl.pallas_call(
        functools.partial(pack_kernel, slots),
        out_shape=jax.ShapeDtypeStruct((n_dev, n, cap, dim), by_table.dtype),
        in_specs=[pl.BlockSpec(memory_space=pltpu.SMEM), pl.BlockSpec(memory_space=pltpu.VMEM), pl.BlockSpec(memory_space=pl.ANY)],
        out_specs=pl.BlockSpec(memory_space=pl.ANY),
        scratch_shapes=[
            pltpu.VMEM((n, n_dev, part, dim), by_table.dtype),
            pltpu.VMEM((cap + BLOCK, dim), jnp.float32),
            pltpu.VMEM((n, n_dev, cap, dim), by_table.dtype),
            pltpu.SemaphoreType.DMA((n, n_dev)),
            pltpu.SemaphoreType.DMA((n, n_dev)),
        ],
        compiler_params=pltpu.CompilerParams(vmem_limit_bytes=VMEM_LIMIT),
        cost_estimate=pl.CostEstimate(flops=n * n_dev * part * dim * 20, bytes_accessed=n * n_dev * part * dim * 3, transcendentals=0),
    )(starts, plan, by_table)


def pack_hops_kernel(slot, me_ref, starts_ref, plan_ref, tables_ref, *refs):
    n_dev, n_slots, _ = plan_ref.shape
    n_tab, part, _ = tables_ref.shape
    out_refs, (grad_v, stage, pack_v, in_sem, out_sem) = refs[:n_dev], refs[n_dev:]
    cap = pack_v.shape[1]
    slot_row = lax.broadcasted_iota(jnp.int32, (BLOCK, BLOCK), 0)
    me = me_ref[0]

    def fetch(o):
        table = jnp.minimum((me + o) % n_dev * n_slots + slot, n_tab - 1)
        return pltpu.make_async_copy(tables_ref.at[table], grad_v.at[o], in_sem.at[o])

    for o in range(n_dev):
        fetch(o).start()

    def one(o, carry):
        d = (me + o) % n_dev
        fetch(o).wait()

        @pl.when(d * n_slots + slot < n_tab)
        def _():
            for b in range(part // BLOCK):
                place = plan_ref[d, slot:slot + 1, b * BLOCK:(b + 1) * BLOCK]
                pick = jnp.where(slot_row == place, 1.0, 0.0).astype(jnp.bfloat16)
                rows = jnp.dot(pick, grad_v[o, b * BLOCK:(b + 1) * BLOCK, :], preferred_element_type=jnp.float32)
                stage[pl.ds(starts_ref[d, slot, b], BLOCK), :] = rows
            pack_v[o] = stage[:cap, :].astype(jnp.bfloat16)

        return carry

    lax.fori_loop(0, n_dev, one, 0)
    copies = [pltpu.make_async_copy(pack_v.at[o], out_refs[o], out_sem.at[o]) for o in range(n_dev)]
    for copy in copies:
        copy.start()
    for copy in copies:
        copy.wait()


def pack_hops(slot, cap, me, starts, plan, by_table):
    n_dev, _, _ = plan.shape
    _, part, dim = by_table.shape
    return pl.pallas_call(
        functools.partial(pack_hops_kernel, slot),
        out_shape=(jax.ShapeDtypeStruct((cap, dim), by_table.dtype),) * n_dev,
        in_specs=[pl.BlockSpec(memory_space=pltpu.SMEM)] * 2 + [pl.BlockSpec(memory_space=pltpu.VMEM), pl.BlockSpec(memory_space=pl.ANY)],
        out_specs=(pl.BlockSpec(memory_space=pl.ANY),) * n_dev,
        scratch_shapes=[
            pltpu.VMEM((n_dev, part, dim), by_table.dtype),
            pltpu.VMEM((cap + BLOCK, dim), jnp.float32),
            pltpu.VMEM((n_dev, cap, dim), by_table.dtype),
            pltpu.SemaphoreType.DMA((n_dev,)),
            pltpu.SemaphoreType.DMA((n_dev,)),
        ],
        compiler_params=pltpu.CompilerParams(vmem_limit_bytes=VMEM_LIMIT),
        cost_estimate=pl.CostEstimate(flops=n_dev * part * dim * 20, bytes_accessed=n_dev * part * dim * 3, transcendentals=0),
    )(me, starts, plan, by_table)


def apply_kernel(slots, n_carried, n_grads, lr_ref, tables_ref, accums_ref, *refs):
    n = len(slots)
    grad_refs, refs = refs[:n_grads], refs[n_grads:]
    ids_refs, carried_refs = refs[:n], refs[n:n + n_carried]
    out_tables_ref, out_accums_ref, *scratch = refs[n + n_carried:]
    banks, (stage, table_v, grad_v, done_v, sem, out_sem, ids_sem, grad_sem), scalars = scratch[:BANKS], scratch[BANKS:BANKS + 8], scratch[BANKS + 8:]
    _, segs, seg_rows, dim = grad_v.shape
    part = (ids_refs[0].shape[1] - BLOCK) // segs
    ids_s = [scalars[i * (segs + 1):(i + 1) * (segs + 1)] for i in range(n)]
    n_rows = tables_ref.shape[1]
    copies = [
        (
            [pltpu.make_async_copy(ref, grad_v.at[i, o], grad_sem.at[i, o]) for o, ref in enumerate(grad_refs)]
            if n_grads > 1
            else [pltpu.make_async_copy(grad_refs[0].at[:, i], grad_v.at[i], grad_sem.at[i, 0])],
            [pltpu.make_async_copy(ids_refs[i].at[:, j * part:(j + 1) * part], ids_s[i][j], ids_sem.at[i, j]) for j in range(segs)]
            + [pltpu.make_async_copy(ids_refs[i].at[:, segs * part:], ids_s[i][segs], ids_sem.at[i, segs])],
            pltpu.make_async_copy(tables_ref.at[slot], table_v.at[i], sem.at[i]),
        )
        for i, slot in enumerate(slots)
    ]
    for grad_copies, ids_copies, table_copy in copies:
        for copy in ids_copies + grad_copies:
            copy.start()
        table_copy.start()

    if n_carried:
        done_copy = pltpu.make_async_copy(carried_refs[1], done_v, out_sem.at[n])
        done_copy.start()
    zero = jnp.zeros((BLOCK, dim), jnp.float32)

    def clear(i, carry):
        for bank in banks:
            bank[pl.ds(pl.multiple_of(i * BLOCK, BLOCK), BLOCK), :] = zero
        return carry

    lax.fori_loop(0, n_rows // BLOCK, clear, 0)
    for bank in banks:
        bank[pl.ds(n_rows, 8), :] = zero[:8]
    eye = lax.broadcasted_iota(jnp.int32, (BLOCK, dim), 0) == lax.broadcasted_iota(jnp.int32, (BLOCK, dim), 1)
    lane = lax.broadcasted_iota(jnp.int32, (8, dim), 1)
    lane_group = lane // 8
    eye_line = lane % 8 == lax.broadcasted_iota(jnp.int32, (8, dim), 0)
    lr = lr_ref[0]

    for i, slot in enumerate(slots):
        grad_copies, ids_copies, table_copy = copies[i]
        for copy in ids_copies + grad_copies:
            copy.wait()

        def widen(t, carry):
            for j in range(segs):
                rows = pl.ds(pl.multiple_of(t * 32, 32), 32)
                stage[j, rows, :] = grad_v[i, j, rows, :].astype(jnp.float32)
            return carry

        lax.fori_loop(0, seg_rows // 32, widen, 0)

        def add_rows(t, carry):
            base = t * UNROLL
            for u in range(UNROLL):
                for j, bank in enumerate(banks):
                    first, second = ids_s[i][2 * j][0, base + u], ids_s[i][2 * j + 1][0, base + u]
                    same = jnp.full((1, dim), first) == jnp.full((1, dim), second)
                    add_first = stage[2 * j, pl.ds(base + u, 1), :]
                    add_second = stage[2 * j + 1, pl.ds(base + u, 1), :]
                    add_second = jnp.where(same, add_first + add_second, add_second)
                    old_first = bank[pl.ds(first, 1), :]
                    old_second = bank[pl.ds(second, 1), :]
                    bank[pl.ds(first, 1), :] = old_first + add_first
                    bank[pl.ds(second, 1), :] = old_second + add_second
            return carry

        lax.fori_loop(0, (ids_s[i][segs][0, 0] + UNROLL - 1) // UNROLL, add_rows, 0)
        table_copy.wait()
        if n_carried and i == 0:
            done_copy.wait()

        def update(c, carry):
            for s in range(CHUNK // BLOCK):
                first_row = pl.multiple_of((c * (CHUNK // BLOCK) + s) * BLOCK, BLOCK)
                rows = pl.ds(first_row, BLOCK)
                grad = banks[0][rows, :]
                for bank in banks[1:]:
                    grad = grad + bank[rows, :]
                if i + 1 < n:
                    for bank in banks:
                        bank[rows, :] = zero
                old = jnp.where(eye, accums_ref[slot:slot + 1, rows], 0.0)
                new = jnp.sum(grad * grad * (1.0 / dim) + old, axis=1, keepdims=True)
                line = jnp.broadcast_to(new[:8], (8, dim))
                for k in range(1, BLOCK // 8):
                    line = jnp.where(lane_group == k, new[8 * k:8 * k + 8], line)
                done_v[slot:slot + 1, rows] = jnp.sum(jnp.where(eye_line, line, 0.0), axis=0, keepdims=True)
                root = lax.rsqrt(jnp.maximum(new, TINY))
                scale = lr * root / (1.0 + EPSILON * root)
                table_v[i, rows, :] = (table_v[i, rows, :].astype(jnp.float32) - grad * scale).astype(jnp.bfloat16)
            done = pl.ds(pl.multiple_of(c * CHUNK, CHUNK), CHUNK)
            pltpu.make_async_copy(table_v.at[i, done], out_tables_ref.at[slot, done], out_sem.at[i]).start()
            if i == n - 1:
                pltpu.make_async_copy(done_v.at[:, done], out_accums_ref.at[:, done], out_sem.at[n]).start()
            return carry

        lax.fori_loop(0, n_rows // CHUNK, update, 0)
    for i, slot in enumerate(slots):
        pltpu.make_async_copy(table_v.at[i], out_tables_ref.at[slot], out_sem.at[i]).wait()
    pltpu.make_async_copy(done_v, out_accums_ref, out_sem.at[n]).wait()


def apply_slots(slots, ids, lr, grads, tables, accums, carried):
    _, n_rows, dim = tables.shape
    n, segs = len(slots), (len(grads) if len(grads) > 1 else grads[0].shape[0])
    seg_rows = grads[0].shape[-2]
    part = (ids[0].shape[1] - BLOCK) // segs
    assert segs == 2 * BANKS
    return pl.pallas_call(
        functools.partial(apply_kernel, slots, len(carried), len(grads)),
        out_shape=tuple(jax.ShapeDtypeStruct(x.shape, x.dtype) for x in (tables, accums)),
        in_specs=[pl.BlockSpec(memory_space=pltpu.SMEM)]
        + [pl.BlockSpec(memory_space=pl.ANY), pl.BlockSpec(memory_space=pltpu.VMEM)]
        + [pl.BlockSpec(memory_space=pl.ANY)] * (len(grads) + n)
        + [pl.BlockSpec(memory_space=pl.ANY)] * len(carried),
        out_specs=(pl.BlockSpec(memory_space=pl.ANY),) * 2,
        input_output_aliases={3 + len(grads) + n + i: i for i in range(len(carried))},
        scratch_shapes=[pltpu.VMEM((n_rows + 8, dim), jnp.float32)] * BANKS
        + [
            pltpu.VMEM((segs, seg_rows, dim), jnp.float32),
            pltpu.VMEM((n, n_rows, dim), tables.dtype),
            pltpu.VMEM((n, segs, seg_rows, dim), grads[0].dtype),
            pltpu.VMEM(accums.shape, accums.dtype),
            pltpu.SemaphoreType.DMA((n,)),
            pltpu.SemaphoreType.DMA((n + 1,)),
            pltpu.SemaphoreType.DMA((n, segs + 1)),
            pltpu.SemaphoreType.DMA((n, segs)),
        ]
        + ([pltpu.SMEM((1, part), jnp.int32)] * segs + [pltpu.SMEM((1, BLOCK), jnp.int32)]) * n,
        compiler_params=pltpu.CompilerParams(vmem_limit_bytes=VMEM_LIMIT),
        cost_estimate=pl.CostEstimate(flops=n * n_rows * dim * 400, bytes_accessed=4 * n * n_rows * dim * 2, transcendentals=0),
    )(lr, tables, accums, *grads, *(ids[k] for k in slots), *carried)


def routes(n_dev, n_slots, n_tab, slot, offset):
    pairs = [(d, (d + offset) % n_dev) for d in range(n_dev)]
    return [(src, dst) for src, dst in pairs if dst * n_slots + slot < n_tab]


def solution(mesh):
    n_group = mesh.shape['mp']
    slot_spec = P(('pod', 'mp'))

    def local_step(d_pool, row_ids, lengths, tables, row_accum, learn_rate):
        n_slots, n_rows, _ = tables.shape
        by_table = jnp.transpose(d_pool, (1, 0, 2))
        part = by_table.shape[1]
        me = lax.axis_index('mp').reshape(1)
        n_tab = by_table.shape[0]
        plan_out = make_plan(lengths, n_group)
        caps = CAPS(part)
        plan, starts, level = share_plan(plan_out, caps)
        lr = learn_rate.reshape(1)

        def exchange(level):
            def run(operands):
                me, by_table, plan, starts, row_ids, lengths, lr, tables, accums = operands
                got = {}
                chunks, hop_slots = CHUNKS(n_slots)
                for c, slots in enumerate(chunks):
                    if slots == hop_slots:
                        pack = pack_hops(slots[0], caps[level], me, starts, plan, by_table)
                    else:
                        pack = pack_slots(slots, caps[level], starts, plan, by_table)
                    if slots == hop_slots:
                        hops = []
                        for o in range(1, n_group):
                            hops.append(lax.ppermute(pack[o], 'mp', routes(n_group, n_slots, n_tab, slots[0], o)))
                        got[c] = [pack[0]] + hops
                    else:
                        got[c] = [lax.all_to_all(pack, 'mp', 0, 0, tiled=True)]
                ids = pack_ids(me, row_ids[:, :, 0], lengths, n_group, n_rows, hop_slots)
                carried = ()
                for c, slots in enumerate(chunks):
                    carried = apply_slots(slots, ids, lr, got[c], tables, accums, carried)
                return tuple(carried)

            return run

        operands = (me, by_table, plan, starts, row_ids, lengths, lr, tables, row_accum)
        return lax.switch(level[0], [exchange(i) for i in range(len(caps))], operands)

    return jax.shard_map(local_step, mesh=mesh, in_specs=(slot_spec, slot_spec, slot_spec, slot_spec, slot_spec, P()), out_specs=(slot_spec, slot_spec), check_vma=False)


def CAPS(part):
    return part * 35 // 64, part * 37 // 64, part


def CHUNKS(n_slots):
    return tuple((k,) for k in range(n_slots)), (n_slots - 2,)
```

```python
import functools

import jax
import jax.numpy as jnp
from jax import lax
from jax.experimental import pallas as pl
from jax.experimental.pallas import tpu as pltpu
from jax.sharding import PartitionSpec as P


EPSILON = 1e-06
TINY = 1e-36
BANKS = 4
UNROLL = 16
BLOCK = 128
CHUNK = 1024
CLEAR = 512
MAX_LANE = 64
VMEM_LIMIT = 66000000


def gather_parts(src_ref, dst, n_dev):
    n_slots, batch = src_ref.shape
    part = batch // n_dev
    for d in range(n_dev):
        dst[d * n_slots:(d + 1) * n_slots, :] = src_ref[:, d * part:(d + 1) * part]


def block_prefix(len_v, b, prefix):
    valid = len_v[:, b * BLOCK:(b + 1) * BLOCK] > 0
    ones = jnp.where(valid, 1.0, 0.0)
    local = jnp.dot(ones.astype(jnp.bfloat16), prefix, preferred_element_type=jnp.float32).astype(jnp.int32)
    return valid, local, jnp.sum(ones, axis=1, keepdims=True).astype(jnp.int32)


def prefix_matrix():
    below = lax.broadcasted_iota(jnp.int32, (BLOCK, BLOCK), 0) < lax.broadcasted_iota(jnp.int32, (BLOCK, BLOCK), 1)
    return jnp.where(below, 1.0, 0.0).astype(jnp.bfloat16)


def ids_kernel(n_dev, n_rows, hop_slots, me_ref, ids_ref, lengths_ref, *refs):
    *packed_refs, ids_v, len_v = refs
    n_slots, batch = ids_ref.shape
    part, rows = batch // n_dev, n_dev * n_slots
    gather_parts(ids_ref, ids_v, n_dev)
    gather_parts(lengths_ref, len_v, n_dev)
    prefix = prefix_matrix()
    lane = lax.broadcasted_iota(jnp.int32, (rows, BLOCK), 1)
    count = jnp.zeros((rows, 1), jnp.int32)
    moves = []
    for b in range(part // BLOCK):
        valid, local, more = block_prefix(len_v, b, prefix)
        shift = (b * BLOCK + lane) - (count + local)
        moves.append(jnp.where(valid, (shift << 16) | ids_v[:, b * BLOCK:(b + 1) * BLOCK], n_rows))
        count = count + more
    move = jnp.concatenate(moves, axis=1)
    step = 1
    while step < part:
        come = pltpu.roll(move, part - step, 1)
        bit = step << 16
        stay = jnp.where((move & bit) != 0, n_rows, move)
        move = jnp.where((come & bit) != 0, come, stay)
        step *= 2
    spot = lax.broadcasted_iota(jnp.int32, (rows, part), 1)
    ids_v[...] = jnp.where(spot < count, move & 0xFFFF, n_rows)
    most = jnp.max(count, axis=0, keepdims=True)
    for s in range(n_slots):
        for d in range(n_dev):
            sender = (me_ref[0] + (n_dev - d)) % n_dev if s in hop_slots else d
            packed_refs[s][:, d * part:(d + 1) * part] = ids_v[pl.ds(sender * n_slots + s, 1), :]
        packed_refs[s][:, n_dev * part:] = jnp.broadcast_to(most, (1, BLOCK))


def pack_ids(me, ids, lengths, n_dev, n_rows, hop_slots):
    n_slots, batch = ids.shape
    part = batch // n_dev
    assert n_rows < 1 << 15 and part <= 1 << 15
    return pl.pallas_call(
        functools.partial(ids_kernel, n_dev, n_rows, hop_slots),
        out_shape=(jax.ShapeDtypeStruct((1, batch + BLOCK), jnp.int32),) * n_slots,
        in_specs=[pl.BlockSpec(memory_space=pltpu.SMEM)] + [pl.BlockSpec(memory_space=pltpu.VMEM)] * 2,
        out_specs=(pl.BlockSpec(memory_space=pltpu.VMEM),) * n_slots,
        scratch_shapes=[pltpu.VMEM((n_dev * n_slots, part), jnp.int32)] * 2,
        compiler_params=pltpu.CompilerParams(vmem_limit_bytes=32000000),
        cost_estimate=pl.CostEstimate(flops=20000000, bytes_accessed=2000000, transcendentals=0),
    )(me, ids, lengths)


def write_plan(lengths_ref, plan_ref, len_v):
    n_dev, n_slots, width = plan_ref.shape
    part, rows = width - BLOCK, n_dev * n_slots
    gather_parts(lengths_ref, len_v, n_dev)
    prefix = prefix_matrix()
    lane = lax.broadcasted_iota(jnp.int32, (rows, BLOCK), 1)
    count = jnp.zeros((rows, 1), jnp.int32)
    starts = jnp.zeros((rows, BLOCK), jnp.int32)
    for b in range(part // BLOCK):
        valid, local, more = block_prefix(len_v, b, prefix)
        place = jnp.where(valid, local, -1)
        for d in range(n_dev):
            plan_ref[d, :, b * BLOCK:(b + 1) * BLOCK] = place[d * n_slots:(d + 1) * n_slots, :]
        starts = jnp.where(lane == b, count, starts)
        count = count + more
    starts = jnp.where(lane == MAX_LANE, jnp.max(count, axis=0, keepdims=True), starts)
    for d in range(n_dev):
        plan_ref[d, :, part:] = starts[d * n_slots:(d + 1) * n_slots, :]


def plan_kernel(n_dev, caps, lengths_ref, plans_ref, starts_ref, level_ref, plan_ref, len_v, send_sem, recv_sem, own_sem):
    pod, me = lax.axis_index('pod'), lax.axis_index('mp')
    barrier = pltpu.get_barrier_semaphore()
    for o in range(1, n_dev):
        pl.semaphore_signal(barrier, inc=1, device_id=(pod, (me + o) % n_dev), device_id_type=pl.DeviceIdType.MESH)
    write_plan(lengths_ref, plan_ref, len_v)
    pl.semaphore_wait(barrier, n_dev - 1)
    copies = [
        pltpu.make_async_remote_copy(
            src_ref=plan_ref.at[(me + o) % n_dev],
            dst_ref=plans_ref.at[me],
            send_sem=send_sem.at[o],
            recv_sem=recv_sem.at[o],
            device_id=(pod, (me + o) % n_dev),
            device_id_type=pl.DeviceIdType.MESH,
        )
        for o in range(1, n_dev)
    ]
    for copy in copies:
        copy.start()
    own = pltpu.make_async_copy(plan_ref.at[me], plans_ref.at[me], own_sem)
    own.start()
    own.wait()
    for copy in copies:
        copy.wait()
    part = plans_ref.shape[2] - BLOCK
    starts = plans_ref[:, :, part:]
    starts_ref[...] = starts
    most = jnp.max(starts[:, :, MAX_LANE:MAX_LANE + 1])
    level_ref[0] = sum((most > cap).astype(jnp.int32) for cap in caps[:-1])


def make_plan(lengths, n_dev, caps):
    n_slots, batch = lengths.shape
    part = batch // n_dev
    plan_shape = (n_dev, n_slots, part + BLOCK)
    return pl.pallas_call(
        functools.partial(plan_kernel, n_dev, caps),
        out_shape=(
            jax.ShapeDtypeStruct(plan_shape, jnp.int32),
            jax.ShapeDtypeStruct((n_dev, n_slots, BLOCK), jnp.int32),
            jax.ShapeDtypeStruct((1,), jnp.int32),
        ),
        in_specs=[pl.BlockSpec(memory_space=pltpu.VMEM)],
        out_specs=(pl.BlockSpec(memory_space=pltpu.VMEM), pl.BlockSpec(memory_space=pltpu.VMEM), pl.BlockSpec(memory_space=pltpu.SMEM)),
        scratch_shapes=[
            pltpu.VMEM(plan_shape, jnp.int32),
            pltpu.VMEM((n_dev * n_slots, part), jnp.int32),
            pltpu.SemaphoreType.DMA((n_dev,)),
            pltpu.SemaphoreType.DMA((n_dev,)),
            pltpu.SemaphoreType.DMA,
        ],
        compiler_params=pltpu.CompilerParams(collective_id=0, has_side_effects=True, vmem_limit_bytes=16000000),
        cost_estimate=pl.CostEstimate(flops=20000000, bytes_accessed=2000000, transcendentals=0),
    )(lengths)


def pack_kernel(slots, starts_ref, plan_ref, tables_ref, out_ref, grad_v, stage, pack_v, in_sem, out_sem):
    n_slots = plan_ref.shape[1]
    cap = out_ref.shape[2]
    n_tab, part, _ = tables_ref.shape
    slot_row = lax.broadcasted_iota(jnp.int32, (BLOCK, BLOCK), 0)
    used = [[d for d in range(out_ref.shape[0]) if d * n_slots + slot < n_tab] for slot in slots]

    def fetch(i, d):
        return pltpu.make_async_copy(tables_ref.at[d * n_slots + slots[i]], grad_v.at[i, d], in_sem.at[i, d])

    def emit(i, d):
        return pltpu.make_async_copy(pack_v.at[i, d], out_ref.at[d, i], out_sem.at[i, d])

    for i, dests in enumerate(used):
        for d in dests:
            fetch(i, d).start()
    for i, dests in enumerate(used):
        def table(d, carry):
            fetch(i, d).wait()
            for b in range(part // BLOCK):
                place = plan_ref[d, slots[i]:slots[i] + 1, b * BLOCK:(b + 1) * BLOCK]
                pick = jnp.where(slot_row == place, 1.0, 0.0).astype(jnp.bfloat16)
                rows = jnp.dot(pick, grad_v[i, d, b * BLOCK:(b + 1) * BLOCK, :], preferred_element_type=jnp.float32)
                stage[pl.ds(starts_ref[d, slots[i], b], BLOCK), :] = rows
            pack_v[i, d] = stage[:cap, :].astype(jnp.bfloat16)
            emit(i, d).start()
            return carry

        lax.fori_loop(0, len(dests), table, 0)
    for i, dests in enumerate(used):
        for d in dests:
            emit(i, d).wait()


def pack_slots(slots, cap, starts, plan, by_table):
    n_dev = plan.shape[0]
    _, part, dim = by_table.shape
    n = len(slots)
    return pl.pallas_call(
        functools.partial(pack_kernel, slots),
        out_shape=jax.ShapeDtypeStruct((n_dev, n, cap, dim), by_table.dtype),
        in_specs=[pl.BlockSpec(memory_space=pltpu.SMEM), pl.BlockSpec(memory_space=pltpu.VMEM), pl.BlockSpec(memory_space=pl.ANY)],
        out_specs=pl.BlockSpec(memory_space=pl.ANY),
        scratch_shapes=[
            pltpu.VMEM((n, n_dev, part, dim), by_table.dtype),
            pltpu.VMEM((cap + BLOCK, dim), jnp.float32),
            pltpu.VMEM((n, n_dev, cap, dim), by_table.dtype),
            pltpu.SemaphoreType.DMA((n, n_dev)),
            pltpu.SemaphoreType.DMA((n, n_dev)),
        ],
        compiler_params=pltpu.CompilerParams(vmem_limit_bytes=VMEM_LIMIT),
        cost_estimate=pl.CostEstimate(flops=n * n_dev * part * dim * 20, bytes_accessed=n * n_dev * part * dim * 3, transcendentals=0),
    )(starts, plan, by_table)


def pack_hops_kernel(slot, me_ref, starts_ref, plan_ref, tables_ref, *refs):
    n_dev, n_slots, _ = plan_ref.shape
    n_tab, part, _ = tables_ref.shape
    out_refs, (grad_v, stage, pack_v, in_sem, out_sem) = refs[:n_dev], refs[n_dev:]
    cap = pack_v.shape[1]
    slot_row = lax.broadcasted_iota(jnp.int32, (BLOCK, BLOCK), 0)
    me = me_ref[0]

    def fetch(o):
        table = jnp.minimum((me + o) % n_dev * n_slots + slot, n_tab - 1)
        return pltpu.make_async_copy(tables_ref.at[table], grad_v.at[o], in_sem.at[o])

    for o in range(n_dev):
        fetch(o).start()

    def one(o, carry):
        d = (me + o) % n_dev
        fetch(o).wait()

        @pl.when(d * n_slots + slot < n_tab)
        def _():
            for b in range(part // BLOCK):
                place = plan_ref[d, slot:slot + 1, b * BLOCK:(b + 1) * BLOCK]
                pick = jnp.where(slot_row == place, 1.0, 0.0).astype(jnp.bfloat16)
                rows = jnp.dot(pick, grad_v[o, b * BLOCK:(b + 1) * BLOCK, :], preferred_element_type=jnp.float32)
                stage[pl.ds(starts_ref[d, slot, b], BLOCK), :] = rows
            pack_v[o] = stage[:cap, :].astype(jnp.bfloat16)

        return carry

    lax.fori_loop(0, n_dev, one, 0)
    copies = [pltpu.make_async_copy(pack_v.at[o], out_refs[o], out_sem.at[o]) for o in range(n_dev)]
    for copy in copies:
        copy.start()
    for copy in copies:
        copy.wait()


def pack_hops(slot, cap, me, starts, plan, by_table):
    n_dev, _, _ = plan.shape
    _, part, dim = by_table.shape
    return pl.pallas_call(
        functools.partial(pack_hops_kernel, slot),
        out_shape=(jax.ShapeDtypeStruct((cap, dim), by_table.dtype),) * n_dev,
        in_specs=[pl.BlockSpec(memory_space=pltpu.SMEM)] * 2 + [pl.BlockSpec(memory_space=pltpu.VMEM), pl.BlockSpec(memory_space=pl.ANY)],
        out_specs=(pl.BlockSpec(memory_space=pl.ANY),) * n_dev,
        scratch_shapes=[
            pltpu.VMEM((n_dev, part, dim), by_table.dtype),
            pltpu.VMEM((cap + BLOCK, dim), jnp.float32),
            pltpu.VMEM((n_dev, cap, dim), by_table.dtype),
            pltpu.SemaphoreType.DMA((n_dev,)),
            pltpu.SemaphoreType.DMA((n_dev,)),
        ],
        compiler_params=pltpu.CompilerParams(vmem_limit_bytes=VMEM_LIMIT),
        cost_estimate=pl.CostEstimate(flops=n_dev * part * dim * 20, bytes_accessed=n_dev * part * dim * 3, transcendentals=0),
    )(me, starts, plan, by_table)


def apply_kernel(slots, n_carried, n_grads, lr_ref, tables_ref, accums_ref, *refs):
    n = len(slots)
    grad_refs, refs = refs[:n_grads], refs[n_grads:]
    ids_refs, carried_refs = refs[:n], refs[n:n + n_carried]
    out_tables_ref, out_accums_ref, *scratch = refs[n + n_carried:]
    banks, (stage, table_v, grad_v, done_v, sem, out_sem, ids_sem, grad_sem), scalars = scratch[:BANKS], scratch[BANKS:BANKS + 8], scratch[BANKS + 8:]
    _, segs, seg_rows, dim = grad_v.shape
    part = (ids_refs[0].shape[1] - BLOCK) // segs
    ids_s = [scalars[i * (segs + 1):(i + 1) * (segs + 1)] for i in range(n)]
    n_rows = tables_ref.shape[1]
    copies = [
        (
            [pltpu.make_async_copy(ref, grad_v.at[i, o], grad_sem.at[i, o]) for o, ref in enumerate(grad_refs)]
            if n_grads > 1
            else [pltpu.make_async_copy(grad_refs[0].at[:, i], grad_v.at[i], grad_sem.at[i, 0])],
            [pltpu.make_async_copy(ids_refs[i].at[:, j * part:(j + 1) * part], ids_s[i][j], ids_sem.at[i, j]) for j in range(segs)]
            + [pltpu.make_async_copy(ids_refs[i].at[:, segs * part:], ids_s[i][segs], ids_sem.at[i, segs])],
            pltpu.make_async_copy(tables_ref.at[slot], table_v.at[i], sem.at[i]),
        )
        for i, slot in enumerate(slots)
    ]
    for grad_copies, ids_copies, table_copy in copies:
        for copy in ids_copies + grad_copies:
            copy.start()
        table_copy.start()

    if n_carried:
        done_copy = pltpu.make_async_copy(carried_refs[1], done_v, out_sem.at[n])
        done_copy.start()
    zero = jnp.zeros((BLOCK, dim), jnp.float32)

    def clear(i, carry):
        for bank in banks:
            for s in range(CLEAR // BLOCK):
                bank[pl.ds(pl.multiple_of(i * CLEAR, CLEAR) + s * BLOCK, BLOCK), :] = zero
        return carry

    lax.fori_loop(0, n_rows // CLEAR, clear, 0)
    for bank in banks:
        bank[pl.ds(n_rows, 8), :] = zero[:8]
    eye = lax.broadcasted_iota(jnp.int32, (BLOCK, dim), 0) == lax.broadcasted_iota(jnp.int32, (BLOCK, dim), 1)
    lane = lax.broadcasted_iota(jnp.int32, (8, dim), 1)
    lane_group = lane // 8
    eye_line = lane % 8 == lax.broadcasted_iota(jnp.int32, (8, dim), 0)
    lr = lr_ref[0]

    for i, slot in enumerate(slots):
        grad_copies, ids_copies, table_copy = copies[i]
        for copy in ids_copies + grad_copies:
            copy.wait()

        def widen(t, carry):
            for j in range(segs):
                rows = pl.ds(pl.multiple_of(t * 32, 32), 32)
                stage[j, rows, :] = grad_v[i, j, rows, :].astype(jnp.float32)
            return carry

        lax.fori_loop(0, seg_rows // 32, widen, 0)

        def add_rows(t, carry):
            base = t * UNROLL
            for u in range(UNROLL):
                for j, bank in enumerate(banks):
                    first, second = ids_s[i][2 * j][0, base + u], ids_s[i][2 * j + 1][0, base + u]
                    same = jnp.full((1, dim), first) == jnp.full((1, dim), second)
                    add_first = stage[2 * j, pl.ds(base + u, 1), :]
                    add_second = stage[2 * j + 1, pl.ds(base + u, 1), :]
                    add_second = jnp.where(same, add_first + add_second, add_second)
                    old_first = bank[pl.ds(first, 1), :]
                    old_second = bank[pl.ds(second, 1), :]
                    bank[pl.ds(first, 1), :] = old_first + add_first
                    bank[pl.ds(second, 1), :] = old_second + add_second
            return carry

        lax.fori_loop(0, (ids_s[i][segs][0, 0] + UNROLL - 1) // UNROLL, add_rows, 0)
        table_copy.wait()
        if n_carried and i == 0:
            done_copy.wait()

        def update(c, carry):
            for s in range(CHUNK // BLOCK):
                first_row = pl.multiple_of((c * (CHUNK // BLOCK) + s) * BLOCK, BLOCK)
                rows = pl.ds(first_row, BLOCK)
                grad = banks[0][rows, :]
                for bank in banks[1:]:
                    grad = grad + bank[rows, :]
                if i + 1 < n:
                    for bank in banks:
                        bank[rows, :] = zero
                old = jnp.where(eye, accums_ref[slot:slot + 1, rows], 0.0)
                new = jnp.sum(grad * grad * (1.0 / dim) + old, axis=1, keepdims=True)
                line = jnp.broadcast_to(new[:8], (8, dim))
                for k in range(1, BLOCK // 8):
                    line = jnp.where(lane_group == k, new[8 * k:8 * k + 8], line)
                done_v[slot:slot + 1, rows] = jnp.sum(jnp.where(eye_line, line, 0.0), axis=0, keepdims=True)
                root = lax.rsqrt(jnp.maximum(new, TINY))
                scale = lr * root / (1.0 + EPSILON * root)
                table_v[i, rows, :] = (table_v[i, rows, :].astype(jnp.float32) - grad * scale).astype(jnp.bfloat16)
            done = pl.ds(pl.multiple_of(c * CHUNK, CHUNK), CHUNK)
            pltpu.make_async_copy(table_v.at[i, done], out_tables_ref.at[slot, done], out_sem.at[i]).start()
            if i == n - 1:
                pltpu.make_async_copy(done_v.at[:, done], out_accums_ref.at[:, done], out_sem.at[n]).start()
            return carry

        lax.fori_loop(0, n_rows // CHUNK, update, 0)
    for i, slot in enumerate(slots):
        pltpu.make_async_copy(table_v.at[i], out_tables_ref.at[slot], out_sem.at[i]).wait()
    pltpu.make_async_copy(done_v, out_accums_ref, out_sem.at[n]).wait()


def apply_slots(slots, ids, lr, grads, tables, accums, carried):
    _, n_rows, dim = tables.shape
    n, segs = len(slots), (len(grads) if len(grads) > 1 else grads[0].shape[0])
    seg_rows = grads[0].shape[-2]
    part = (ids[0].shape[1] - BLOCK) // segs
    assert segs == 2 * BANKS
    return pl.pallas_call(
        functools.partial(apply_kernel, slots, len(carried), len(grads)),
        out_shape=tuple(jax.ShapeDtypeStruct(x.shape, x.dtype) for x in (tables, accums)),
        in_specs=[pl.BlockSpec(memory_space=pltpu.SMEM)]
        + [pl.BlockSpec(memory_space=pl.ANY), pl.BlockSpec(memory_space=pltpu.VMEM)]
        + [pl.BlockSpec(memory_space=pl.ANY)] * (len(grads) + n)
        + [pl.BlockSpec(memory_space=pl.ANY)] * len(carried),
        out_specs=(pl.BlockSpec(memory_space=pl.ANY),) * 2,
        input_output_aliases={3 + len(grads) + n + i: i for i in range(len(carried))},
        scratch_shapes=[pltpu.VMEM((n_rows + 8, dim), jnp.float32)] * BANKS
        + [
            pltpu.VMEM((segs, seg_rows, dim), jnp.float32),
            pltpu.VMEM((n, n_rows, dim), tables.dtype),
            pltpu.VMEM((n, segs, seg_rows, dim), grads[0].dtype),
            pltpu.VMEM(accums.shape, accums.dtype),
            pltpu.SemaphoreType.DMA((n,)),
            pltpu.SemaphoreType.DMA((n + 1,)),
            pltpu.SemaphoreType.DMA((n, segs + 1)),
            pltpu.SemaphoreType.DMA((n, segs)),
        ]
        + ([pltpu.SMEM((1, part), jnp.int32)] * segs + [pltpu.SMEM((1, BLOCK), jnp.int32)]) * n,
        compiler_params=pltpu.CompilerParams(vmem_limit_bytes=VMEM_LIMIT),
        cost_estimate=pl.CostEstimate(flops=n * n_rows * dim * 400, bytes_accessed=4 * n * n_rows * dim * 2, transcendentals=0),
    )(lr, tables, accums, *grads, *(ids[k] for k in slots), *carried)


def routes(n_dev, n_slots, n_tab, slot, offset):
    pairs = [(d, (d + offset) % n_dev) for d in range(n_dev)]
    return [(src, dst) for src, dst in pairs if dst * n_slots + slot < n_tab]


def solution(mesh):
    n_group = mesh.shape['mp']
    slot_spec = P(('pod', 'mp'))

    def local_step(d_pool, row_ids, lengths, tables, row_accum, learn_rate):
        n_slots, n_rows, _ = tables.shape
        by_table = jnp.transpose(d_pool, (1, 0, 2))
        part = by_table.shape[1]
        me = lax.axis_index('mp').reshape(1)
        n_tab = by_table.shape[0]
        caps = CAPS(part)
        plan, starts, level = make_plan(lengths, n_group, caps)
        lr = learn_rate.reshape(1)

        def exchange(level):
            def run(operands):
                me, by_table, plan, starts, row_ids, lengths, lr, tables, accums = operands
                got = {}
                chunks, hop_slots = CHUNKS(n_slots)
                for c, slots in enumerate(chunks):
                    if slots == hop_slots:
                        pack = pack_hops(slots[0], caps[level], me, starts, plan, by_table)
                    else:
                        pack = pack_slots(slots, caps[level], starts, plan, by_table)
                    if slots == hop_slots:
                        hops = []
                        for o in range(1, n_group):
                            hops.append(lax.ppermute(pack[o], 'mp', routes(n_group, n_slots, n_tab, slots[0], o)))
                        got[c] = [pack[0]] + hops
                    else:
                        got[c] = [lax.all_to_all(pack, 'mp', 0, 0, tiled=True)]
                ids = pack_ids(me, row_ids[:, :, 0], lengths, n_group, n_rows, hop_slots)
                carried = ()
                for c, slots in enumerate(chunks):
                    carried = apply_slots(slots, ids, lr, got[c], tables, accums, carried)
                return tuple(carried)

            return run

        operands = (me, by_table, plan, starts, row_ids, lengths, lr, tables, row_accum)
        return lax.switch(level[0], [exchange(i) for i in range(len(caps))], operands)

    return jax.shard_map(local_step, mesh=mesh, in_specs=(slot_spec, slot_spec, slot_spec, slot_spec, slot_spec, P()), out_specs=(slot_spec, slot_spec), check_vma=False)


def CAPS(part):
    return part * 35 // 64, part * 37 // 64, part


def CHUNKS(n_slots):
    return tuple((k,) for k in range(n_slots)), (n_slots - 2,)
```

```python
import functools

import jax
import jax.numpy as jnp
from jax import lax
from jax.experimental import pallas as pl
from jax.experimental.pallas import tpu as pltpu
from jax.sharding import PartitionSpec as P


EPSILON = 1e-06
TINY = 1e-36
BANKS = 4
UNROLL = 16
BLOCK = 128
CHUNK = 1024
CLEAR = 512
MAX_LANE = 64
VMEM_LIMIT = 67000000


def gather_parts(src_ref, dst, n_dev):
    n_slots, batch = src_ref.shape
    part = batch // n_dev
    for d in range(n_dev):
        dst[d * n_slots:(d + 1) * n_slots, :] = src_ref[:, d * part:(d + 1) * part]


def block_prefix(len_v, b, prefix):
    valid = len_v[:, b * BLOCK:(b + 1) * BLOCK] > 0
    ones = jnp.where(valid, 1.0, 0.0)
    local = jnp.dot(ones.astype(jnp.bfloat16), prefix, preferred_element_type=jnp.float32).astype(jnp.int32)
    return valid, local, jnp.sum(ones, axis=1, keepdims=True).astype(jnp.int32)


def prefix_matrix():
    below = lax.broadcasted_iota(jnp.int32, (BLOCK, BLOCK), 0) < lax.broadcasted_iota(jnp.int32, (BLOCK, BLOCK), 1)
    return jnp.where(below, 1.0, 0.0).astype(jnp.bfloat16)


def ids_kernel(n_dev, n_rows, hop_slots, me_ref, ids_ref, lengths_ref, *refs):
    n_slots, batch = ids_ref.shape
    out_refs, packed_refs, (ids_v, len_v, sem) = refs[:n_slots], refs[n_slots:2 * n_slots], refs[2 * n_slots:]
    part, rows = batch // n_dev, n_dev * n_slots
    gather_parts(ids_ref, ids_v, n_dev)
    gather_parts(lengths_ref, len_v, n_dev)
    prefix = prefix_matrix()
    lane = lax.broadcasted_iota(jnp.int32, (rows, BLOCK), 1)
    count = jnp.zeros((rows, 1), jnp.int32)
    moves = []
    for b in range(part // BLOCK):
        valid, local, more = block_prefix(len_v, b, prefix)
        shift = (b * BLOCK + lane) - (count + local)
        moves.append(jnp.where(valid, (shift << 16) | ids_v[:, b * BLOCK:(b + 1) * BLOCK], n_rows))
        count = count + more
    move = jnp.concatenate(moves, axis=1)
    step = 1
    while step < part:
        come = pltpu.roll(move, part - step, 1)
        bit = step << 16
        stay = jnp.where((move & bit) != 0, n_rows, move)
        move = jnp.where((come & bit) != 0, come, stay)
        step *= 2
    spot = lax.broadcasted_iota(jnp.int32, (rows, part), 1)
    ids_v[...] = jnp.where(spot < count, move & 0xFFFF, n_rows)
    slot_of = lax.broadcasted_iota(jnp.int32, (rows, 1), 0) % n_slots
    for s in range(n_slots):
        most = jnp.max(jnp.where(slot_of == s, count, 0), axis=0, keepdims=True)
        for d in range(n_dev):
            sender = (me_ref[0] + (n_dev - d)) % n_dev if s in hop_slots else d
            packed_refs[s][:, d * part:(d + 1) * part] = ids_v[pl.ds(sender * n_slots + s, 1), :]
        packed_refs[s][:, n_dev * part:] = jnp.broadcast_to(most, (1, BLOCK))
        pltpu.make_async_copy(packed_refs[s], out_refs[s], sem.at[s]).start()
    for s in range(n_slots):
        pltpu.make_async_copy(packed_refs[s], out_refs[s], sem.at[s]).wait()


def pack_ids(me, ids, lengths, n_dev, n_rows, hop_slots):
    n_slots, batch = ids.shape
    part = batch // n_dev
    assert n_rows < 1 << 15 and part <= 1 << 15
    return pl.pallas_call(
        functools.partial(ids_kernel, n_dev, n_rows, hop_slots),
        out_shape=(jax.ShapeDtypeStruct((1, batch + BLOCK), jnp.int32),) * n_slots,
        in_specs=[pl.BlockSpec(memory_space=pltpu.SMEM)] + [pl.BlockSpec(memory_space=pltpu.VMEM)] * 2,
        out_specs=(pl.BlockSpec(memory_space=pl.ANY),) * n_slots,
        scratch_shapes=[pltpu.VMEM((1, batch + BLOCK), jnp.int32)] * n_slots
        + [pltpu.VMEM((n_dev * n_slots, part), jnp.int32)] * 2
        + [pltpu.SemaphoreType.DMA((n_slots,))],
        compiler_params=pltpu.CompilerParams(vmem_limit_bytes=VMEM_LIMIT),
        cost_estimate=pl.CostEstimate(flops=20000000, bytes_accessed=2000000, transcendentals=0),
    )(me, ids, lengths)


def write_plan(lengths_ref, plan_ref, len_v):
    n_dev, n_slots, width = plan_ref.shape
    part, rows = width - BLOCK, n_dev * n_slots
    gather_parts(lengths_ref, len_v, n_dev)
    prefix = prefix_matrix()
    lane = lax.broadcasted_iota(jnp.int32, (rows, BLOCK), 1)
    count = jnp.zeros((rows, 1), jnp.int32)
    starts = jnp.zeros((rows, BLOCK), jnp.int32)
    for b in range(part // BLOCK):
        valid, local, more = block_prefix(len_v, b, prefix)
        place = jnp.where(valid, local, -1)
        for d in range(n_dev):
            plan_ref[d, :, b * BLOCK:(b + 1) * BLOCK] = place[d * n_slots:(d + 1) * n_slots, :]
        starts = jnp.where(lane == b, count, starts)
        count = count + more
    starts = jnp.where(lane == MAX_LANE, jnp.max(count, axis=0, keepdims=True), starts)
    for d in range(n_dev):
        plan_ref[d, :, part:] = starts[d * n_slots:(d + 1) * n_slots, :]


def plan_kernel(n_dev, caps, lengths_ref, plans_ref, starts_ref, level_ref, plan_ref, len_v, send_sem, recv_sem, own_sem):
    pod, me = lax.axis_index('pod'), lax.axis_index('mp')
    barrier = pltpu.get_barrier_semaphore()
    for o in range(1, n_dev):
        pl.semaphore_signal(barrier, inc=1, device_id=(pod, (me + o) % n_dev), device_id_type=pl.DeviceIdType.MESH)
    write_plan(lengths_ref, plan_ref, len_v)
    pl.semaphore_wait(barrier, n_dev - 1)
    copies = [
        pltpu.make_async_remote_copy(
            src_ref=plan_ref.at[(me + o) % n_dev],
            dst_ref=plans_ref.at[me],
            send_sem=send_sem.at[o],
            recv_sem=recv_sem.at[o],
            device_id=(pod, (me + o) % n_dev),
            device_id_type=pl.DeviceIdType.MESH,
        )
        for o in range(1, n_dev)
    ]
    for copy in copies:
        copy.start()
    own = pltpu.make_async_copy(plan_ref.at[me], plans_ref.at[me], own_sem)
    own.start()
    own.wait()
    for copy in copies:
        copy.wait()
    part = plans_ref.shape[2] - BLOCK
    starts = plans_ref[:, :, part:]
    starts_ref[...] = starts
    most = jnp.max(starts[:, :, MAX_LANE:MAX_LANE + 1])
    level_ref[0] = sum((most > cap).astype(jnp.int32) for cap in caps[:-1])


def make_plan(lengths, n_dev, caps):
    n_slots, batch = lengths.shape
    part = batch // n_dev
    plan_shape = (n_dev, n_slots, part + BLOCK)
    return pl.pallas_call(
        functools.partial(plan_kernel, n_dev, caps),
        out_shape=(
            jax.ShapeDtypeStruct(plan_shape, jnp.int32),
            jax.ShapeDtypeStruct((n_dev, n_slots, BLOCK), jnp.int32),
            jax.ShapeDtypeStruct((1,), jnp.int32),
        ),
        in_specs=[pl.BlockSpec(memory_space=pltpu.VMEM)],
        out_specs=(pl.BlockSpec(memory_space=pltpu.VMEM), pl.BlockSpec(memory_space=pltpu.VMEM), pl.BlockSpec(memory_space=pltpu.SMEM)),
        scratch_shapes=[
            pltpu.VMEM(plan_shape, jnp.int32),
            pltpu.VMEM((n_dev * n_slots, part), jnp.int32),
            pltpu.SemaphoreType.DMA((n_dev,)),
            pltpu.SemaphoreType.DMA((n_dev,)),
            pltpu.SemaphoreType.DMA,
        ],
        compiler_params=pltpu.CompilerParams(collective_id=0, has_side_effects=True, vmem_limit_bytes=16000000),
        cost_estimate=pl.CostEstimate(flops=20000000, bytes_accessed=2000000, transcendentals=0),
    )(lengths)


def pack_kernel(slots, starts_ref, plan_ref, tables_ref, out_ref, grad_v, stage, pack_v, in_sem, out_sem):
    n_slots = plan_ref.shape[1]
    cap = out_ref.shape[2]
    n_tab, part, _ = tables_ref.shape
    slot_row = lax.broadcasted_iota(jnp.int32, (BLOCK, BLOCK), 0)
    used = [[d for d in range(out_ref.shape[0]) if d * n_slots + slot < n_tab] for slot in slots]

    def fetch(i, d):
        return pltpu.make_async_copy(tables_ref.at[d * n_slots + slots[i]], grad_v.at[i, d], in_sem.at[i, d])

    def emit(i, d):
        return pltpu.make_async_copy(pack_v.at[i, d], out_ref.at[d, i], out_sem.at[i, d])

    for i, dests in enumerate(used):
        for d in dests:
            fetch(i, d).start()
    for i, dests in enumerate(used):
        def table(d, carry):
            fetch(i, d).wait()
            for b in range(part // BLOCK):
                place = plan_ref[d, slots[i]:slots[i] + 1, b * BLOCK:(b + 1) * BLOCK]
                pick = jnp.where(slot_row == place, 1.0, 0.0).astype(jnp.bfloat16)
                rows = jnp.dot(pick, grad_v[i, d, b * BLOCK:(b + 1) * BLOCK, :], preferred_element_type=jnp.float32)
                stage[pl.ds(starts_ref[d, slots[i], b], BLOCK), :] = rows
            pack_v[i, d] = stage[:cap, :].astype(jnp.bfloat16)
            emit(i, d).start()
            return carry

        lax.fori_loop(0, len(dests), table, 0)
    for i, dests in enumerate(used):
        for d in dests:
            emit(i, d).wait()


def pack_slots(slots, cap, starts, plan, by_table):
    n_dev = plan.shape[0]
    _, part, dim = by_table.shape
    n = len(slots)
    return pl.pallas_call(
        functools.partial(pack_kernel, slots),
        out_shape=jax.ShapeDtypeStruct((n_dev, n, cap, dim), by_table.dtype),
        in_specs=[pl.BlockSpec(memory_space=pltpu.SMEM), pl.BlockSpec(memory_space=pltpu.VMEM), pl.BlockSpec(memory_space=pl.ANY)],
        out_specs=pl.BlockSpec(memory_space=pl.ANY),
        scratch_shapes=[
            pltpu.VMEM((n, n_dev, part, dim), by_table.dtype),
            pltpu.VMEM((cap + BLOCK, dim), jnp.float32),
            pltpu.VMEM((n, n_dev, cap, dim), by_table.dtype),
            pltpu.SemaphoreType.DMA((n, n_dev)),
            pltpu.SemaphoreType.DMA((n, n_dev)),
        ],
        compiler_params=pltpu.CompilerParams(vmem_limit_bytes=VMEM_LIMIT),
        cost_estimate=pl.CostEstimate(flops=n * n_dev * part * dim * 20, bytes_accessed=n * n_dev * part * dim * 3, transcendentals=0),
    )(starts, plan, by_table)


def pack_hops_kernel(slot, me_ref, starts_ref, plan_ref, tables_ref, *refs):
    n_dev, n_slots, _ = plan_ref.shape
    n_tab, part, _ = tables_ref.shape
    out_refs, (grad_v, stage, pack_v, in_sem, out_sem) = refs[:n_dev], refs[n_dev:]
    cap = pack_v.shape[1]
    slot_row = lax.broadcasted_iota(jnp.int32, (BLOCK, BLOCK), 0)
    me = me_ref[0]

    def fetch(o):
        table = jnp.minimum((me + o) % n_dev * n_slots + slot, n_tab - 1)
        return pltpu.make_async_copy(tables_ref.at[table], grad_v.at[o], in_sem.at[o])

    for o in range(n_dev):
        fetch(o).start()

    def one(o, carry):
        d = (me + o) % n_dev
        fetch(o).wait()

        @pl.when(d * n_slots + slot < n_tab)
        def _():
            for b in range(part // BLOCK):
                place = plan_ref[d, slot:slot + 1, b * BLOCK:(b + 1) * BLOCK]
                pick = jnp.where(slot_row == place, 1.0, 0.0).astype(jnp.bfloat16)
                rows = jnp.dot(pick, grad_v[o, b * BLOCK:(b + 1) * BLOCK, :], preferred_element_type=jnp.float32)
                stage[pl.ds(starts_ref[d, slot, b], BLOCK), :] = rows
            pack_v[o] = stage[:cap, :].astype(jnp.bfloat16)

        return carry

    lax.fori_loop(0, n_dev, one, 0)
    copies = [pltpu.make_async_copy(pack_v.at[o], out_refs[o], out_sem.at[o]) for o in range(n_dev)]
    for copy in copies:
        copy.start()
    for copy in copies:
        copy.wait()


def pack_hops(slot, cap, me, starts, plan, by_table):
    n_dev, _, _ = plan.shape
    _, part, dim = by_table.shape
    return pl.pallas_call(
        functools.partial(pack_hops_kernel, slot),
        out_shape=(jax.ShapeDtypeStruct((cap, dim), by_table.dtype),) * n_dev,
        in_specs=[pl.BlockSpec(memory_space=pltpu.SMEM)] * 2 + [pl.BlockSpec(memory_space=pltpu.VMEM), pl.BlockSpec(memory_space=pl.ANY)],
        out_specs=(pl.BlockSpec(memory_space=pl.ANY),) * n_dev,
        scratch_shapes=[
            pltpu.VMEM((n_dev, part, dim), by_table.dtype),
            pltpu.VMEM((cap + BLOCK, dim), jnp.float32),
            pltpu.VMEM((n_dev, cap, dim), by_table.dtype),
            pltpu.SemaphoreType.DMA((n_dev,)),
            pltpu.SemaphoreType.DMA((n_dev,)),
        ],
        compiler_params=pltpu.CompilerParams(vmem_limit_bytes=VMEM_LIMIT),
        cost_estimate=pl.CostEstimate(flops=n_dev * part * dim * 20, bytes_accessed=n_dev * part * dim * 3, transcendentals=0),
    )(me, starts, plan, by_table)


def apply_kernel(slots, n_carried, n_grads, lr_ref, tables_ref, accums_ref, *refs):
    n = len(slots)
    grad_refs, refs = refs[:n_grads], refs[n_grads:]
    ids_refs, carried_refs = refs[:n], refs[n:n + n_carried]
    out_tables_ref, out_accums_ref, *scratch = refs[n + n_carried:]
    banks, (stage, table_v, grad_v, accum_v, done_v, sem, out_sem, ids_sem, grad_sem), scalars = scratch[:BANKS], scratch[BANKS:BANKS + 9], scratch[BANKS + 9:]
    _, segs, seg_rows, dim = grad_v.shape
    part = (ids_refs[0].shape[1] - BLOCK) // segs
    ids_s = [scalars[i * (segs + 1):(i + 1) * (segs + 1)] for i in range(n)]
    n_rows = tables_ref.shape[1]
    copies = [
        (
            [pltpu.make_async_copy(ref, grad_v.at[i, o], grad_sem.at[i, o]) for o, ref in enumerate(grad_refs)]
            if n_grads > 1
            else [pltpu.make_async_copy(grad_refs[0].at[:, i], grad_v.at[i], grad_sem.at[i, 0])],
            [pltpu.make_async_copy(ids_refs[i].at[:, j * part:(j + 1) * part], ids_s[i][j], ids_sem.at[i, j]) for j in range(segs)]
            + [pltpu.make_async_copy(ids_refs[i].at[:, segs * part:], ids_s[i][segs], ids_sem.at[i, segs])],
            pltpu.make_async_copy(tables_ref.at[slot], table_v.at[i], sem.at[i]),
        )
        for i, slot in enumerate(slots)
    ]
    for grad_copies, ids_copies, table_copy in copies:
        for copy in ids_copies + grad_copies:
            copy.start()
        table_copy.start()

    accum_copy = pltpu.make_async_copy(accums_ref, accum_v, out_sem.at[n + 1])
    accum_copy.start()
    if n_carried:
        done_copy = pltpu.make_async_copy(carried_refs[1], done_v, out_sem.at[n])
        done_copy.start()
    zero = jnp.zeros((BLOCK, dim), jnp.float32)

    def clear(i, carry):
        for bank in banks:
            for s in range(CLEAR // BLOCK):
                bank[pl.ds(pl.multiple_of(i * CLEAR, CLEAR) + s * BLOCK, BLOCK), :] = zero
        return carry

    lax.fori_loop(0, n_rows // CLEAR, clear, 0)
    for bank in banks:
        bank[pl.ds(n_rows, 8), :] = zero[:8]
    eye = lax.broadcasted_iota(jnp.int32, (BLOCK, dim), 0) == lax.broadcasted_iota(jnp.int32, (BLOCK, dim), 1)
    lane = lax.broadcasted_iota(jnp.int32, (8, dim), 1)
    lane_group = lane // 8
    eye_line = lane % 8 == lax.broadcasted_iota(jnp.int32, (8, dim), 0)
    lr = lr_ref[0]

    for i, slot in enumerate(slots):
        grad_copies, ids_copies, table_copy = copies[i]
        for copy in ids_copies + grad_copies:
            copy.wait()

        def widen(t, carry):
            for j in range(segs):
                rows = pl.ds(pl.multiple_of(t * 32, 32), 32)
                stage[j, rows, :] = grad_v[i, j, rows, :].astype(jnp.float32)
            return carry

        lax.fori_loop(0, seg_rows // 32, widen, 0)

        def add_rows(t, carry):
            base = t * UNROLL
            for u in range(UNROLL):
                for j, bank in enumerate(banks):
                    first, second = ids_s[i][2 * j][0, base + u], ids_s[i][2 * j + 1][0, base + u]
                    same = jnp.full((1, dim), first) == jnp.full((1, dim), second)
                    add_first = stage[2 * j, pl.ds(base + u, 1), :]
                    add_second = stage[2 * j + 1, pl.ds(base + u, 1), :]
                    add_second = jnp.where(same, add_first + add_second, add_second)
                    old_first = bank[pl.ds(first, 1), :]
                    old_second = bank[pl.ds(second, 1), :]
                    bank[pl.ds(first, 1), :] = old_first + add_first
                    bank[pl.ds(second, 1), :] = old_second + add_second
            return carry

        lax.fori_loop(0, (ids_s[i][segs][0, 0] + UNROLL - 1) // UNROLL, add_rows, 0)
        table_copy.wait()
        if i == 0:
            accum_copy.wait()
        if n_carried and i == 0:
            done_copy.wait()

        def update(c, carry):
            for s in range(CHUNK // BLOCK):
                first_row = pl.multiple_of((c * (CHUNK // BLOCK) + s) * BLOCK, BLOCK)
                rows = pl.ds(first_row, BLOCK)
                grad = banks[0][rows, :]
                for bank in banks[1:]:
                    grad = grad + bank[rows, :]
                if i + 1 < n:
                    for bank in banks:
                        bank[rows, :] = zero
                old = jnp.where(eye, accum_v[slot:slot + 1, rows], 0.0)
                new = jnp.sum(grad * grad * (1.0 / dim) + old, axis=1, keepdims=True)
                line = jnp.broadcast_to(new[:8], (8, dim))
                for k in range(1, BLOCK // 8):
                    line = jnp.where(lane_group == k, new[8 * k:8 * k + 8], line)
                done_v[slot:slot + 1, rows] = jnp.sum(jnp.where(eye_line, line, 0.0), axis=0, keepdims=True)
                root = lax.rsqrt(jnp.maximum(new, TINY))
                scale = lr * root / (1.0 + EPSILON * root)
                table_v[i, rows, :] = (table_v[i, rows, :].astype(jnp.float32) - grad * scale).astype(jnp.bfloat16)
            done = pl.ds(pl.multiple_of(c * CHUNK, CHUNK), CHUNK)
            pltpu.make_async_copy(table_v.at[i, done], out_tables_ref.at[slot, done], out_sem.at[i]).start()
            if i == n - 1:
                pltpu.make_async_copy(done_v.at[:, done], out_accums_ref.at[:, done], out_sem.at[n]).start()
            return carry

        lax.fori_loop(0, n_rows // CHUNK, update, 0)
    for i, slot in enumerate(slots):
        pltpu.make_async_copy(table_v.at[i], out_tables_ref.at[slot], out_sem.at[i]).wait()
    pltpu.make_async_copy(done_v, out_accums_ref, out_sem.at[n]).wait()


def apply_slots(slots, ids, lr, grads, tables, accums, carried):
    _, n_rows, dim = tables.shape
    n, segs = len(slots), (len(grads) if len(grads) > 1 else grads[0].shape[0])
    seg_rows = grads[0].shape[-2]
    part = (ids[0].shape[1] - BLOCK) // segs
    assert segs == 2 * BANKS
    return pl.pallas_call(
        functools.partial(apply_kernel, slots, len(carried), len(grads)),
        out_shape=tuple(jax.ShapeDtypeStruct(x.shape, x.dtype) for x in (tables, accums)),
        in_specs=[pl.BlockSpec(memory_space=pltpu.SMEM)]
        + [pl.BlockSpec(memory_space=pl.ANY)] * 2
        + [pl.BlockSpec(memory_space=pl.ANY)] * len(grads)
        + [pl.BlockSpec(memory_space=pl.ANY)] * n
        + [pl.BlockSpec(memory_space=pl.ANY)] * len(carried),
        out_specs=(pl.BlockSpec(memory_space=pl.ANY),) * 2,
        input_output_aliases={3 + len(grads) + n + i: i for i in range(len(carried))},
        scratch_shapes=[pltpu.VMEM((n_rows + 8, dim), jnp.float32)] * BANKS
        + [
            pltpu.VMEM((segs, seg_rows, dim), jnp.float32),
            pltpu.VMEM((n, n_rows, dim), tables.dtype),
            pltpu.VMEM((n, segs, seg_rows, dim), grads[0].dtype),
            pltpu.VMEM(accums.shape, accums.dtype),
            pltpu.VMEM(accums.shape, accums.dtype),
            pltpu.SemaphoreType.DMA((n,)),
            pltpu.SemaphoreType.DMA((n + 2,)),
            pltpu.SemaphoreType.DMA((n, segs + 1)),
            pltpu.SemaphoreType.DMA((n, segs)),
        ]
        + ([pltpu.SMEM((1, part), jnp.int32)] * segs + [pltpu.SMEM((1, BLOCK), jnp.int32)]) * n,
        compiler_params=pltpu.CompilerParams(vmem_limit_bytes=VMEM_LIMIT),
        cost_estimate=pl.CostEstimate(flops=n * n_rows * dim * 400, bytes_accessed=4 * n * n_rows * dim * 2, transcendentals=0),
    )(lr, tables, accums, *grads, *(ids[k] for k in slots), *carried)


def routes(n_dev, n_slots, n_tab, slot, offset):
    pairs = [(d, (d + offset) % n_dev) for d in range(n_dev)]
    return [(src, dst) for src, dst in pairs if dst * n_slots + slot < n_tab]


def solution(mesh):
    n_group = mesh.shape['mp']
    slot_spec = P(('pod', 'mp'))

    def local_step(d_pool, row_ids, lengths, tables, row_accum, learn_rate):
        n_slots, n_rows, _ = tables.shape
        by_table = jnp.transpose(d_pool, (1, 0, 2))
        part = by_table.shape[1]
        me = lax.axis_index('mp').reshape(1)
        n_tab = by_table.shape[0]
        caps = CAPS(part)
        plan, starts, level = make_plan(lengths, n_group, caps)
        lr = learn_rate.reshape(1)

        def exchange(level):
            def run(operands):
                me, by_table, plan, starts, row_ids, lengths, lr, tables, accums = operands
                got = {}
                chunks, hop_slots = CHUNKS(n_slots)
                for c, slots in enumerate(chunks):
                    if slots == hop_slots:
                        pack = pack_hops(slots[0], caps[level], me, starts, plan, by_table)
                    else:
                        pack = pack_slots(slots, caps[level], starts, plan, by_table)
                    if slots == hop_slots:
                        hops = []
                        for o in range(1, n_group):
                            hops.append(lax.ppermute(pack[o], 'mp', routes(n_group, n_slots, n_tab, slots[0], o)))
                        got[c] = [pack[0]] + hops
                    else:
                        got[c] = [lax.all_to_all(pack, 'mp', 0, 0, tiled=True)]
                ids = pack_ids(me, row_ids[:, :, 0], lengths, n_group, n_rows, hop_slots)
                carried = ()
                for c, slots in enumerate(chunks):
                    carried = apply_slots(slots, ids, lr, got[c], tables, accums, carried)
                return tuple(carried)

            return run

        operands = (me, by_table, plan, starts, row_ids, lengths, lr, tables, row_accum)
        return lax.switch(level[0], [exchange(i) for i in range(len(caps))], operands)

    return jax.shard_map(local_step, mesh=mesh, in_specs=(slot_spec, slot_spec, slot_spec, slot_spec, slot_spec, P()), out_specs=(slot_spec, slot_spec), check_vma=False)


def CAPS(part):
    return part * 35 // 64, part * 37 // 64, part


def CHUNKS(n_slots):
    return tuple((k,) for k in range(n_slots)), (n_slots - 2,)
```

```python
import functools

import jax
import jax.numpy as jnp
from jax import lax
from jax.experimental import pallas as pl
from jax.experimental.pallas import tpu as pltpu
from jax.sharding import PartitionSpec as P


EPSILON = 1e-06
TINY = 1e-36
BANKS = 4
UNROLL = 16
BLOCK = 128
CHUNK = 1024
CLEAR = 512
MAX_LANE = 64
VMEM_LIMIT = 66000000
APPLY_VMEM = 66600000


def gather_parts(src_ref, dst, n_dev):
    n_slots, batch = src_ref.shape
    part = batch // n_dev
    for d in range(n_dev):
        dst[d * n_slots:(d + 1) * n_slots, :] = src_ref[:, d * part:(d + 1) * part]


def block_prefix(len_v, b, prefix):
    valid = len_v[:, b * BLOCK:(b + 1) * BLOCK] > 0
    ones = jnp.where(valid, 1.0, 0.0)
    local = jnp.dot(ones.astype(jnp.bfloat16), prefix, preferred_element_type=jnp.float32).astype(jnp.int32)
    return valid, local, jnp.sum(ones, axis=1, keepdims=True).astype(jnp.int32)


def prefix_matrix():
    below = lax.broadcasted_iota(jnp.int32, (BLOCK, BLOCK), 0) < lax.broadcasted_iota(jnp.int32, (BLOCK, BLOCK), 1)
    return jnp.where(below, 1.0, 0.0).astype(jnp.bfloat16)


def ids_kernel(n_dev, n_rows, hop_slots, me_ref, ids_ref, lengths_ref, *refs):
    *packed_refs, ids_v, len_v = refs
    n_slots, batch = ids_ref.shape
    part, rows = batch // n_dev, n_dev * n_slots
    gather_parts(ids_ref, ids_v, n_dev)
    gather_parts(lengths_ref, len_v, n_dev)
    prefix = prefix_matrix()
    lane = lax.broadcasted_iota(jnp.int32, (rows, BLOCK), 1)
    count = jnp.zeros((rows, 1), jnp.int32)
    moves = []
    for b in range(part // BLOCK):
        valid, local, more = block_prefix(len_v, b, prefix)
        shift = (b * BLOCK + lane) - (count + local)
        moves.append(jnp.where(valid, (shift << 16) | ids_v[:, b * BLOCK:(b + 1) * BLOCK], n_rows))
        count = count + more
    move = jnp.concatenate(moves, axis=1)
    step = 1
    while step < part:
        come = pltpu.roll(move, part - step, 1)
        bit = step << 16
        stay = jnp.where((move & bit) != 0, n_rows, move)
        move = jnp.where((come & bit) != 0, come, stay)
        step *= 2
    spot = lax.broadcasted_iota(jnp.int32, (rows, part), 1)
    ids_v[...] = jnp.where(spot < count, move & 0xFFFF, n_rows)
    slot_of = lax.broadcasted_iota(jnp.int32, (rows, 1), 0) % n_slots
    for s in range(n_slots):
        most = jnp.max(jnp.where(slot_of == s, count, 0), axis=0, keepdims=True)
        for d in range(n_dev):
            sender = (me_ref[0] + (n_dev - d)) % n_dev if s in hop_slots else d
            packed_refs[s][:, d * part:(d + 1) * part] = ids_v[pl.ds(sender * n_slots + s, 1), :]
        packed_refs[s][:, n_dev * part:] = jnp.broadcast_to(most, (1, BLOCK))


def pack_ids(me, ids, lengths, n_dev, n_rows, hop_slots):
    n_slots, batch = ids.shape
    part = batch // n_dev
    assert n_rows < 1 << 15 and part <= 1 << 15
    return pl.pallas_call(
        functools.partial(ids_kernel, n_dev, n_rows, hop_slots),
        out_shape=(jax.ShapeDtypeStruct((1, batch + BLOCK), jnp.int32),) * n_slots,
        in_specs=[pl.BlockSpec(memory_space=pltpu.SMEM)] + [pl.BlockSpec(memory_space=pltpu.VMEM)] * 2,
        out_specs=(pl.BlockSpec(memory_space=pltpu.VMEM),) * n_slots,
        scratch_shapes=[pltpu.VMEM((n_dev * n_slots, part), jnp.int32)] * 2,
        compiler_params=pltpu.CompilerParams(vmem_limit_bytes=32000000),
        cost_estimate=pl.CostEstimate(flops=20000000, bytes_accessed=2000000, transcendentals=0),
    )(me, ids, lengths)


def write_plan(lengths_ref, plan_ref, len_v):
    n_dev, n_slots, width = plan_ref.shape
    part, rows = width - BLOCK, n_dev * n_slots
    gather_parts(lengths_ref, len_v, n_dev)
    prefix = prefix_matrix()
    lane = lax.broadcasted_iota(jnp.int32, (rows, BLOCK), 1)
    count = jnp.zeros((rows, 1), jnp.int32)
    starts = jnp.zeros((rows, BLOCK), jnp.int32)
    for b in range(part // BLOCK):
        valid, local, more = block_prefix(len_v, b, prefix)
        place = jnp.where(valid, local, -1)
        for d in range(n_dev):
            plan_ref[d, :, b * BLOCK:(b + 1) * BLOCK] = place[d * n_slots:(d + 1) * n_slots, :]
        starts = jnp.where(lane == b, count, starts)
        count = count + more
    starts = jnp.where(lane == MAX_LANE, jnp.max(count, axis=0, keepdims=True), starts)
    for d in range(n_dev):
        plan_ref[d, :, part:] = starts[d * n_slots:(d + 1) * n_slots, :]


def plan_kernel(n_dev, caps, lengths_ref, plans_ref, starts_ref, level_ref, plan_ref, len_v, send_sem, recv_sem, own_sem):
    pod, me = lax.axis_index('pod'), lax.axis_index('mp')
    barrier = pltpu.get_barrier_semaphore()
    for o in range(1, n_dev):
        pl.semaphore_signal(barrier, inc=1, device_id=(pod, (me + o) % n_dev), device_id_type=pl.DeviceIdType.MESH)
    write_plan(lengths_ref, plan_ref, len_v)
    pl.semaphore_wait(barrier, n_dev - 1)
    copies = [
        pltpu.make_async_remote_copy(
            src_ref=plan_ref.at[(me + o) % n_dev],
            dst_ref=plans_ref.at[me],
            send_sem=send_sem.at[o],
            recv_sem=recv_sem.at[o],
            device_id=(pod, (me + o) % n_dev),
            device_id_type=pl.DeviceIdType.MESH,
        )
        for o in range(1, n_dev)
    ]
    for copy in copies:
        copy.start()
    own = pltpu.make_async_copy(plan_ref.at[me], plans_ref.at[me], own_sem)
    own.start()
    own.wait()
    for copy in copies:
        copy.wait()
    part = plans_ref.shape[2] - BLOCK
    starts = plans_ref[:, :, part:]
    starts_ref[...] = starts
    most = jnp.max(starts[:, :, MAX_LANE:MAX_LANE + 1])
    level_ref[0] = sum((most > cap).astype(jnp.int32) for cap in caps[:-1])


def make_plan(lengths, n_dev, caps):
    n_slots, batch = lengths.shape
    part = batch // n_dev
    plan_shape = (n_dev, n_slots, part + BLOCK)
    return pl.pallas_call(
        functools.partial(plan_kernel, n_dev, caps),
        out_shape=(
            jax.ShapeDtypeStruct(plan_shape, jnp.int32),
            jax.ShapeDtypeStruct((n_dev, n_slots, BLOCK), jnp.int32),
            jax.ShapeDtypeStruct((1,), jnp.int32),
        ),
        in_specs=[pl.BlockSpec(memory_space=pltpu.VMEM)],
        out_specs=(pl.BlockSpec(memory_space=pltpu.VMEM), pl.BlockSpec(memory_space=pltpu.VMEM), pl.BlockSpec(memory_space=pltpu.SMEM)),
        scratch_shapes=[
            pltpu.VMEM(plan_shape, jnp.int32),
            pltpu.VMEM((n_dev * n_slots, part), jnp.int32),
            pltpu.SemaphoreType.DMA((n_dev,)),
            pltpu.SemaphoreType.DMA((n_dev,)),
            pltpu.SemaphoreType.DMA,
        ],
        compiler_params=pltpu.CompilerParams(collective_id=0, has_side_effects=True, vmem_limit_bytes=16000000),
        cost_estimate=pl.CostEstimate(flops=20000000, bytes_accessed=2000000, transcendentals=0),
    )(lengths)


def pack_kernel(slots, starts_ref, plan_ref, tables_ref, out_ref, grad_v, stage, pack_v, in_sem, out_sem):
    n_slots = plan_ref.shape[1]
    cap = out_ref.shape[2]
    n_tab, part, _ = tables_ref.shape
    slot_row = lax.broadcasted_iota(jnp.int32, (BLOCK, BLOCK), 0)
    used = [[d for d in range(out_ref.shape[0]) if d * n_slots + slot < n_tab] for slot in slots]

    def fetch(i, d):
        return pltpu.make_async_copy(tables_ref.at[d * n_slots + slots[i]], grad_v.at[i, d], in_sem.at[i, d])

    def emit(i, d):
        return pltpu.make_async_copy(pack_v.at[i, d], out_ref.at[d, i], out_sem.at[i, d])

    for i, dests in enumerate(used):
        for d in dests:
            fetch(i, d).start()
    for i, dests in enumerate(used):
        def table(d, carry):
            fetch(i, d).wait()
            for b in range(part // BLOCK):
                place = plan_ref[d, slots[i]:slots[i] + 1, b * BLOCK:(b + 1) * BLOCK]
                pick = jnp.where(slot_row == place, 1.0, 0.0).astype(jnp.bfloat16)
                rows = jnp.dot(pick, grad_v[i, d, b * BLOCK:(b + 1) * BLOCK, :], preferred_element_type=jnp.float32)
                stage[pl.ds(starts_ref[d, slots[i], b], BLOCK), :] = rows
            pack_v[i, d] = stage[:cap, :].astype(jnp.bfloat16)
            emit(i, d).start()
            return carry

        lax.fori_loop(0, len(dests), table, 0)
    for i, dests in enumerate(used):
        for d in dests:
            emit(i, d).wait()


def pack_slots(slots, cap, starts, plan, by_table):
    n_dev = plan.shape[0]
    _, part, dim = by_table.shape
    n = len(slots)
    return pl.pallas_call(
        functools.partial(pack_kernel, slots),
        out_shape=jax.ShapeDtypeStruct((n_dev, n, cap, dim), by_table.dtype),
        in_specs=[pl.BlockSpec(memory_space=pltpu.SMEM), pl.BlockSpec(memory_space=pltpu.VMEM), pl.BlockSpec(memory_space=pl.ANY)],
        out_specs=pl.BlockSpec(memory_space=pl.ANY),
        scratch_shapes=[
            pltpu.VMEM((n, n_dev, part, dim), by_table.dtype),
            pltpu.VMEM((cap + BLOCK, dim), jnp.float32),
            pltpu.VMEM((n, n_dev, cap, dim), by_table.dtype),
            pltpu.SemaphoreType.DMA((n, n_dev)),
            pltpu.SemaphoreType.DMA((n, n_dev)),
        ],
        compiler_params=pltpu.CompilerParams(vmem_limit_bytes=VMEM_LIMIT),
        cost_estimate=pl.CostEstimate(flops=n * n_dev * part * dim * 20, bytes_accessed=n * n_dev * part * dim * 3, transcendentals=0),
    )(starts, plan, by_table)


def pack_hops_kernel(slot, me_ref, starts_ref, plan_ref, tables_ref, *refs):
    n_dev, n_slots, _ = plan_ref.shape
    n_tab, part, _ = tables_ref.shape
    out_refs, (grad_v, stage, pack_v, in_sem, out_sem) = refs[:n_dev], refs[n_dev:]
    cap = pack_v.shape[1]
    slot_row = lax.broadcasted_iota(jnp.int32, (BLOCK, BLOCK), 0)
    me = me_ref[0]

    def fetch(o):
        table = jnp.minimum((me + o) % n_dev * n_slots + slot, n_tab - 1)
        return pltpu.make_async_copy(tables_ref.at[table], grad_v.at[o], in_sem.at[o])

    for o in range(n_dev):
        fetch(o).start()

    def one(o, carry):
        d = (me + o) % n_dev
        fetch(o).wait()

        @pl.when(d * n_slots + slot < n_tab)
        def _():
            for b in range(part // BLOCK):
                place = plan_ref[d, slot:slot + 1, b * BLOCK:(b + 1) * BLOCK]
                pick = jnp.where(slot_row == place, 1.0, 0.0).astype(jnp.bfloat16)
                rows = jnp.dot(pick, grad_v[o, b * BLOCK:(b + 1) * BLOCK, :], preferred_element_type=jnp.float32)
                stage[pl.ds(starts_ref[d, slot, b], BLOCK), :] = rows
            pack_v[o] = stage[:cap, :].astype(jnp.bfloat16)

        return carry

    lax.fori_loop(0, n_dev, one, 0)
    copies = [pltpu.make_async_copy(pack_v.at[o], out_refs[o], out_sem.at[o]) for o in range(n_dev)]
    for copy in copies:
        copy.start()
    for copy in copies:
        copy.wait()


def pack_hops(slot, cap, me, starts, plan, by_table):
    n_dev, _, _ = plan.shape
    _, part, dim = by_table.shape
    return pl.pallas_call(
        functools.partial(pack_hops_kernel, slot),
        out_shape=(jax.ShapeDtypeStruct((cap, dim), by_table.dtype),) * n_dev,
        in_specs=[pl.BlockSpec(memory_space=pltpu.SMEM)] * 2 + [pl.BlockSpec(memory_space=pltpu.VMEM), pl.BlockSpec(memory_space=pl.ANY)],
        out_specs=(pl.BlockSpec(memory_space=pl.ANY),) * n_dev,
        scratch_shapes=[
            pltpu.VMEM((n_dev, part, dim), by_table.dtype),
            pltpu.VMEM((cap + BLOCK, dim), jnp.float32),
            pltpu.VMEM((n_dev, cap, dim), by_table.dtype),
            pltpu.SemaphoreType.DMA((n_dev,)),
            pltpu.SemaphoreType.DMA((n_dev,)),
        ],
        compiler_params=pltpu.CompilerParams(vmem_limit_bytes=VMEM_LIMIT),
        cost_estimate=pl.CostEstimate(flops=n_dev * part * dim * 20, bytes_accessed=n_dev * part * dim * 3, transcendentals=0),
    )(me, starts, plan, by_table)


def apply_kernel(slots, n_carried, n_grads, lr_ref, tables_ref, accums_ref, *refs):
    n = len(slots)
    grad_refs, refs = refs[:n_grads], refs[n_grads:]
    ids_refs, carried_refs = refs[:n], refs[n:n + n_carried]
    out_tables_ref, out_accums_ref, *scratch = refs[n + n_carried:]
    banks, (stage, table_v, grad_v, done_v, sem, out_sem, ids_sem, grad_sem), scalars = scratch[:BANKS], scratch[BANKS:BANKS + 8], scratch[BANKS + 8:]
    _, segs, seg_rows, dim = grad_v.shape
    part = (ids_refs[0].shape[1] - BLOCK) // segs
    ids_s = [scalars[i * (segs + 1):(i + 1) * (segs + 1)] for i in range(n)]
    n_rows = tables_ref.shape[1]
    copies = [
        (
            [pltpu.make_async_copy(ref, grad_v.at[i, o], grad_sem.at[i, o]) for o, ref in enumerate(grad_refs)]
            if n_grads > 1
            else [pltpu.make_async_copy(grad_refs[0].at[:, i], grad_v.at[i], grad_sem.at[i, 0])],
            [pltpu.make_async_copy(ids_refs[i].at[:, j * part:(j + 1) * part], ids_s[i][j], ids_sem.at[i, j]) for j in range(segs)]
            + [pltpu.make_async_copy(ids_refs[i].at[:, segs * part:], ids_s[i][segs], ids_sem.at[i, segs])],
            pltpu.make_async_copy(tables_ref.at[slot], table_v.at[i], sem.at[i]),
        )
        for i, slot in enumerate(slots)
    ]
    for grad_copies, ids_copies, table_copy in copies:
        for copy in ids_copies + grad_copies:
            copy.start()
        table_copy.start()

    if n_carried:
        done_copy = pltpu.make_async_copy(carried_refs[1], done_v, out_sem.at[n])
        done_copy.start()
    zero = jnp.zeros((BLOCK, dim), jnp.float32)

    def clear(i, carry):
        for bank in banks:
            for s in range(CLEAR // BLOCK):
                bank[pl.ds(pl.multiple_of(i * CLEAR, CLEAR) + s * BLOCK, BLOCK), :] = zero
        return carry

    lax.fori_loop(0, n_rows // CLEAR, clear, 0)
    for bank in banks:
        bank[pl.ds(n_rows, 8), :] = zero[:8]
    eye = lax.broadcasted_iota(jnp.int32, (BLOCK, dim), 0) == lax.broadcasted_iota(jnp.int32, (BLOCK, dim), 1)
    lane = lax.broadcasted_iota(jnp.int32, (8, dim), 1)
    lane_group = lane // 8
    eye_line = lane % 8 == lax.broadcasted_iota(jnp.int32, (8, dim), 0)
    lr = lr_ref[0]

    for i, slot in enumerate(slots):
        grad_copies, ids_copies, table_copy = copies[i]
        for copy in ids_copies + grad_copies:
            copy.wait()

        def widen(t, carry):
            for j in range(segs):
                rows = pl.ds(pl.multiple_of(t * 32, 32), 32)
                stage[j, rows, :] = grad_v[i, j, rows, :].astype(jnp.float32)
            return carry

        lax.fori_loop(0, seg_rows // 32, widen, 0)

        def add_rows(t, carry):
            base = t * UNROLL
            for u in range(UNROLL):
                for j, bank in enumerate(banks):
                    first, second = ids_s[i][2 * j][0, base + u], ids_s[i][2 * j + 1][0, base + u]
                    same = jnp.full((1, dim), first) == jnp.full((1, dim), second)
                    add_first = stage[2 * j, pl.ds(base + u, 1), :]
                    add_second = stage[2 * j + 1, pl.ds(base + u, 1), :]
                    add_second = jnp.where(same, add_first + add_second, add_second)
                    old_first = bank[pl.ds(first, 1), :]
                    old_second = bank[pl.ds(second, 1), :]
                    bank[pl.ds(first, 1), :] = old_first + add_first
                    bank[pl.ds(second, 1), :] = old_second + add_second
            return carry

        lax.fori_loop(0, (ids_s[i][segs][0, 0] + UNROLL - 1) // UNROLL, add_rows, 0)
        table_copy.wait()
        if n_carried and i == 0:
            done_copy.wait()

        def update(c, carry):
            for s in range(CHUNK // BLOCK):
                first_row = pl.multiple_of((c * (CHUNK // BLOCK) + s) * BLOCK, BLOCK)
                rows = pl.ds(first_row, BLOCK)
                grad = banks[0][rows, :]
                for bank in banks[1:]:
                    grad = grad + bank[rows, :]
                if i + 1 < n:
                    for bank in banks:
                        bank[rows, :] = zero
                old = jnp.where(eye, accums_ref[slot:slot + 1, rows], 0.0)
                new = jnp.sum(grad * grad * (1.0 / dim) + old, axis=1, keepdims=True)
                line = jnp.broadcast_to(new[:8], (8, dim))
                for k in range(1, BLOCK // 8):
                    line = jnp.where(lane_group == k, new[8 * k:8 * k + 8], line)
                done_v[slot:slot + 1, rows] = jnp.sum(jnp.where(eye_line, line, 0.0), axis=0, keepdims=True)
                root = lax.rsqrt(jnp.maximum(new, TINY))
                scale = lr * root / (1.0 + EPSILON * root)
                table_v[i, rows, :] = (table_v[i, rows, :].astype(jnp.float32) - grad * scale).astype(jnp.bfloat16)
            done = pl.ds(pl.multiple_of(c * CHUNK, CHUNK), CHUNK)
            pltpu.make_async_copy(table_v.at[i, done], out_tables_ref.at[slot, done], out_sem.at[i]).start()
            if i == n - 1:
                pltpu.make_async_copy(done_v.at[:, done], out_accums_ref.at[:, done], out_sem.at[n]).start()
            return carry

        lax.fori_loop(0, n_rows // CHUNK, update, 0)
    for i, slot in enumerate(slots):
        pltpu.make_async_copy(table_v.at[i], out_tables_ref.at[slot], out_sem.at[i]).wait()
    pltpu.make_async_copy(done_v, out_accums_ref, out_sem.at[n]).wait()


def apply_slots(slots, ids, lr, grads, tables, accums, carried):
    _, n_rows, dim = tables.shape
    n, segs = len(slots), (len(grads) if len(grads) > 1 else grads[0].shape[0])
    seg_rows = grads[0].shape[-2]
    part = (ids[0].shape[1] - BLOCK) // segs
    assert segs == 2 * BANKS
    return pl.pallas_call(
        functools.partial(apply_kernel, slots, len(carried), len(grads)),
        out_shape=tuple(jax.ShapeDtypeStruct(x.shape, x.dtype) for x in (tables, accums)),
        in_specs=[pl.BlockSpec(memory_space=pltpu.SMEM)]
        + [pl.BlockSpec(memory_space=pl.ANY), pl.BlockSpec(memory_space=pltpu.VMEM)]
        + [pl.BlockSpec(memory_space=pl.ANY)] * (len(grads) + n)
        + [pl.BlockSpec(memory_space=pl.ANY)] * len(carried),
        out_specs=(pl.BlockSpec(memory_space=pl.ANY),) * 2,
        input_output_aliases={3 + len(grads) + n + i: i for i in range(len(carried))},
        scratch_shapes=[pltpu.VMEM((n_rows + 8, dim), jnp.float32)] * BANKS
        + [
            pltpu.VMEM((segs, seg_rows, dim), jnp.float32),
            pltpu.VMEM((n, n_rows, dim), tables.dtype),
            pltpu.VMEM((n, segs, seg_rows, dim), grads[0].dtype),
            pltpu.VMEM(accums.shape, accums.dtype),
            pltpu.SemaphoreType.DMA((n,)),
            pltpu.SemaphoreType.DMA((n + 1,)),
            pltpu.SemaphoreType.DMA((n, segs + 1)),
            pltpu.SemaphoreType.DMA((n, segs)),
        ]
        + ([pltpu.SMEM((1, part), jnp.int32)] * segs + [pltpu.SMEM((1, BLOCK), jnp.int32)]) * n,
        compiler_params=pltpu.CompilerParams(vmem_limit_bytes=APPLY_VMEM),
        cost_estimate=pl.CostEstimate(flops=n * n_rows * dim * 400, bytes_accessed=4 * n * n_rows * dim * 2, transcendentals=0),
    )(lr, tables, accums, *grads, *(ids[k] for k in slots), *carried)


def routes(n_dev, n_slots, n_tab, slot, offset):
    pairs = [(d, (d + offset) % n_dev) for d in range(n_dev)]
    return [(src, dst) for src, dst in pairs if dst * n_slots + slot < n_tab]


def solution(mesh):
    n_group = mesh.shape['mp']
    slot_spec = P(('pod', 'mp'))

    def local_step(d_pool, row_ids, lengths, tables, row_accum, learn_rate):
        n_slots, n_rows, _ = tables.shape
        by_table = jnp.transpose(d_pool, (1, 0, 2))
        part = by_table.shape[1]
        me = lax.axis_index('mp').reshape(1)
        n_tab = by_table.shape[0]
        caps = CAPS(part)
        plan, starts, level = make_plan(lengths, n_group, caps)
        lr = learn_rate.reshape(1)

        def exchange(level):
            def run(operands):
                me, by_table, plan, starts, row_ids, lengths, lr, tables, accums = operands
                got = {}
                chunks, hop_slots = CHUNKS(n_slots)
                for c, slots in enumerate(chunks):
                    if slots == hop_slots:
                        pack = pack_hops(slots[0], caps[level], me, starts, plan, by_table)
                    else:
                        pack = pack_slots(slots, caps[level], starts, plan, by_table)
                    if slots == hop_slots:
                        hops = []
                        for o in range(1, n_group):
                            hops.append(lax.ppermute(pack[o], 'mp', routes(n_group, n_slots, n_tab, slots[0], o)))
                        got[c] = [pack[0]] + hops
                    else:
                        got[c] = [lax.all_to_all(pack, 'mp', 0, 0, tiled=True)]
                ids = pack_ids(me, row_ids[:, :, 0], lengths, n_group, n_rows, hop_slots)
                carried = ()
                for c, slots in enumerate(chunks):
                    carried = apply_slots(slots, ids, lr, got[c], tables, accums, carried)
                return tuple(carried)

            return run

        operands = (me, by_table, plan, starts, row_ids, lengths, lr, tables, row_accum)
        return lax.switch(level[0], [exchange(i) for i in range(len(caps))], operands)

    return jax.shard_map(local_step, mesh=mesh, in_specs=(slot_spec, slot_spec, slot_spec, slot_spec, slot_spec, P()), out_specs=(slot_spec, slot_spec), check_vma=False)


def CAPS(part):
    return part * 35 // 64, part * 37 // 64, part


def CHUNKS(n_slots):
    return tuple((k,) for k in range(n_slots)), (n_slots - 2,)
```
